512 devices in a mesh: img: 2 (over y), sub: 32 (over z, core), rng: 8 (over x).
Axes of the slice: x: 8, y: 2, z: 16, core: 2. Of those that a mesh axis runs over, the one named last changes fastest.
The devices are a block of a 8x8x16 slice.
Arguments:
- image: bfloat16 [2, 128, 128, 4096], P(None, ('img', 'sub'), None, 'rng'), parts along dimension 1, may hold values from -6 to 6
- interp_weights: bfloat16 [4, 2, 2, 2, 128, 128], replicated, may hold values from -0.25 to 0.25
- range_taps: float32 [4, 4], replicated, may hold values from -2 to 2
- range_shifts: int32 [4, 2, 128], replicated, may hold values from -8 to 5
Outputs:
- merged_image: bfloat16 [2, 128, 128, 4096], P(None, ('img', 'sub'), None, 'rng'), parts along dimension 1
The draws below stay inside these ranges and needn't reach their ends.
There are 2 independent parts, one for each index of `img`. The reference program is written for one: setup_inputs(seed, part) draws one part's arguments, and reference() takes and returns one part's arrays. A program takes and returns all parts, laid end to end along the dimension named above; an argument that names none is the same for every part. Nothing has to cross between parts.
All inputs are finite; a program needn't handle non-finite values.
Results may differ from the reference program's by a relative error of at most 0.0095.
Values may be sent and summed in bfloat16 or wider, within the bound.
A program may use at most 64 MiB of HBM per device.

```python
import math
import jax
import jax.numpy as jnp
import numpy as np

ANGLES = 128
RANGE = 4096
RIM = 8
TAPS = 4
LEVELS = 4
GROUPS = 2
SUBIMAGES = 64
N_SUB = 32


def touch_ends(entries, rng, smallest, top_value):
    spot = [jax.random.randint(jax.random.fold_in(rng, axis), (), 0, length) for axis, length in enumerate(entries.shape)]
    widest = entries.shape.index(max(entries.shape))
    next_to = spot[:widest] + [(spot[widest] + 1) % entries.shape[widest]] + spot[widest + 1:]
    return entries.at[tuple(spot)].set(smallest).at[tuple(next_to)].set(top_value)


def block_levels(own_key, dims, cuts, least, high):
    gain, own = 1.0, jax.random.fold_in(own_key, 6)
    for dim, shards_of in cuts:
        draws = jnp.exp(jax.random.uniform(jax.random.fold_in(own, dim), (shards_of,), jnp.float32, least / len(cuts), high / len(cuts)))
        gain = gain * jnp.repeat(draws, dims[dim] // shards_of).reshape([-1 if axis == dim else 1 for axis in range(len(dims))])
    return gain


def normal_values(stream_key, shape, deviation, bound, cuts=(), held_as=jnp.bfloat16):
    entries = deviation * jax.random.normal(stream_key, shape, jnp.float32)
    if cuts:
        entries = entries * block_levels(stream_key, shape, cuts, -0.22, 0.18)
    return jnp.clip(entries, -bound, bound).astype(held_as)


def setup_inputs(seed: int = 0, part: int = 0) -> dict:
    streams_of = jax.random.split(jax.random.key(seed), 5)
    part_keys = jax.random.split(jax.random.fold_in(streams_of[4], part), 5)
    image = normal_values(part_keys[0], (2, SUBIMAGES, ANGLES, RANGE), 1.0, 6.0, ((1, 32), (3, 8)))
    interp_weights = normal_values(streams_of[1], (LEVELS, 2, 2, 2, ANGLES, ANGLES), (4 * ANGLES) ** -0.5, 0.25)
    range_taps = normal_values(streams_of[2], (LEVELS, TAPS), 0.5, 2.0, (), jnp.float32)
    range_shifts = touch_ends(jax.random.randint(streams_of[3], (LEVELS, 2, ANGLES), 0 - RIM, RIM - TAPS + 2), jax.random.fold_in(streams_of[3], 1), 0 - RIM, (RIM - TAPS + 2) - 1).astype(jnp.int32)
    return dict(image=image, interp_weights=interp_weights, range_taps=range_taps, range_shifts=range_shifts)


phase_step = 2.0 * math.pi / 64.0


def rotate(merged_sum, level_index, half_index, range_start, range_width):
    angle_rows = half_index * ANGLES + jnp.arange(ANGLES, dtype=jnp.int32)
    range_cols = range_start + jnp.arange(range_width, dtype=jnp.int32)
    wrapped = (range_cols[None, :] * (angle_rows[:, None] + 1) * (7 + level_index)) % 64
    phase = wrapped.astype(jnp.float32) * phase_step
    cosine = jnp.cos(phase)
    sinus = jnp.sin(phase)
    return jnp.stack([merged_sum[0] * cosine - merged_sum[1] * sinus, merged_sum[0] * sinus + merged_sum[1] * cosine])


def reference(image, interp_weights, range_taps, range_shifts):
    bit_count = N_SUB.bit_length() - 1
    count = N_SUB * GROUPS
    current = image
    for level_index in range(LEVELS):
        bit = level_index % bit_count
        stride = 2 ** bit
        side_of_rows = (np.arange(count) // GROUPS // stride) % 2
        padded = jnp.pad(current, ((0, 0), (0, 0), (0, 0), (RIM, RIM)))
        shift_rows = range_shifts[level_index][side_of_rows]
        base_index = (RIM + shift_rows[:, :, None] + jnp.arange(RANGE, dtype=jnp.int32)[None, None, :]).astype(jnp.int32)
        total = jnp.zeros(current.shape, jnp.float32)
        for tap_index in range(TAPS):
            gathered = jnp.stack([jnp.take_along_axis(padded[channel], base_index + tap_index, axis=2) for channel in range(2)])
            total = total + range_taps[level_index, tap_index] * gathered.astype(jnp.float32)
        interpolated = total.astype(jnp.bfloat16)
        split_rows = interpolated.reshape(2, N_SUB // (2 * stride), 2, stride, GROUPS, ANGLES, RANGE)
        half_images = []
        for half_index in range(2):
            merged_sum = jnp.zeros((2, N_SUB // (2 * stride), stride, GROUPS, ANGLES, RANGE), jnp.float32)
            for side_index in range(2):
                weight_pair = interp_weights[level_index, side_index, half_index].astype(jnp.float32)
                block_matrix = jnp.stack([jnp.stack([weight_pair[0], -weight_pair[1]]), jnp.stack([weight_pair[1], weight_pair[0]])])
                source = split_rows[:, :, side_index].astype(jnp.float32)
                merged_sum = merged_sum + jnp.einsum('xcij,chmgjr->xhmgir', block_matrix, source)
            half_images.append(rotate(merged_sum, level_index, half_index, 0, RANGE))
        current = jnp.stack(half_images, axis=2).reshape(2, count, ANGLES, RANGE).astype(jnp.bfloat16)
    return current
```

```python
import math

import jax
import jax.numpy as jnp
from jax import lax
from jax.experimental import pallas as pl
from jax.experimental.pallas import tpu as pltpu
from jax.sharding import PartitionSpec as P

ANGLES = 128
RIM = 8
TAPS = 4
LEVELS = 4
PERIOD = 64
PHASE_STEP = 2.0 * math.pi / PERIOD

MESH = pl.DeviceIdType.MESH
F32 = jnp.float32
BF16 = jnp.bfloat16

CHUNK1 = ((0, 160), (160, 128))
CHUNK2 = ((0, 144), (144, 128))
CHUNK3 = ((0, 128), (128, 128))
ROWS0 = 112
TABLE = 256


def xor2(a, m):
    return (a % 2 + m % 2) % 2 + 2 * ((a // 2 + m // 2) % 2)


def kernel(
    image_hbm, weights_hbm, taps, shifts, out,
    image, weights, wide, cos_t, sin_t, cos_last, sin_last,
    rows_bf, first, from_core, halo, x1, y1, units, x2, x3, y3, turned,
    load_sem, core_sem, halo_send, halo_recv, in_send, in_recv, pair_send, pair_recv, out_send, out_recv,
):
    sub = lax.axis_index("sub")
    rng = lax.axis_index("rng")
    last_rng = lax.axis_size("rng") - 1
    core = sub % 2
    z = sub // 2
    zl = z % 8
    base = z - zl
    quad = zl % 4
    upper = zl // 4
    half = (zl // 2) % 2
    side0 = zl % 2
    width = image.shape[3]
    hw = width // 2

    def device(z_local, core_index):
        return {"sub": (base + z_local) * 2 + core_index}

    partner = {"sub": z * 2 + (1 - core)}
    in_peers = [device(4 * core + xor2(quad, m), upper) for m in range(4)]
    self_in = upper == core
    out_dests = [device(4 * core + xor2(quad, m), side0) for m in range(4)]
    out_sources = [device(2 * k + core, upper) for k in range(4)]
    self_out = jnp.logical_and(upper == core, side0 == core)

    barrier = pltpu.get_barrier_semaphore()

    def greet(who):
        pl.semaphore_signal(barrier, inc=1, device_id=who, device_id_type=MESH)

    greet(partner)
    for c in range(2):
        @pl.when(rng > 0)
        def _():
            greet({"sub": z * 2 + c, "rng": rng - 1})

        @pl.when(rng < last_rng)
        def _():
            greet({"sub": z * 2 + c, "rng": rng + 1})

    for m in range(4):
        if m == 0:
            @pl.when(jnp.logical_not(self_in))
            def _():
                greet(in_peers[0])

            @pl.when(jnp.logical_not(self_out))
            def _():
                greet(out_dests[0])
        else:
            greet(in_peers[m])
            greet(out_dests[m])
    for k in range(4):
        @pl.when(jnp.logical_not(jnp.logical_and(self_out, zl // 2 == k)))
        def _():
            greet(out_sources[k])

    load_image = pltpu.make_async_copy(image_hbm, image, load_sem.at[0])
    load_weights = pltpu.make_async_copy(weights_hbm, weights, load_sem.at[1])
    load_image.start()
    load_weights.start()

    def fill_table(level):
        r = lax.broadcasted_iota(jnp.int32, (PERIOD, ANGLES), 0)
        a = lax.broadcasted_iota(jnp.int32, (PERIOD, ANGLES), 1)
        for h in range(2):
            phase = ((r * (h * ANGLES + a + 1) * (7 + level)) % PERIOD).astype(F32) * PHASE_STEP
            c, s = jnp.cos(phase), jnp.sin(phase)
            for i in range(TABLE // PERIOD):
                cos_t[level, h, pl.ds(i * PERIOD, PERIOD), :] = c
                sin_t[level, h, pl.ds(i * PERIOD, PERIOD), :] = s

    fill_table(0)
    load_image.wait()

    for ch in range(2):
        for j in range(2):
            for k in range(width // 128):
                block = image[ch, j, :, pl.ds(k * 128, 128)].astype(F32).T
                rows_bf[j, ch, pl.ds(k * 128, 128), :] = block.astype(BF16)

    load_weights.wait()

    def fill_wide(level):
        for side in range(2):
            for h in range(2):
                wr = weights[level, side, h, 0].astype(F32).T.astype(BF16)
                wi = weights[level, side, h, 1].astype(F32).T.astype(BF16)
                for c, x, value in ((0, 0, wr), (1, 0, -wi), (0, 1, wi), (1, 1, wr)):
                    wide[level, pl.ds((side * 2 + c) * 128, 128), pl.ds((h * 2 + x) * 128, 128)] = value

    fill_wide(0)

    count = (
        1
        + 2 * jnp.where(rng > 0, 1, 0)
        + 2 * jnp.where(rng < last_rng, 1, 0)
        + jnp.where(self_in, 3, 4)
        + jnp.where(self_out, 6, 8)
    )
    pl.semaphore_wait(barrier, count)

    to_core = pltpu.make_async_remote_copy(
        src_ref=rows_bf.at[1 - core],
        dst_ref=from_core,
        send_sem=core_sem.at[0],
        recv_sem=core_sem.at[1],
        device_id=partner,
        device_id_type=MESH,
    )
    margin = LEVELS * RIM

    def halo_copy(j, lr):
        start = 0 if lr == 0 else width - margin
        return pltpu.make_async_remote_copy(
            src_ref=rows_bf.at[j, :, pl.ds(start, margin), :],
            dst_ref=halo.at[core, lr],
            send_sem=halo_send.at[j, lr],
            recv_sem=halo_recv.at[core, lr],
            device_id={"sub": z * 2 + j, "rng": rng - 1 + 2 * lr},
            device_id_type=MESH,
        )

    def halo_wait(side, lr):
        return pltpu.make_async_remote_copy(
            src_ref=rows_bf.at[0, :, pl.ds(0, margin), :],
            dst_ref=halo.at[side, lr],
            send_sem=halo_send.at[0, lr],
            recv_sem=halo_recv.at[side, lr],
            device_id=partner,
            device_id_type=MESH,
        )

    to_core.start()
    for j in range(2):
        @pl.when(rng > 0)
        def _():
            halo_copy(j, 0).start()

        @pl.when(rng < last_rng)
        def _():
            halo_copy(j, 1).start()

    for ch in range(2):
        first[core, ch, pl.ds(margin, width), :] = rows_bf[core, ch].astype(F32)
    to_core.wait_recv()
    for ch in range(2):
        first[1 - core, ch, pl.ds(margin, width), :] = from_core[ch].astype(F32)

    for lr, start, there in ((1, 0, rng > 0), (0, margin + width, rng < last_rng)):
        @pl.when(there)
        def _():
            for side in range(2):
                halo_wait(side, lr).wait_recv()
                for ch in range(2):
                    first[side, ch, pl.ds(start, margin), :] = halo[side, lr, ch].astype(F32)

        @pl.when(jnp.logical_not(there))
        def _():
            first[:, :, pl.ds(start, margin), :] = jnp.zeros((2, 2, margin, ANGLES), F32)

    def bits_of(row):
        code = row + RIM
        return [((code // v) % 2) == 1 for v in (1, 2, 4, 8)]

    def shift_row(level, side):
        return shifts[level, pl.ds(side, 1), :]

    def interpolate(load, rows, bits, level):
        n = rows + 8
        b0, b1, b2, b3 = bits
        v = jnp.where(
            b3,
            jnp.where(b2, load(12, n), load(8, n)),
            jnp.where(b2, load(4, n), load(0, n)),
        )
        v = jnp.where(b0, pltpu.roll(v, n - 1, 0), v)
        v = jnp.where(b1, pltpu.roll(v, n - 2, 0), v)
        total = v * taps[level, 0]
        for t in range(1, TAPS):
            total = total + pltpu.roll(v, n - t, 0) * taps[level, t]
        return total[:rows].astype(BF16)

    def turn(level, h, start, rows, re, im):
        c = cos_t[level, h, pl.ds(start, rows), :]
        s = sin_t[level, h, pl.ds(start, rows), :]
        return re * c - im * s, re * s + im * c

    bits0 = [bits_of(shift_row(0, side)) for side in range(2)]
    rows1 = width + 2 * (margin - RIM)

    def level0(i, carry):
        b = pl.multiple_of(i * ROWS0, 16)
        parts = []
        for side in range(2):
            for ch in range(2):
                parts.append(interpolate(lambda o, n: first[side, ch, pl.ds(b + o, n), :], ROWS0, bits0[side], 0))
        z = jnp.dot(jnp.concatenate(parts, axis=1), wide[0], preferred_element_type=F32)
        start = pl.multiple_of((b + PERIOD - (margin - RIM)) % PERIOD, 8)
        for h in range(2):
            re, im = turn(0, h, start, ROWS0, z[:, h * 256 : h * 256 + 128], z[:, h * 256 + 128 : h * 256 + 256])
            x1[h, 0, pl.ds(b, ROWS0), :] = re
            x1[h, 1, pl.ds(b, ROWS0), :] = im
        return carry

    lax.fori_loop(0, rows1 // ROWS0, level0, 0)

    @pl.when(rng == 0)
    def _():
        x1[:, :, pl.ds(0, margin - RIM), :] = jnp.zeros((2, 2, margin - RIM, ANGLES), F32)

    @pl.when(rng == last_rng)
    def _():
        x1[:, :, pl.ds(rows1 - (margin - RIM), margin - RIM), :] = jnp.zeros((2, 2, margin - RIM, ANGLES), F32)

    own_bits1 = [((shift_row(1, side0) + RIM) // v) % 2 == 1 for v in (1, 2, 4, 8)]

    def in_copy(m, k):
        start, rows = CHUNK1[k]
        dest = xor2(quad, m)
        src_row = pl.multiple_of((dest // 2) * hw + start, 32)
        return (
            y1.at[dest % 2, :, pl.ds(src_row, rows), :],
            units.at[quad, :, pl.ds(start, rows), :],
            in_send.at[m, k],
            in_recv.at[quad, k],
            in_peers[m],
        )

    def start_copy(parts, local):
        src, dst, send, recv, peer = parts

        def remote():
            pltpu.make_async_remote_copy(
                src_ref=src, dst_ref=dst, send_sem=send, recv_sem=recv, device_id=peer, device_id_type=MESH
            ).start()

        if local is None:
            remote()
        else:
            @pl.when(local)
            def _():
                pltpu.make_async_copy(src, dst, recv).start()

            @pl.when(jnp.logical_not(local))
            def _():
                remote()

    def wait_sent(parts, local):
        src, dst, send, recv, peer = parts

        def wait():
            pltpu.make_async_remote_copy(
                src_ref=src, dst_ref=dst, send_sem=send, recv_sem=recv, device_id=peer, device_id_type=MESH
            ).wait_send()

        if local is None:
            wait()
        else:
            @pl.when(jnp.logical_not(local))
            def _():
                wait()

    for k in range(2):
        start, rows = CHUNK1[k]
        for part in range(2):
            if k == 1 and part == 0:
                rows = hw - start
            else:
                rows = CHUNK1[k][1]
            for h in range(2):
                for ch in range(2):
                    at = part * hw + start
                    y1[h, ch, pl.ds(at, rows), :] = interpolate(
                        lambda o, n: x1[h, ch, pl.ds(at + o, n), :], rows, own_bits1, 1
                    )
        for m in range(4):
            start_copy(in_copy(m, k), self_in if m == 0 else None)

    fill_wide(1)
    fill_table(1)
    fill_wide(2)
    fill_table(2)
    for side in range(2):
        wr = weights[3, side, core, 0]
        wi = weights[3, side, core, 1]
        for c, x, value in ((0, 0, wr), (1, 0, -wi), (0, 1, wi), (1, 1, wr)):
            wide[3, pl.ds(x * 128, 128), pl.ds((side * 2 + c) * 128, 128)] = value
    a = lax.broadcasted_iota(jnp.int32, (ANGLES, 128), 0)
    r = lax.broadcasted_iota(jnp.int32, (ANGLES, 128), 1)
    phase = ((r * (core * ANGLES + a + 1) * (7 + 3)) % PERIOD).astype(F32) * PHASE_STEP
    cos_last[...] = jnp.cos(phase)
    sin_last[...] = jnp.sin(phase)

    bits2 = [bits_of(shift_row(2, side)) for side in range(2)]
    bits3 = bits_of(shift_row(3, core))
    at_start = jnp.logical_and(rng == 0, half == 0)
    at_end = jnp.logical_and(rng == last_rng, half == 1)

    def merge(level, lhs, start_row, rows, margin_rows, dst, slots):
        z = jnp.dot(lhs, wide[level], preferred_element_type=F32)
        start = (start_row - margin_rows) % PERIOD
        for h in range(2):
            re, im = turn(level, h, start, rows, z[:, h * 256 : h * 256 + 128], z[:, h * 256 + 128 : h * 256 + 256])
            dst[slots[h], 0, pl.ds(start_row, rows), :] = re
            dst[slots[h], 1, pl.ds(start_row, rows), :] = im

    def clear(dst, k, margin_rows):
        total = hw + 2 * margin_rows

        @pl.when(at_start if k == 0 else at_end)
        def _():
            at = 0 if k == 0 else total - margin_rows
            dst[:, :, pl.ds(at, margin_rows), :] = jnp.zeros((4, 2, margin_rows, ANGLES), F32)

    def pair_copy(k):
        start, rows = CHUNK3[k]
        ref = y3.at[core, :, :, pl.ds(start, rows), :]
        return pltpu.make_async_remote_copy(
            src_ref=ref, dst_ref=ref, send_sem=pair_send.at[k], recv_sem=pair_recv.at[k],
            device_id=partner, device_id_type=MESH,
        )

    def pair_wait(k):
        start, rows = CHUNK3[k]
        ref = y3.at[1 - core, :, :, pl.ds(start, rows), :]
        return pltpu.make_async_remote_copy(
            src_ref=ref, dst_ref=ref, send_sem=pair_send.at[k], recv_sem=pair_recv.at[k],
            device_id=partner, device_id_type=MESH,
        )

    def out_copy(m, k):
        start, rows = CHUNK3[k]
        dest = xor2(quad, m)
        col = pl.multiple_of(half * hw + start, 128)
        return (
            turned.at[dest, :, :, pl.ds(start, rows)],
            out.at[:, upper, :, pl.ds(col, rows)],
            out_send.at[m, k],
            out_recv.at[zl // 2, k],
            out_dests[m],
        )

    for k in range(2):
        start, rows = CHUNK1[k]
        for s in range(4):
            ref = units.at[s, :, pl.ds(start, rows), :]
            pltpu.make_async_remote_copy(
                src_ref=ref, dst_ref=ref, send_sem=in_send.at[0, k], recv_sem=in_recv.at[s, k],
                device_id=partner, device_id_type=MESH,
            ).wait_recv()
        for p in range(2):
            lhs = jnp.concatenate(
                [units[2 * p + side, ch, pl.ds(start, rows), :] for side in range(2) for ch in range(2)], axis=1
            )
            merge(1, lhs, start, rows, 2 * RIM, x2, (2 * p, 2 * p + 1))
        clear(x2, k, 2 * RIM)
        start, rows = CHUNK2[k]
        for p in range(2):
            lhs = jnp.concatenate(
                [
                    interpolate(lambda o, n: x2[p + 2 * side, ch, pl.ds(start + o, n), :], rows, bits2[side], 2)
                    for side in range(2)
                    for ch in range(2)
                ],
                axis=1,
            )
            merge(2, lhs, start, rows, RIM, x3, (p, p + 2))
        clear(x3, k, RIM)
        start, rows = CHUNK3[k]
        for s in range(4):
            for ch in range(2):
                y3[core, s, ch, pl.ds(start, rows), :] = interpolate(
                    lambda o, n: x3[s, ch, pl.ds(start + o, n), :], rows, bits3, 3
                )
        pair_copy(k).start()
        pair_wait(k).wait_recv()
        for s in range(4):
            rhs = jnp.concatenate(
                [y3[side, s, ch, pl.ds(start, rows), :] for side in range(2) for ch in range(2)], axis=1
            )
            z = lax.dot_general(
                wide[3, pl.ds(0, 256), :], rhs, (((1,), (1,)), ((), ())), preferred_element_type=F32
            )
            re, im = z[:128], z[128:]
            turned[s, 0, :, pl.ds(start, rows)] = (re * cos_last[...] - im * sin_last[...]).astype(BF16)
            turned[s, 1, :, pl.ds(start, rows)] = (re * sin_last[...] + im * cos_last[...]).astype(BF16)
        for m in range(4):
            start_copy(out_copy(m, k), self_out if m == 0 else None)

    to_core.wait_send()
    for j in range(2):
        @pl.when(rng > 0)
        def _():
            halo_copy(j, 0).wait_send()

        @pl.when(rng < last_rng)
        def _():
            halo_copy(j, 1).wait_send()

    for k in range(2):
        for m in range(4):
            wait_sent(in_copy(m, k), self_in if m == 0 else None)
        pair_copy(k).wait_send()
        for m in range(4):
            wait_sent(out_copy(m, k), self_out if m == 0 else None)
    for k in range(2):
        start, rows = CHUNK3[k]
        for s in range(4):
            pltpu.make_async_remote_copy(
                src_ref=turned.at[0, :, :, pl.ds(start, rows)],
                dst_ref=out.at[:, s // 2, :, pl.ds((s % 2) * hw + start, rows)],
                send_sem=out_send.at[0, k],
                recv_sem=out_recv.at[s, k],
                device_id=partner,
                device_id_type=MESH,
            ).wait_recv()


def on_device(image, interp_weights, range_taps, range_shifts):
    width = image.shape[3]
    hw = width // 2
    margin = LEVELS * RIM
    dma = pltpu.SemaphoreType.DMA
    vmem = pltpu.VMEM
    return pl.pallas_call(
        kernel,
        out_shape=jax.ShapeDtypeStruct(image.shape, image.dtype),
        in_specs=[
            pl.BlockSpec(memory_space=pl.ANY),
            pl.BlockSpec(memory_space=pl.ANY),
            pl.BlockSpec(memory_space=pltpu.SMEM),
            pl.BlockSpec(memory_space=pltpu.VMEM),
        ],
        out_specs=pl.BlockSpec(memory_space=pl.ANY),
        scratch_shapes=[
            vmem(image.shape, BF16),
            vmem(interp_weights.shape, BF16),
            vmem((LEVELS, 512, 512), BF16),
            vmem((3, 2, TABLE, ANGLES), F32),
            vmem((3, 2, TABLE, ANGLES), F32),
            vmem((ANGLES, 128), F32),
            vmem((ANGLES, 128), F32),
            vmem((2, 2, width, ANGLES), BF16),
            vmem((2, 2, width + 2 * margin + 16, ANGLES), F32),
            vmem((2, width, ANGLES), BF16),
            vmem((2, 2, 2, margin, ANGLES), BF16),
            vmem((2, 2, width + 6 * RIM + 16, ANGLES), F32),
            vmem((2, 2, width + 4 * RIM, ANGLES), BF16),
            vmem((4, 2, hw + 4 * RIM, ANGLES), BF16),
            vmem((4, 2, hw + 4 * RIM + 16, ANGLES), F32),
            vmem((4, 2, hw + 2 * RIM + 16, ANGLES), F32),
            vmem((2, 4, 2, hw, ANGLES), BF16),
            vmem((4, 2, ANGLES, hw), BF16),
            dma((2,)),
            dma((2,)),
            dma((2, 2)),
            dma((2, 2)),
            dma((4, 2)),
            dma((4, 2)),
            dma((2,)),
            dma((2,)),
            dma((4, 2)),
            dma((4, 2)),
        ],
        compiler_params=pltpu.CompilerParams(collective_id=0, has_side_effects=True),
        name="backprojection",
    )(image, interp_weights, range_taps, range_shifts)


def solution(mesh):
    return jax.shard_map(
        on_device,
        mesh=mesh,
        in_specs=(P(None, ("img", "sub"), None, "rng"), P(), P(), P()),
        out_specs=P(None, ("img", "sub"), None, "rng"),
        check_vma=False,
    )
```

```python
import math

import jax
import jax.numpy as jnp
from jax import lax
from jax.experimental import pallas as pl
from jax.experimental.pallas import tpu as pltpu
from jax.sharding import PartitionSpec as P

ANGLES = 128
RIM = 8
TAPS = 4
LEVELS = 4
PERIOD = 64
PHASE_STEP = 2.0 * math.pi / PERIOD

MESH = pl.DeviceIdType.MESH
F32 = jnp.float32
BF16 = jnp.bfloat16

CHUNK1 = ((0, 160), (160, 128))
CHUNK2 = ((0, 144), (144, 128))
CHUNK3 = ((0, 128), (128, 128))
ROWS0 = (((0, 176), (256, 176)), ((176, 80), (432, 128)))
TABLE = 256


def kernel(
    image_hbm, weights_hbm, taps, shifts, out,
    image, weights, wide, cos_t, sin_t, cos_last, sin_last,
    rows_bf, first, from_core, halo, x1, y1, units, x2, x3, y3, turned,
    load_sem, core_sem, halo_send, halo_recv, in_send, in_recv, pair_send, pair_recv, out_send, out_recv,
    ready_core, ready_rng, ready_in, ready_out,
):
    sub = lax.axis_index("sub")
    rng = lax.axis_index("rng")
    last_rng = lax.axis_size("rng") - 1
    core = sub % 2
    z = sub // 2
    zl = z % 8
    base = z - zl
    quad = zl % 4
    upper = zl // 4
    half = (zl // 2) % 2
    side0 = zl % 2
    width = image.shape[3]
    hw = width // 2

    load_image = pltpu.make_async_copy(image_hbm, image, load_sem.at[0])
    load_weights = pltpu.make_async_copy(weights_hbm, weights, load_sem.at[1])
    load_image.start()
    load_weights.start()

    def device(z_local, core_index):
        return {"sub": (base + z_local) * 2 + core_index}

    def order(z_local, core_index):
        return ((z_local + 7) % 8) * 2 + (1 - core_index)

    me = order(zl, core)
    partner = {"sub": z * 2 + (1 - core)}
    in_chips = [4 * core + q for q in range(4)]
    in_self = [jnp.logical_and(upper == core, quad == q) for q in range(4)]
    in_peers = [device(chip, upper) for chip in in_chips]
    in_later = [order(chip, upper) > me for chip in in_chips]
    out_self = [jnp.logical_and(in_self[q], side0 == core) for q in range(4)]
    out_dests = [device(chip, side0) for chip in in_chips]
    out_later = [order(chip, side0) > me for chip in in_chips]
    source_chips = [2 * k + core for k in range(4)]
    source_self = [jnp.logical_and(zl == source_chips[k], upper == core) for k in range(4)]
    out_sources = [device(chip, upper) for chip in source_chips]
    source_later = [order(chip, upper) > me for chip in source_chips]
    lower_rng, upper_rng = rng > 0, rng < last_rng

    barrier = pltpu.get_barrier_semaphore()

    def greet(who):
        pl.semaphore_signal(barrier, inc=1, device_id=who, device_id_type=MESH)

    def answer(sem, who):
        pl.semaphore_signal(sem, inc=1, device_id=who, device_id_type=MESH)

    def earlier(later, own):
        return jnp.logical_not(jnp.logical_or(later, own))

    @pl.when(core == 1)
    def _():
        greet(partner)

    @pl.when(lower_rng)
    def _():
        for c in range(2):
            greet({"sub": z * 2 + c, "rng": rng - 1})

    for peers, later in ((in_peers, in_later), (out_dests, out_later), (out_sources, source_later)):
        for q in range(4):
            @pl.when(later[q])
            def _():
                greet(peers[q])

    count = jnp.where(core == 0, 1, 0) + jnp.where(upper_rng, 2, 0)
    for later, own in ((in_later, in_self), (out_later, out_self), (source_later, source_self)):
        for q in range(4):
            count = count + jnp.where(earlier(later[q], own[q]), 1, 0)
    pl.when(count > 0)(lambda: pl.semaphore_wait(barrier, count))

    @pl.when(upper_rng)
    def _():
        for c in range(2):
            answer(ready_rng.at[core], {"sub": z * 2 + c, "rng": rng + 1})

    @pl.when(core == 0)
    def _():
        answer(ready_core, partner)

    for q in range(4):
        @pl.when(earlier(in_later[q], in_self[q]))
        def _():
            answer(ready_in.at[quad], in_peers[q])

        @pl.when(earlier(source_later[q], source_self[q]))
        def _():
            answer(ready_out.at[quad], out_sources[q])

    def fill_table(level):
        r = lax.broadcasted_iota(jnp.int32, (PERIOD, ANGLES), 0)
        a = lax.broadcasted_iota(jnp.int32, (PERIOD, ANGLES), 1)
        for h in range(2):
            phase = ((r * (h * ANGLES + a + 1) * (7 + level)) % PERIOD).astype(F32) * PHASE_STEP
            c, s = jnp.cos(phase), jnp.sin(phase)
            for i in range(TABLE // PERIOD):
                cos_t[level, h, pl.ds(i * PERIOD, PERIOD), :] = c
                sin_t[level, h, pl.ds(i * PERIOD, PERIOD), :] = s

    load_image.wait()

    for ch in range(2):
        for j in range(2):
            for k in range(width // 128):
                block = image[ch, j, :, pl.ds(k * 128, 128)].astype(F32).T
                rows_bf[j, ch, pl.ds(k * 128, 128), :] = block.astype(BF16)

    def fill_wide(level):
        for side in range(2):
            for h in range(2):
                wr = weights[level, side, h, 0].astype(F32).T.astype(BF16)
                wi = weights[level, side, h, 1].astype(F32).T.astype(BF16)
                for c, x, value in ((0, 0, wr), (1, 0, -wi), (0, 1, wi), (1, 1, wr)):
                    wide[level, pl.ds((side * 2 + c) * 128, 128), pl.ds((h * 2 + x) * 128, 128)] = value

    to_core = pltpu.make_async_remote_copy(
        src_ref=rows_bf.at[1 - core],
        dst_ref=from_core,
        send_sem=core_sem.at[0],
        recv_sem=core_sem.at[1],
        device_id=partner,
        device_id_type=MESH,
    )
    margin = LEVELS * RIM

    def halo_copy(j, lr):
        start = 0 if lr == 0 else width - margin
        return pltpu.make_async_remote_copy(
            src_ref=rows_bf.at[j, :, pl.ds(start, margin), :],
            dst_ref=halo.at[core, lr],
            send_sem=halo_send.at[j, lr],
            recv_sem=halo_recv.at[core, lr],
            device_id={"sub": z * 2 + j, "rng": rng - 1 + 2 * lr},
            device_id_type=MESH,
        )

    def halo_wait(side, lr):
        return pltpu.make_async_remote_copy(
            src_ref=rows_bf.at[0, :, pl.ds(0, margin), :],
            dst_ref=halo.at[side, lr],
            send_sem=halo_send.at[0, lr],
            recv_sem=halo_recv.at[side, lr],
            device_id=partner,
            device_id_type=MESH,
        )

    @pl.when(core == 1)
    def _():
        pl.semaphore_wait(ready_core, 1)

    to_core.start()

    @pl.when(upper_rng)
    def _():
        for j in range(2):
            halo_copy(j, 1).start()

    load_weights.wait()
    fill_wide(0)
    fill_table(0)

    @pl.when(lower_rng)
    def _():
        for j in range(2):
            pl.semaphore_wait(ready_rng.at[j], 1)
            halo_copy(j, 0).start()

    for ch in range(2):
        first[core, ch, pl.ds(margin, width), :] = rows_bf[core, ch].astype(F32)
    to_core.wait_recv()
    for ch in range(2):
        first[1 - core, ch, pl.ds(margin, width), :] = from_core[ch].astype(F32)

    for lr, start, there in ((1, 0, lower_rng), (0, margin + width, upper_rng)):
        @pl.when(there)
        def _():
            for side in range(2):
                halo_wait(side, lr).wait_recv()
                for ch in range(2):
                    first[side, ch, pl.ds(start, margin), :] = halo[side, lr, ch].astype(F32)

        @pl.when(jnp.logical_not(there))
        def _():
            first[:, :, pl.ds(start, margin), :] = jnp.zeros((2, 2, margin, ANGLES), F32)

    def bits_of(row):
        code = row + RIM
        return [((code // v) % 2) == 1 for v in (1, 2, 4, 8)]

    def shift_row(level, side):
        return shifts[level, pl.ds(side, 1), :]

    def interpolate(load, rows, bits, level):
        n = rows + 8
        b0, b1, b2, b3 = bits
        v = jnp.where(
            b3,
            jnp.where(b2, load(12, n), load(8, n)),
            jnp.where(b2, load(4, n), load(0, n)),
        )
        v = jnp.where(b0, pltpu.roll(v, n - 1, 0), v)
        v = jnp.where(b1, pltpu.roll(v, n - 2, 0), v)
        total = v * taps[level, 0]
        for t in range(1, TAPS):
            total = total + pltpu.roll(v, n - t, 0) * taps[level, t]
        return total[:rows].astype(BF16)

    def turn(level, h, start, rows, re, im):
        c = cos_t[level, h, pl.ds(start, rows), :]
        s = sin_t[level, h, pl.ds(start, rows), :]
        return re * c - im * s, re * s + im * c

    bits0 = [bits_of(shift_row(0, side)) for side in range(2)]
    rows1 = width + 2 * (margin - RIM)

    def level0(b, rows):
        parts = []
        for side in range(2):
            for ch in range(2):
                parts.append(interpolate(lambda o, n: first[side, ch, pl.ds(b + o, n), :], rows, bits0[side], 0))
        merged = jnp.dot(jnp.concatenate(parts, axis=1), wide[0], preferred_element_type=F32)
        start = (b - (margin - RIM)) % PERIOD
        for h in range(2):
            re, im = merged[:, h * 256 : h * 256 + 128], merged[:, h * 256 + 128 : h * 256 + 256]
            re, im = turn(0, h, start, rows, re, im)
            x1[h, 0, pl.ds(b, rows), :] = re
            x1[h, 1, pl.ds(b, rows), :] = im

    def clear1(start):
        x1[:, :, pl.ds(start, margin - RIM), :] = jnp.zeros((2, 2, margin - RIM, ANGLES), F32)

    own_bits1 = [((shift_row(1, side0) + RIM) // v) % 2 == 1 for v in (1, 2, 4, 8)]

    def in_copy(q, k):
        start, rows = CHUNK1[k]
        return (
            y1.at[q % 2, :, pl.ds((q // 2) * hw + start, rows), :],
            units.at[quad, :, pl.ds(start, rows), :],
            in_send.at[q, k],
            in_recv.at[quad, k],
            in_peers[q],
        )

    def remote(src, dst, send, recv, peer):
        return pltpu.make_async_remote_copy(
            src_ref=src, dst_ref=dst, send_sem=send, recv_sem=recv, device_id=peer, device_id_type=MESH
        )

    def start_copy(parts, local):
        src, dst, send, recv, peer = parts

        @pl.when(local)
        def _():
            pltpu.make_async_copy(src, dst, recv).start()

        @pl.when(jnp.logical_not(local))
        def _():
            remote(*parts).start()

    def wait_sent(parts, local):
        @pl.when(jnp.logical_not(local))
        def _():
            remote(*parts).wait_send()

    for k in range(2):
        for b, rows in ROWS0[k]:
            level0(b, rows)
        if k == 0:
            pl.when(jnp.logical_not(lower_rng))(lambda: clear1(0))
        else:
            pl.when(jnp.logical_not(upper_rng))(lambda: clear1(rows1 - (margin - RIM)))
        start = CHUNK1[k][0]
        for part in range(2):
            if k == 1 and part == 0:
                rows = hw - start
            else:
                rows = CHUNK1[k][1]
            for h in range(2):
                for ch in range(2):
                    at = part * hw + start
                    y1[h, ch, pl.ds(at, rows), :] = interpolate(
                        lambda o, n: x1[h, ch, pl.ds(at + o, n), :], rows, own_bits1, 1
                    )
        for q in (3, 2, 1, 0):
            if k == 0:
                pl.when(in_later[q])(lambda: pl.semaphore_wait(ready_in.at[q], 1))
            start_copy(in_copy(q, k), in_self[q])

    fill_wide(1)
    fill_table(1)
    fill_wide(2)
    fill_table(2)
    for side in range(2):
        wr = weights[3, side, core, 0]
        wi = weights[3, side, core, 1]
        for c, x, value in ((0, 0, wr), (1, 0, -wi), (0, 1, wi), (1, 1, wr)):
            wide[3, pl.ds(x * 128, 128), pl.ds((side * 2 + c) * 128, 128)] = value
    a = lax.broadcasted_iota(jnp.int32, (ANGLES, 128), 0)
    r = lax.broadcasted_iota(jnp.int32, (ANGLES, 128), 1)
    phase = ((r * (core * ANGLES + a + 1) * (7 + 3)) % PERIOD).astype(F32) * PHASE_STEP
    cos_last[...] = jnp.cos(phase)
    sin_last[...] = jnp.sin(phase)

    bits2 = [bits_of(shift_row(2, side)) for side in range(2)]
    bits3 = bits_of(shift_row(3, core))
    at_start = jnp.logical_and(rng == 0, half == 0)
    at_end = jnp.logical_and(rng == last_rng, half == 1)

    def merge(level, lhs, start_row, rows, margin_rows, dst, slots):
        z = jnp.dot(lhs, wide[level], preferred_element_type=F32)
        start = (start_row - margin_rows) % PERIOD
        for h in range(2):
            re, im = turn(level, h, start, rows, z[:, h * 256 : h * 256 + 128], z[:, h * 256 + 128 : h * 256 + 256])
            dst[slots[h], 0, pl.ds(start_row, rows), :] = re
            dst[slots[h], 1, pl.ds(start_row, rows), :] = im

    def clear(dst, k, margin_rows):
        total = hw + 2 * margin_rows

        @pl.when(at_start if k == 0 else at_end)
        def _():
            at = 0 if k == 0 else total - margin_rows
            dst[:, :, pl.ds(at, margin_rows), :] = jnp.zeros((4, 2, margin_rows, ANGLES), F32)

    def pair_copy(k):
        start, rows = CHUNK3[k]
        ref = y3.at[core, :, :, pl.ds(start, rows), :]
        return pltpu.make_async_remote_copy(
            src_ref=ref, dst_ref=ref, send_sem=pair_send.at[k], recv_sem=pair_recv.at[k],
            device_id=partner, device_id_type=MESH,
        )

    def pair_wait(k):
        start, rows = CHUNK3[k]
        ref = y3.at[1 - core, :, :, pl.ds(start, rows), :]
        return pltpu.make_async_remote_copy(
            src_ref=ref, dst_ref=ref, send_sem=pair_send.at[k], recv_sem=pair_recv.at[k],
            device_id=partner, device_id_type=MESH,
        )

    def out_copy(q, k):
        start, rows = CHUNK3[k]
        col = pl.multiple_of(half * hw + start, 128)
        return (
            turned.at[q, :, :, pl.ds(start, rows)],
            out.at[:, upper, :, pl.ds(col, rows)],
            out_send.at[q, k],
            out_recv.at[zl // 2, k],
            out_dests[q],
        )

    for k in range(2):
        start, rows = CHUNK1[k]
        for s in range(4):
            ref = units.at[s, :, pl.ds(start, rows), :]
            pltpu.make_async_remote_copy(
                src_ref=ref, dst_ref=ref, send_sem=in_send.at[0, k], recv_sem=in_recv.at[s, k],
                device_id=partner, device_id_type=MESH,
            ).wait_recv()
        for p in range(2):
            lhs = jnp.concatenate(
                [units[2 * p + side, ch, pl.ds(start, rows), :] for side in range(2) for ch in range(2)], axis=1
            )
            merge(1, lhs, start, rows, 2 * RIM, x2, (2 * p, 2 * p + 1))
        clear(x2, k, 2 * RIM)
        start, rows = CHUNK2[k]
        for p in range(2):
            lhs = jnp.concatenate(
                [
                    interpolate(lambda o, n: x2[p + 2 * side, ch, pl.ds(start + o, n), :], rows, bits2[side], 2)
                    for side in range(2)
                    for ch in range(2)
                ],
                axis=1,
            )
            merge(2, lhs, start, rows, RIM, x3, (p, p + 2))
        clear(x3, k, RIM)
        start, rows = CHUNK3[k]
        for s in range(4):
            for ch in range(2):
                y3[core, s, ch, pl.ds(start, rows), :] = interpolate(
                    lambda o, n: x3[s, ch, pl.ds(start + o, n), :], rows, bits3, 3
                )
        pair_copy(k).start()
        pair_wait(k).wait_recv()
        for s in range(4):
            rhs = jnp.concatenate(
                [y3[side, s, ch, pl.ds(start, rows), :] for side in range(2) for ch in range(2)], axis=1
            )
            z = lax.dot_general(
                wide[3, pl.ds(0, 256), :], rhs, (((1,), (1,)), ((), ())), preferred_element_type=F32
            )
            re, im = z[:128], z[128:]
            turned[s, 0, :, pl.ds(start, rows)] = (re * cos_last[...] - im * sin_last[...]).astype(BF16)
            turned[s, 1, :, pl.ds(start, rows)] = (re * sin_last[...] + im * cos_last[...]).astype(BF16)
        for q in (3, 2, 1, 0):
            if k == 0:
                pl.when(out_later[q])(lambda: pl.semaphore_wait(ready_out.at[q], 1))
            start_copy(out_copy(q, k), out_self[q])

    to_core.wait_send()
    for j in range(2):
        @pl.when(lower_rng)
        def _():
            halo_copy(j, 0).wait_send()

        @pl.when(upper_rng)
        def _():
            halo_copy(j, 1).wait_send()

    for k in range(2):
        for q in range(4):
            wait_sent(in_copy(q, k), in_self[q])
        pair_copy(k).wait_send()
        for q in range(4):
            wait_sent(out_copy(q, k), out_self[q])
    for k in range(2):
        start, rows = CHUNK3[k]
        for s in range(4):
            pltpu.make_async_remote_copy(
                src_ref=turned.at[0, :, :, pl.ds(start, rows)],
                dst_ref=out.at[:, s // 2, :, pl.ds((s % 2) * hw + start, rows)],
                send_sem=out_send.at[0, k],
                recv_sem=out_recv.at[s, k],
                device_id=partner,
                device_id_type=MESH,
            ).wait_recv()


def on_device(image, interp_weights, range_taps, range_shifts):
    width = image.shape[3]
    hw = width // 2
    margin = LEVELS * RIM
    dma = pltpu.SemaphoreType.DMA
    vmem = pltpu.VMEM
    return pl.pallas_call(
        kernel,
        out_shape=jax.ShapeDtypeStruct(image.shape, image.dtype),
        in_specs=[
            pl.BlockSpec(memory_space=pl.ANY),
            pl.BlockSpec(memory_space=pl.ANY),
            pl.BlockSpec(memory_space=pltpu.SMEM),
            pl.BlockSpec(memory_space=pltpu.VMEM),
        ],
        out_specs=pl.BlockSpec(memory_space=pl.ANY),
        scratch_shapes=[
            vmem(image.shape, BF16),
            vmem(interp_weights.shape, BF16),
            vmem((LEVELS, 512, 512), BF16),
            vmem((3, 2, TABLE, ANGLES), F32),
            vmem((3, 2, TABLE, ANGLES), F32),
            vmem((ANGLES, 128), F32),
            vmem((ANGLES, 128), F32),
            vmem((2, 2, width, ANGLES), BF16),
            vmem((2, 2, width + 2 * margin + 16, ANGLES), F32),
            vmem((2, width, ANGLES), BF16),
            vmem((2, 2, 2, margin, ANGLES), BF16),
            vmem((2, 2, width + 6 * RIM + 16, ANGLES), F32),
            vmem((2, 2, width + 4 * RIM, ANGLES), BF16),
            vmem((4, 2, hw + 4 * RIM, ANGLES), BF16),
            vmem((4, 2, hw + 4 * RIM + 16, ANGLES), F32),
            vmem((4, 2, hw + 2 * RIM + 16, ANGLES), F32),
            vmem((2, 4, 2, hw, ANGLES), BF16),
            vmem((4, 2, ANGLES, hw), BF16),
            dma((2,)),
            dma((2,)),
            dma((2, 2)),
            dma((2, 2)),
            dma((4, 2)),
            dma((4, 2)),
            dma((2,)),
            dma((2,)),
            dma((4, 2)),
            dma((4, 2)),
            pltpu.SemaphoreType.REGULAR,
            pltpu.SemaphoreType.REGULAR((2,)),
            pltpu.SemaphoreType.REGULAR((4,)),
            pltpu.SemaphoreType.REGULAR((4,)),
        ],
        compiler_params=pltpu.CompilerParams(collective_id=0, has_side_effects=True),
        name="backprojection",
    )(image, interp_weights, range_taps, range_shifts)


def solution(mesh):
    return jax.shard_map(
        on_device,
        mesh=mesh,
        in_specs=(P(None, ("img", "sub"), None, "rng"), P(), P(), P()),
        out_specs=P(None, ("img", "sub"), None, "rng"),
        check_vma=False,
    )
```

```python
import math

import jax
import jax.numpy as jnp
from jax import lax
from jax.experimental import pallas as pl
from jax.experimental.pallas import tpu as pltpu
from jax.sharding import PartitionSpec as P

ANGLES = 128
RIM = 8
TAPS = 4
LEVELS = 4
PERIOD = 64
PHASE_STEP = 2.0 * math.pi / PERIOD

MESH = pl.DeviceIdType.MESH
F32 = jnp.float32
BF16 = jnp.bfloat16

CHUNK1 = ((0, 160), (160, 128))
CHUNK2 = ((0, 144), (144, 128))
CHUNK3 = ((0, 128), (128, 128))
ROWS0 = (((256, 176), (0, 176)), ((176, 80), (432, 128)))
TABLE = 256


def kernel(
    image_hbm, weights_hbm, taps_hbm, shifts_hbm, out,
    image, weights, taps, shifts, wide, cos_t, sin_t, cos_last, sin_last,
    rows_bf, first, from_core, halo, x1, y1, units, x2, x3, y3, turned,
    load_sem, core_sem, halo_send, halo_recv, in_send, in_recv, pair_send, pair_recv, out_send, out_recv,
    ready_core, ready_rng, ready_in, ready_out,
):
    sub = lax.axis_index("sub")
    rng = lax.axis_index("rng")
    last_rng = lax.axis_size("rng") - 1
    core = sub % 2
    z = sub // 2
    zl = z % 8
    base = z - zl
    quad = zl % 4
    upper = zl // 4
    half = (zl // 2) % 2
    side0 = zl % 2
    width = image.shape[3]
    hw = width // 2

    load_image = pltpu.make_async_copy(image_hbm, image, load_sem.at[0])
    load_weights = pltpu.make_async_copy(weights_hbm, weights, load_sem.at[1])
    load_taps = pltpu.make_async_copy(taps_hbm, taps, load_sem.at[2])
    load_shifts = pltpu.make_async_copy(shifts_hbm, shifts, load_sem.at[3])
    load_image.start()
    load_weights.start()
    load_taps.start()
    load_shifts.start()

    def device(z_local, core_index):
        return {"sub": (base + z_local) * 2 + core_index}

    def order(z_local, core_index):
        return jnp.where(z_local * 2 + core_index == 0, 16, z_local * 2 + (1 - core_index))

    me = order(zl, core)
    partner = {"sub": z * 2 + (1 - core)}
    in_chips = [4 * core + q for q in range(4)]
    in_self = [jnp.logical_and(upper == core, quad == q) for q in range(4)]
    in_peers = [device(chip, upper) for chip in in_chips]
    in_later = [order(chip, upper) > me for chip in in_chips]
    out_self = [jnp.logical_and(in_self[q], side0 == core) for q in range(4)]
    out_dests = [device(chip, side0) for chip in in_chips]
    out_later = [order(chip, side0) > me for chip in in_chips]
    source_chips = [2 * k + core for k in range(4)]
    source_self = [jnp.logical_and(zl == source_chips[k], upper == core) for k in range(4)]
    out_sources = [device(chip, upper) for chip in source_chips]
    source_later = [order(chip, upper) > me for chip in source_chips]
    lower_rng, upper_rng = rng > 0, rng < last_rng

    barrier = pltpu.get_barrier_semaphore()

    def greet(who):
        pl.semaphore_signal(barrier, inc=1, device_id=who, device_id_type=MESH)

    def answer(sem, who):
        pl.semaphore_signal(sem, inc=1, device_id=who, device_id_type=MESH)

    def earlier(later, own):
        return jnp.logical_not(jnp.logical_or(later, own))

    @pl.when(core == 1)
    def _():
        greet(partner)

    @pl.when(lower_rng)
    def _():
        for c in range(2):
            greet({"sub": z * 2 + c, "rng": rng - 1})

    for peers, later in ((in_peers, in_later), (out_dests, out_later), (out_sources, source_later)):
        for q in range(4):
            @pl.when(later[q])
            def _():
                greet(peers[q])

    count = jnp.where(core == 0, 1, 0) + jnp.where(upper_rng, 2, 0)
    for later, own in ((in_later, in_self), (out_later, out_self), (source_later, source_self)):
        for q in range(4):
            count = count + jnp.where(earlier(later[q], own[q]), 1, 0)
    pl.when(count > 0)(lambda: pl.semaphore_wait(barrier, count))

    @pl.when(upper_rng)
    def _():
        for c in range(2):
            answer(ready_rng.at[core], {"sub": z * 2 + c, "rng": rng + 1})

    @pl.when(core == 0)
    def _():
        answer(ready_core, partner)

    for q in range(4):
        @pl.when(earlier(in_later[q], in_self[q]))
        def _():
            answer(ready_in.at[quad], in_peers[q])

        @pl.when(earlier(source_later[q], source_self[q]))
        def _():
            answer(ready_out.at[quad], out_sources[q])

    def fill_table(level):
        r = lax.broadcasted_iota(jnp.int32, (PERIOD, ANGLES), 0)
        a = lax.broadcasted_iota(jnp.int32, (PERIOD, ANGLES), 1)
        for h in range(2):
            phase = ((r * (h * ANGLES + a + 1) * (7 + level)) % PERIOD).astype(F32) * PHASE_STEP
            c, s = jnp.cos(phase), jnp.sin(phase)
            for i in range(TABLE // PERIOD):
                cos_t[level, h, pl.ds(i * PERIOD, PERIOD), :] = c
                sin_t[level, h, pl.ds(i * PERIOD, PERIOD), :] = s

    load_image.wait()

    for ch in range(2):
        for j in range(2):
            for k in range(width // 128):
                block = image[ch, j, :, pl.ds(k * 128, 128)].astype(F32).T
                rows_bf[j, ch, pl.ds(k * 128, 128), :] = block.astype(BF16)

    def fill_wide(level):
        for side in range(2):
            for h in range(2):
                wr = weights[level, side, h, 0].astype(F32).T.astype(BF16)
                wi = weights[level, side, h, 1].astype(F32).T.astype(BF16)
                for c, x, value in ((0, 0, wr), (1, 0, -wi), (0, 1, wi), (1, 1, wr)):
                    wide[level, pl.ds((side * 2 + c) * 128, 128), pl.ds((h * 2 + x) * 128, 128)] = value

    to_core = pltpu.make_async_remote_copy(
        src_ref=rows_bf.at[1 - core],
        dst_ref=from_core,
        send_sem=core_sem.at[0],
        recv_sem=core_sem.at[1],
        device_id=partner,
        device_id_type=MESH,
    )
    margin = LEVELS * RIM

    def halo_copy(j, lr):
        start = 0 if lr == 0 else width - margin
        return pltpu.make_async_remote_copy(
            src_ref=rows_bf.at[j, :, pl.ds(start, margin), :],
            dst_ref=halo.at[core, lr],
            send_sem=halo_send.at[j, lr],
            recv_sem=halo_recv.at[core, lr],
            device_id={"sub": z * 2 + j, "rng": rng - 1 + 2 * lr},
            device_id_type=MESH,
        )

    def halo_wait(side, lr):
        return pltpu.make_async_remote_copy(
            src_ref=rows_bf.at[0, :, pl.ds(0, margin), :],
            dst_ref=halo.at[side, lr],
            send_sem=halo_send.at[0, lr],
            recv_sem=halo_recv.at[side, lr],
            device_id=partner,
            device_id_type=MESH,
        )

    @pl.when(core == 1)
    def _():
        pl.semaphore_wait(ready_core, 1)

    to_core.start()

    @pl.when(upper_rng)
    def _():
        for j in range(2):
            halo_copy(j, 1).start()

    load_taps.wait()
    load_shifts.wait()
    load_weights.wait()
    fill_wide(0)
    fill_table(0)

    @pl.when(lower_rng)
    def _():
        for j in range(2):
            pl.semaphore_wait(ready_rng.at[j], 1)
            halo_copy(j, 0).start()

    for ch in range(2):
        first[core, ch, pl.ds(margin, width), :] = rows_bf[core, ch].astype(F32)
    to_core.wait_recv()
    for ch in range(2):
        first[1 - core, ch, pl.ds(margin, width), :] = from_core[ch].astype(F32)

    def take_halo(lr):
        start, there = ((margin + width, upper_rng), (0, lower_rng))[lr]

        @pl.when(there)
        def _():
            for side in range(2):
                halo_wait(side, lr).wait_recv()
                for ch in range(2):
                    first[side, ch, pl.ds(start, margin), :] = halo[side, lr, ch].astype(F32)

        @pl.when(jnp.logical_not(there))
        def _():
            first[:, :, pl.ds(start, margin), :] = jnp.zeros((2, 2, margin, ANGLES), F32)

    def bits_of(row):
        code = row + RIM
        return [((code // v) % 2) == 1 for v in (1, 2, 4, 8)]

    def shift_row(level, side):
        return shifts[level, pl.ds(side, 1), :]

    def interpolate(load, rows, bits, level):
        n = rows + 8
        b0, b1, b2, b3 = bits
        v = jnp.where(
            b3,
            jnp.where(b2, load(12, n), load(8, n)),
            jnp.where(b2, load(4, n), load(0, n)),
        )
        v = jnp.where(b0, pltpu.roll(v, n - 1, 0), v)
        v = jnp.where(b1, pltpu.roll(v, n - 2, 0), v)
        total = v * taps[level, 0]
        for t in range(1, TAPS):
            total = total + pltpu.roll(v, n - t, 0) * taps[level, t]
        return total[:rows].astype(BF16)

    def turn(level, h, start, rows, re, im):
        c = cos_t[level, h, pl.ds(start, rows), :]
        s = sin_t[level, h, pl.ds(start, rows), :]
        return re * c - im * s, re * s + im * c

    bits0 = [bits_of(shift_row(0, side)) for side in range(2)]
    rows1 = width + 2 * (margin - RIM)

    def level0(b, rows):
        parts = []
        for side in range(2):
            for ch in range(2):
                parts.append(interpolate(lambda o, n: first[side, ch, pl.ds(b + o, n), :], rows, bits0[side], 0))
        merged = jnp.dot(jnp.concatenate(parts, axis=1), wide[0], preferred_element_type=F32)
        start = (b - (margin - RIM)) % PERIOD
        for h in range(2):
            re, im = merged[:, h * 256 : h * 256 + 128], merged[:, h * 256 + 128 : h * 256 + 256]
            re, im = turn(0, h, start, rows, re, im)
            x1[h, 0, pl.ds(b, rows), :] = re
            x1[h, 1, pl.ds(b, rows), :] = im

    def clear1(start):
        x1[:, :, pl.ds(start, margin - RIM), :] = jnp.zeros((2, 2, margin - RIM, ANGLES), F32)

    own_bits1 = [((shift_row(1, side0) + RIM) // v) % 2 == 1 for v in (1, 2, 4, 8)]

    def nth(i):
        q = jnp.where(jnp.logical_and(core == 1, zl > 0), i, 3 - i)
        chip = 4 * core + q
        own = jnp.logical_and(upper == core, quad == q)
        return q, own, device(chip, upper), order(chip, upper) > me

    def in_copy(i, k):
        start, rows = CHUNK1[k]
        q, own, peer, later = nth(i)
        row = pl.multiple_of((q // 2) * hw + start, 32)
        return (
            y1.at[q % 2, :, pl.ds(row, rows), :],
            units.at[quad, :, pl.ds(start, rows), :],
            in_send.at[i, k],
            in_recv.at[quad, k],
            peer,
        )

    def send_unit(i, k):
        q, own, peer, later = nth(i)
        if k == 0:
            pl.when(later)(lambda: pl.semaphore_wait(ready_in.at[q], 1))
        start_copy(in_copy(i, k), own)

    def remote(src, dst, send, recv, peer):
        return pltpu.make_async_remote_copy(
            src_ref=src, dst_ref=dst, send_sem=send, recv_sem=recv, device_id=peer, device_id_type=MESH
        )

    def start_copy(parts, local):
        src, dst, send, recv, peer = parts

        @pl.when(local)
        def _():
            pltpu.make_async_copy(src, dst, recv).start()

        @pl.when(jnp.logical_not(local))
        def _():
            remote(*parts).start()

    def wait_sent(parts, local):
        @pl.when(jnp.logical_not(local))
        def _():
            remote(*parts).wait_send()

    for k in range(2):
        level0(*ROWS0[k][0])
        take_halo(1 - k)
        level0(*ROWS0[k][1])
        if k == 0:
            pl.when(jnp.logical_not(lower_rng))(lambda: clear1(0))
        else:
            pl.when(jnp.logical_not(upper_rng))(lambda: clear1(rows1 - (margin - RIM)))
        start = CHUNK1[k][0]
        for part in range(2):
            if k == 1 and part == 0:
                rows = hw - start
            else:
                rows = CHUNK1[k][1]
            for h in range(2):
                for ch in range(2):
                    at = part * hw + start
                    y1[h, ch, pl.ds(at, rows), :] = interpolate(
                        lambda o, n: x1[h, ch, pl.ds(at + o, n), :], rows, own_bits1, 1
                    )
        for i in range(3):
            send_unit(i, k)
        if k == 0:
            pl.when(zl == 0)(lambda: send_unit(3, 0))
        else:
            pl.when(zl > 0)(lambda: send_unit(3, 0))
            send_unit(3, 1)

    fill_wide(1)
    fill_table(1)
    fill_wide(2)
    fill_table(2)
    for side in range(2):
        wr = weights[3, side, core, 0]
        wi = weights[3, side, core, 1]
        for c, x, value in ((0, 0, wr), (1, 0, -wi), (0, 1, wi), (1, 1, wr)):
            wide[3, pl.ds(x * 128, 128), pl.ds((side * 2 + c) * 128, 128)] = value
    a = lax.broadcasted_iota(jnp.int32, (ANGLES, 128), 0)
    r = lax.broadcasted_iota(jnp.int32, (ANGLES, 128), 1)
    phase = ((r * (core * ANGLES + a + 1) * (7 + 3)) % PERIOD).astype(F32) * PHASE_STEP
    cos_last[...] = jnp.cos(phase)
    sin_last[...] = jnp.sin(phase)

    bits2 = [bits_of(shift_row(2, side)) for side in range(2)]
    bits3 = bits_of(shift_row(3, core))
    at_start = jnp.logical_and(rng == 0, half == 0)
    at_end = jnp.logical_and(rng == last_rng, half == 1)

    def merge(level, lhs, start_row, rows, margin_rows, dst, slots):
        z = jnp.dot(lhs, wide[level], preferred_element_type=F32)
        start = (start_row - margin_rows) % PERIOD
        for h in range(2):
            re, im = turn(level, h, start, rows, z[:, h * 256 : h * 256 + 128], z[:, h * 256 + 128 : h * 256 + 256])
            dst[slots[h], 0, pl.ds(start_row, rows), :] = re
            dst[slots[h], 1, pl.ds(start_row, rows), :] = im

    def clear(dst, k, margin_rows):
        total = hw + 2 * margin_rows

        @pl.when(at_start if k == 0 else at_end)
        def _():
            at = 0 if k == 0 else total - margin_rows
            dst[:, :, pl.ds(at, margin_rows), :] = jnp.zeros((4, 2, margin_rows, ANGLES), F32)

    def pair_copy(k):
        start, rows = CHUNK3[k]
        ref = y3.at[core, :, :, pl.ds(start, rows), :]
        return pltpu.make_async_remote_copy(
            src_ref=ref, dst_ref=ref, send_sem=pair_send.at[k], recv_sem=pair_recv.at[k],
            device_id=partner, device_id_type=MESH,
        )

    def pair_wait(k):
        start, rows = CHUNK3[k]
        ref = y3.at[1 - core, :, :, pl.ds(start, rows), :]
        return pltpu.make_async_remote_copy(
            src_ref=ref, dst_ref=ref, send_sem=pair_send.at[k], recv_sem=pair_recv.at[k],
            device_id=partner, device_id_type=MESH,
        )

    def nth_out(i):
        q = core * (3 - i) + (1 - core) * i
        chip = 4 * core + q
        own = jnp.logical_and(jnp.logical_and(upper == core, side0 == core), quad == q)
        return q, own, device(chip, side0), order(chip, side0) > me

    def out_copy(i, k):
        start, rows = CHUNK3[k]
        q, own, peer, later = nth_out(i)
        col = pl.multiple_of(half * hw + start, 128)
        return (
            turned.at[q, :, :, pl.ds(start, rows)],
            out.at[:, upper, :, pl.ds(col, rows)],
            out_send.at[i, k],
            out_recv.at[zl // 2, k],
            peer,
        )

    def send_block(i, k):
        q, own, peer, later = nth_out(i)
        if k == 0:
            pl.when(later)(lambda: pl.semaphore_wait(ready_out.at[q], 1))
        start_copy(out_copy(i, k), own)

    for k in range(2):
        start, rows = CHUNK1[k]
        for s in range(4):
            ref = units.at[s, :, pl.ds(start, rows), :]
            pltpu.make_async_remote_copy(
                src_ref=ref, dst_ref=ref, send_sem=in_send.at[0, k], recv_sem=in_recv.at[s, k],
                device_id=partner, device_id_type=MESH,
            ).wait_recv()
        for p in range(2):
            lhs = jnp.concatenate(
                [units[2 * p + side, ch, pl.ds(start, rows), :] for side in range(2) for ch in range(2)], axis=1
            )
            merge(1, lhs, start, rows, 2 * RIM, x2, (2 * p, 2 * p + 1))
        clear(x2, k, 2 * RIM)
        start, rows = CHUNK2[k]
        for p in range(2):
            lhs = jnp.concatenate(
                [
                    interpolate(lambda o, n: x2[p + 2 * side, ch, pl.ds(start + o, n), :], rows, bits2[side], 2)
                    for side in range(2)
                    for ch in range(2)
                ],
                axis=1,
            )
            merge(2, lhs, start, rows, RIM, x3, (p, p + 2))
        clear(x3, k, RIM)
        start, rows = CHUNK3[k]
        for s in range(4):
            for ch in range(2):
                y3[core, s, ch, pl.ds(start, rows), :] = interpolate(
                    lambda o, n: x3[s, ch, pl.ds(start + o, n), :], rows, bits3, 3
                )
        pair_copy(k).start()
        pair_wait(k).wait_recv()
        for s in range(4):
            rhs = jnp.concatenate(
                [y3[side, s, ch, pl.ds(start, rows), :] for side in range(2) for ch in range(2)], axis=1
            )
            z = lax.dot_general(
                wide[3, pl.ds(0, 256), :], rhs, (((1,), (1,)), ((), ())), preferred_element_type=F32
            )
            re, im = z[:128], z[128:]
            turned[s, 0, :, pl.ds(start, rows)] = (re * cos_last[...] - im * sin_last[...]).astype(BF16)
            turned[s, 1, :, pl.ds(start, rows)] = (re * sin_last[...] + im * cos_last[...]).astype(BF16)
        for i in range(4):
            send_block(i, k)

    to_core.wait_send()
    for j in range(2):
        @pl.when(lower_rng)
        def _():
            halo_copy(j, 0).wait_send()

        @pl.when(upper_rng)
        def _():
            halo_copy(j, 1).wait_send()

    for k in range(2):
        for i in range(4):
            wait_sent(in_copy(i, k), nth(i)[1])
        pair_copy(k).wait_send()
        for i in range(4):
            wait_sent(out_copy(i, k), nth_out(i)[1])
    for k in range(2):
        start, rows = CHUNK3[k]
        for s in range(4):
            pltpu.make_async_remote_copy(
                src_ref=turned.at[0, :, :, pl.ds(start, rows)],
                dst_ref=out.at[:, s // 2, :, pl.ds((s % 2) * hw + start, rows)],
                send_sem=out_send.at[0, k],
                recv_sem=out_recv.at[s, k],
                device_id=partner,
                device_id_type=MESH,
            ).wait_recv()


def on_device(image, interp_weights, range_taps, range_shifts):
    width = image.shape[3]
    hw = width // 2
    margin = LEVELS * RIM
    dma = pltpu.SemaphoreType.DMA
    vmem = pltpu.VMEM
    return pl.pallas_call(
        kernel,
        out_shape=pltpu.VMEM(image.shape, image.dtype),
        in_specs=[
            pl.BlockSpec(memory_space=pl.ANY),
            pl.BlockSpec(memory_space=pl.ANY),
            pl.BlockSpec(memory_space=pl.ANY),
            pl.BlockSpec(memory_space=pl.ANY),
        ],
        out_specs=pl.BlockSpec(memory_space=pltpu.VMEM),
        scratch_shapes=[
            vmem(image.shape, BF16),
            vmem(interp_weights.shape, BF16),
            pltpu.SMEM(range_taps.shape, F32),
            vmem(range_shifts.shape, jnp.int32),
            vmem((LEVELS, 512, 512), BF16),
            vmem((3, 2, TABLE, ANGLES), F32),
            vmem((3, 2, TABLE, ANGLES), F32),
            vmem((ANGLES, 128), F32),
            vmem((ANGLES, 128), F32),
            vmem((2, 2, width, ANGLES), BF16),
            vmem((2, 2, width + 2 * margin + 16, ANGLES), F32),
            vmem((2, width, ANGLES), BF16),
            vmem((2, 2, 2, margin, ANGLES), BF16),
            vmem((2, 2, width + 6 * RIM + 16, ANGLES), F32),
            vmem((2, 2, width + 4 * RIM, ANGLES), BF16),
            vmem((4, 2, hw + 4 * RIM, ANGLES), BF16),
            vmem((4, 2, hw + 4 * RIM + 16, ANGLES), F32),
            vmem((4, 2, hw + 2 * RIM + 16, ANGLES), F32),
            vmem((2, 4, 2, hw, ANGLES), BF16),
            vmem((4, 2, ANGLES, hw), BF16),
            dma((4,)),
            dma((2,)),
            dma((2, 2)),
            dma((2, 2)),
            dma((4, 2)),
            dma((4, 2)),
            dma((2,)),
            dma((2,)),
            dma((4, 2)),
            dma((4, 2)),
            pltpu.SemaphoreType.REGULAR,
            pltpu.SemaphoreType.REGULAR((2,)),
            pltpu.SemaphoreType.REGULAR((4,)),
            pltpu.SemaphoreType.REGULAR((4,)),
        ],
        compiler_params=pltpu.CompilerParams(collective_id=0, has_side_effects=True),
        name="backprojection",
    )(image, interp_weights, range_taps, range_shifts)


def solution(mesh):
    return jax.shard_map(
        on_device,
        mesh=mesh,
        in_specs=(P(None, ("img", "sub"), None, "rng"), P(), P(), P()),
        out_specs=P(None, ("img", "sub"), None, "rng"),
        check_vma=False,
    )
```

```python
import math

import jax
import jax.numpy as jnp
from jax import lax
from jax.experimental import pallas as pl
from jax.experimental.pallas import tpu as pltpu
from jax.sharding import PartitionSpec as P

ANGLES = 128
RIM = 8
TAPS = 4
LEVELS = 4
PERIOD = 64
PHASE_STEP = 2.0 * math.pi / PERIOD

MESH = pl.DeviceIdType.MESH
F32 = jnp.float32
BF16 = jnp.bfloat16

CHUNK1 = ((0, 96), (96, 64), (160, 128))
CHUNK2 = ((0, 80), (80, 64), (144, 128))
CHUNK3 = ((0, 64), (64, 64), (128, 128))
CHUNKS = len(CHUNK3)
ROWS0 = (((256, 112), (0, 112)), ((112, 64), (368, 64)), ((176, 80), (432, 128)))
TABLE = 256


def kernel(
    image_hbm, weights_hbm, taps_hbm, shifts_hbm, out,
    image, weights, taps, shifts, wide, cos_t, sin_t,
    rows_bf, first, from_core, halo, x1, y1, units, x2, x3, y3, turned, blocks,
    load_sem, core_sem, halo_send, halo_recv, in_send, in_recv, pair_send, pair_recv, out_send, out_recv,
    ready_core, ready_rng, ready_in, ready_out,
):
    sub = lax.axis_index("sub")
    rng = lax.axis_index("rng")
    last_rng = lax.axis_size("rng") - 1
    core = sub % 2
    z = sub // 2
    zl = z % 8
    base = z - zl
    quad = zl % 4
    upper = zl // 4
    half = (zl // 2) % 2
    side0 = zl % 2
    width = image.shape[3]
    hw = width // 2

    load_image = pltpu.make_async_copy(image_hbm, image, load_sem.at[0])
    load_weights = pltpu.make_async_copy(weights_hbm, weights, load_sem.at[1])
    load_taps = pltpu.make_async_copy(taps_hbm, taps, load_sem.at[2])
    load_shifts = pltpu.make_async_copy(shifts_hbm, shifts, load_sem.at[3])
    load_image.start()
    load_weights.start()
    load_taps.start()
    load_shifts.start()

    def device(z_local, core_index):
        return {"sub": (base + z_local) * 2 + core_index}

    def order(z_local, core_index):
        return jnp.where(z_local * 2 + core_index == 0, 16, z_local * 2 + (1 - core_index))

    me = order(zl, core)
    partner = {"sub": z * 2 + (1 - core)}
    in_chips = [4 * core + q for q in range(4)]
    in_self = [jnp.logical_and(upper == core, quad == q) for q in range(4)]
    in_peers = [device(chip, upper) for chip in in_chips]
    in_later = [order(chip, upper) > me for chip in in_chips]
    out_self = [jnp.logical_and(in_self[q], side0 == core) for q in range(4)]
    out_dests = [device(chip, side0) for chip in in_chips]
    out_later = [order(chip, side0) > me for chip in in_chips]
    source_chips = [2 * k + core for k in range(4)]
    source_self = [jnp.logical_and(zl == source_chips[k], upper == core) for k in range(4)]
    out_sources = [device(chip, upper) for chip in source_chips]
    source_later = [order(chip, upper) > me for chip in source_chips]
    lower_rng, upper_rng = rng > 0, rng < last_rng

    barrier = pltpu.get_barrier_semaphore()

    def greet(who):
        pl.semaphore_signal(barrier, inc=1, device_id=who, device_id_type=MESH)

    def answer(sem, who):
        pl.semaphore_signal(sem, inc=1, device_id=who, device_id_type=MESH)

    def earlier(later, own):
        return jnp.logical_not(jnp.logical_or(later, own))

    @pl.when(core == 1)
    def _():
        greet(partner)

    @pl.when(lower_rng)
    def _():
        for c in range(2):
            greet({"sub": z * 2 + c, "rng": rng - 1})

    for peers, later in ((in_peers, in_later), (out_dests, out_later), (out_sources, source_later)):
        for q in range(4):
            @pl.when(later[q])
            def _():
                greet(peers[q])

    count = jnp.where(core == 0, 1, 0) + jnp.where(upper_rng, 2, 0)
    for later, own in ((in_later, in_self), (out_later, out_self), (source_later, source_self)):
        for q in range(4):
            count = count + jnp.where(earlier(later[q], own[q]), 1, 0)
    pl.when(count > 0)(lambda: pl.semaphore_wait(barrier, count))

    @pl.when(upper_rng)
    def _():
        for c in range(2):
            answer(ready_rng.at[core], {"sub": z * 2 + c, "rng": rng + 1})

    @pl.when(core == 0)
    def _():
        answer(ready_core, partner)

    for q in range(4):
        @pl.when(earlier(in_later[q], in_self[q]))
        def _():
            answer(ready_in.at[quad], in_peers[q])

        @pl.when(earlier(source_later[q], source_self[q]))
        def _():
            answer(ready_out.at[quad], out_sources[q])

    def fill_phase(level, h, place):
        r = lax.broadcasted_iota(jnp.int32, (PERIOD, ANGLES), 0)
        a = lax.broadcasted_iota(jnp.int32, (PERIOD, ANGLES), 1)
        phase = ((r * (h * ANGLES + a + 1) * (7 + level)) % PERIOD).astype(F32) * PHASE_STEP
        c, s = jnp.cos(phase), jnp.sin(phase)
        for i in range(TABLE // PERIOD):
            cos_t[level, place, pl.ds(i * PERIOD, PERIOD), :] = c
            sin_t[level, place, pl.ds(i * PERIOD, PERIOD), :] = s

    def fill_table(level):
        for h in range(2):
            fill_phase(level, h, h)

    load_image.wait()

    for ch in range(2):
        for j in range(2):
            for k in range(width // 128):
                block = image[ch, j, :, pl.ds(k * 128, 128)].astype(F32).T
                rows_bf[j, ch, pl.ds(k * 128, 128), :] = block.astype(BF16)

    def fill_part(level, side, h, place):
        wr = weights[level, side, h, 0].astype(F32).T.astype(BF16)
        wi = weights[level, side, h, 1].astype(F32).T.astype(BF16)
        for c, x, value in ((0, 0, wr), (1, 0, -wi), (0, 1, wi), (1, 1, wr)):
            wide[level, pl.ds((side * 2 + c) * 128, 128), pl.ds((place * 2 + x) * 128, 128)] = value

    def fill_wide(level):
        for side in range(2):
            for h in range(2):
                fill_part(level, side, h, h)

    to_core = pltpu.make_async_remote_copy(
        src_ref=rows_bf.at[1 - core],
        dst_ref=from_core,
        send_sem=core_sem.at[0],
        recv_sem=core_sem.at[1],
        device_id=partner,
        device_id_type=MESH,
    )
    margin = LEVELS * RIM

    def halo_copy(j, lr):
        start = 0 if lr == 0 else width - margin
        return pltpu.make_async_remote_copy(
            src_ref=rows_bf.at[j, :, pl.ds(start, margin), :],
            dst_ref=halo.at[core, lr],
            send_sem=halo_send.at[j, lr],
            recv_sem=halo_recv.at[core, lr],
            device_id={"sub": z * 2 + j, "rng": rng - 1 + 2 * lr},
            device_id_type=MESH,
        )

    def halo_wait(side, lr):
        return pltpu.make_async_remote_copy(
            src_ref=rows_bf.at[0, :, pl.ds(0, margin), :],
            dst_ref=halo.at[side, lr],
            send_sem=halo_send.at[0, lr],
            recv_sem=halo_recv.at[side, lr],
            device_id=partner,
            device_id_type=MESH,
        )

    @pl.when(core == 1)
    def _():
        pl.semaphore_wait(ready_core, 1)

    to_core.start()

    @pl.when(upper_rng)
    def _():
        for j in range(2):
            halo_copy(j, 1).start()

    load_taps.wait()
    load_shifts.wait()
    load_weights.wait()
    fill_wide(0)
    fill_table(0)

    @pl.when(lower_rng)
    def _():
        for j in range(2):
            pl.semaphore_wait(ready_rng.at[j], 1)
            halo_copy(j, 0).start()

    for ch in range(2):
        first[core, ch, pl.ds(margin, width), :] = rows_bf[core, ch].astype(F32)
    to_core.wait_recv()
    for ch in range(2):
        first[1 - core, ch, pl.ds(margin, width), :] = from_core[ch].astype(F32)

    def take_halo(lr):
        start, there = ((margin + width, upper_rng), (0, lower_rng))[lr]

        @pl.when(there)
        def _():
            for side in range(2):
                halo_wait(side, lr).wait_recv()
                for ch in range(2):
                    first[side, ch, pl.ds(start, margin), :] = halo[side, lr, ch].astype(F32)

        @pl.when(jnp.logical_not(there))
        def _():
            first[:, :, pl.ds(start, margin), :] = jnp.zeros((2, 2, margin, ANGLES), F32)

    def bits_of(row):
        code = row + RIM
        return [((code // v) % 2) == 1 for v in (1, 2, 4, 8)]

    def shift_row(level, side):
        return shifts[level, pl.ds(side, 1), :]

    def interpolate(load, rows, bits, level):
        n = rows + 8
        b0, b1, b2, b3 = bits
        v = jnp.where(
            b3,
            jnp.where(b2, load(12, n), load(8, n)),
            jnp.where(b2, load(4, n), load(0, n)),
        )
        v = jnp.where(b0, pltpu.roll(v, n - 1, 0), v)
        v = jnp.where(b1, pltpu.roll(v, n - 2, 0), v)
        total = v * taps[level, 0]
        for t in range(1, TAPS):
            total = total + pltpu.roll(v, n - t, 0) * taps[level, t]
        return total[:rows].astype(BF16)

    def turn(level, h, start, rows, re, im):
        c = cos_t[level, h, pl.ds(start, rows), :]
        s = sin_t[level, h, pl.ds(start, rows), :]
        return re * c - im * s, re * s + im * c

    bits0 = [bits_of(shift_row(0, side)) for side in range(2)]
    rows1 = width + 2 * (margin - RIM)

    def level0(b, rows):
        parts = []
        for side in range(2):
            for ch in range(2):
                parts.append(interpolate(lambda o, n: first[side, ch, pl.ds(b + o, n), :], rows, bits0[side], 0))
        merged = jnp.dot(jnp.concatenate(parts, axis=1), wide[0], preferred_element_type=F32)
        start = (b - (margin - RIM)) % PERIOD
        for h in range(2):
            re, im = merged[:, h * 256 : h * 256 + 128], merged[:, h * 256 + 128 : h * 256 + 256]
            re, im = turn(0, h, start, rows, re, im)
            x1[h, 0, pl.ds(b, rows), :] = re
            x1[h, 1, pl.ds(b, rows), :] = im

    def clear1(start):
        x1[:, :, pl.ds(start, margin - RIM), :] = jnp.zeros((2, 2, margin - RIM, ANGLES), F32)

    own_bits1 = [((shift_row(1, side0) + RIM) // v) % 2 == 1 for v in (1, 2, 4, 8)]

    def nth(i):
        q = jnp.where(jnp.logical_and(core == 1, zl > 0), i, 3 - i)
        chip = 4 * core + q
        own = jnp.logical_and(upper == core, quad == q)
        return q, own, device(chip, upper), order(chip, upper) > me

    def in_copy(i, k):
        start, rows = CHUNK1[k]
        q, own, peer, later = nth(i)
        row = pl.multiple_of((q // 2) * hw + start, 32)
        return (
            y1.at[q % 2, :, pl.ds(row, rows), :],
            units.at[quad, :, pl.ds(start, rows), :],
            in_send.at[i, k],
            in_recv.at[quad, k],
            peer,
        )

    def send_unit(i, k):
        q, own, peer, later = nth(i)
        if k == 0:
            pl.when(later)(lambda: pl.semaphore_wait(ready_in.at[q], 1))
        start_copy(in_copy(i, k), own)

    def remote(src, dst, send, recv, peer):
        return pltpu.make_async_remote_copy(
            src_ref=src, dst_ref=dst, send_sem=send, recv_sem=recv, device_id=peer, device_id_type=MESH
        )

    def start_copy(parts, local):
        src, dst, send, recv, peer = parts

        @pl.when(local)
        def _():
            pltpu.make_async_copy(src, dst, recv).start()

        @pl.when(jnp.logical_not(local))
        def _():
            remote(*parts).start()

    def wait_sent(parts, local):
        @pl.when(jnp.logical_not(local))
        def _():
            remote(*parts).wait_send()

    for k in range(CHUNKS):
        level0(*ROWS0[k][0])
        if k == 0:
            take_halo(1)
        elif k == CHUNKS - 1:
            take_halo(0)
        level0(*ROWS0[k][1])
        if k == 0:
            pl.when(jnp.logical_not(lower_rng))(lambda: clear1(0))
        elif k == CHUNKS - 1:
            pl.when(jnp.logical_not(upper_rng))(lambda: clear1(rows1 - (margin - RIM)))
        start = CHUNK1[k][0]
        for part in range(2):
            if k == CHUNKS - 1 and part == 0:
                rows = hw - start
            else:
                rows = CHUNK1[k][1]
            for h in range(2):
                for ch in range(2):
                    at = part * hw + start
                    y1[h, ch, pl.ds(at, rows), :] = interpolate(
                        lambda o, n: x1[h, ch, pl.ds(at + o, n), :], rows, own_bits1, 1
                    )
        for i in range(3):
            send_unit(i, k)
        if k < CHUNKS - 1:
            pl.when(zl == 0)(lambda: send_unit(3, k))
        else:
            @pl.when(zl > 0)
            def _():
                for early in range(CHUNKS - 1):
                    send_unit(3, early)

            send_unit(3, k)

    fill_wide(1)
    fill_table(1)
    fill_wide(2)
    fill_table(2)
    for side in range(2):
        fill_part(3, side, core, 0)
    fill_phase(3, core, 0)

    bits2 = [bits_of(shift_row(2, side)) for side in range(2)]
    bits3 = bits_of(shift_row(3, core))
    at_start = jnp.logical_and(rng == 0, half == 0)
    at_end = jnp.logical_and(rng == last_rng, half == 1)

    def merge(level, lhs, start_row, rows, margin_rows, dst, slots):
        z = jnp.dot(lhs, wide[level], preferred_element_type=F32)
        start = (start_row - margin_rows) % PERIOD
        for h in range(2):
            re, im = turn(level, h, start, rows, z[:, h * 256 : h * 256 + 128], z[:, h * 256 + 128 : h * 256 + 256])
            dst[slots[h], 0, pl.ds(start_row, rows), :] = re
            dst[slots[h], 1, pl.ds(start_row, rows), :] = im

    def clear(dst, k, margin_rows):
        total = hw + 2 * margin_rows
        if 0 < k < CHUNKS - 1:
            return

        @pl.when(at_start if k == 0 else at_end)
        def _():
            at = 0 if k == 0 else total - margin_rows
            dst[:, :, pl.ds(at, margin_rows), :] = jnp.zeros((4, 2, margin_rows, ANGLES), F32)

    def pair_copy(k):
        start, rows = CHUNK3[k]
        ref = y3.at[core, :, :, pl.ds(start, rows), :]
        return pltpu.make_async_remote_copy(
            src_ref=ref, dst_ref=ref, send_sem=pair_send.at[k], recv_sem=pair_recv.at[k],
            device_id=partner, device_id_type=MESH,
        )

    def pair_wait(k):
        start, rows = CHUNK3[k]
        ref = y3.at[1 - core, :, :, pl.ds(start, rows), :]
        return pltpu.make_async_remote_copy(
            src_ref=ref, dst_ref=ref, send_sem=pair_send.at[k], recv_sem=pair_recv.at[k],
            device_id=partner, device_id_type=MESH,
        )

    def nth_out(i):
        q = core * (3 - i) + (1 - core) * i
        chip = 4 * core + q
        own = jnp.logical_and(jnp.logical_and(upper == core, side0 == core), quad == q)
        return q, own, device(chip, side0), order(chip, side0) > me

    def out_copy(i, k):
        start, rows = CHUNK3[k]
        q, own, peer, later = nth_out(i)
        row = pl.multiple_of(half * hw + start, 64)
        return (
            turned.at[q, :, pl.ds(start, rows), :],
            blocks.at[upper, :, pl.ds(row, rows), :],
            out_send.at[i, k],
            out_recv.at[zl // 2, k],
            peer,
        )

    def send_block(i, k):
        q, own, peer, later = nth_out(i)
        if k == 0:
            pl.when(later)(lambda: pl.semaphore_wait(ready_out.at[q], 1))
        start_copy(out_copy(i, k), own)

    for k in range(CHUNKS):
        start, rows = CHUNK1[k]
        for s in range(4):
            ref = units.at[s, :, pl.ds(start, rows), :]
            pltpu.make_async_remote_copy(
                src_ref=ref, dst_ref=ref, send_sem=in_send.at[0, k], recv_sem=in_recv.at[s, k],
                device_id=partner, device_id_type=MESH,
            ).wait_recv()
        for p in range(2):
            lhs = jnp.concatenate(
                [units[2 * p + side, ch, pl.ds(start, rows), :] for side in range(2) for ch in range(2)], axis=1
            )
            merge(1, lhs, start, rows, 2 * RIM, x2, (2 * p, 2 * p + 1))
        clear(x2, k, 2 * RIM)
        start, rows = CHUNK2[k]
        for p in range(2):
            lhs = jnp.concatenate(
                [
                    interpolate(lambda o, n: x2[p + 2 * side, ch, pl.ds(start + o, n), :], rows, bits2[side], 2)
                    for side in range(2)
                    for ch in range(2)
                ],
                axis=1,
            )
            merge(2, lhs, start, rows, RIM, x3, (p, p + 2))
        clear(x3, k, RIM)
        start, rows = CHUNK3[k]
        for s in range(4):
            for ch in range(2):
                y3[core, s, ch, pl.ds(start, rows), :] = interpolate(
                    lambda o, n: x3[s, ch, pl.ds(start + o, n), :], rows, bits3, 3
                )
        pair_copy(k).start()
        pair_wait(k).wait_recv()
        for s in range(4):
            lhs = jnp.concatenate(
                [y3[side, s, ch, pl.ds(start, rows), :] for side in range(2) for ch in range(2)], axis=1
            )
            merged = jnp.dot(lhs, wide[3, :, pl.ds(0, 256)], preferred_element_type=F32)
            re, im = turn(3, 0, start % PERIOD, rows, merged[:, :128], merged[:, 128:])
            turned[s, 0, pl.ds(start, rows), :] = re.astype(BF16)
            turned[s, 1, pl.ds(start, rows), :] = im.astype(BF16)
        for i in range(4):
            send_block(i, k)

    def block_wait(s, k):
        start, rows = CHUNK3[k]
        ref = blocks.at[s // 2, :, pl.ds((s % 2) * hw + start, rows), :]
        remote(ref, ref, out_send.at[0, k], out_recv.at[s, k], partner).wait_recv()

    for first_chunk, last_chunk, col in ((0, 1, 0), (2, 2, 128)):
        for s in range(4):
            for k in range(first_chunk, last_chunk + 1):
                block_wait(s, k)
            at = (s % 2) * hw + col
            for ch in range(2):
                block = blocks[s // 2, ch, pl.ds(at, 128), :].astype(F32).T
                out[ch, s // 2, :, pl.ds(at, 128)] = block.astype(BF16)

    to_core.wait_send()
    for j in range(2):
        @pl.when(lower_rng)
        def _():
            halo_copy(j, 0).wait_send()

        @pl.when(upper_rng)
        def _():
            halo_copy(j, 1).wait_send()

    for k in range(CHUNKS):
        for i in range(4):
            wait_sent(in_copy(i, k), nth(i)[1])
        pair_copy(k).wait_send()
        for i in range(4):
            wait_sent(out_copy(i, k), nth_out(i)[1])


def on_device(image, interp_weights, range_taps, range_shifts):
    width = image.shape[3]
    hw = width // 2
    margin = LEVELS * RIM
    dma = pltpu.SemaphoreType.DMA
    vmem = pltpu.VMEM
    return pl.pallas_call(
        kernel,
        out_shape=pltpu.VMEM(image.shape, image.dtype),
        in_specs=[
            pl.BlockSpec(memory_space=pl.ANY),
            pl.BlockSpec(memory_space=pl.ANY),
            pl.BlockSpec(memory_space=pl.ANY),
            pl.BlockSpec(memory_space=pl.ANY),
        ],
        out_specs=pl.BlockSpec(memory_space=pltpu.VMEM),
        scratch_shapes=[
            vmem(image.shape, BF16),
            vmem(interp_weights.shape, BF16),
            pltpu.SMEM(range_taps.shape, F32),
            vmem(range_shifts.shape, jnp.int32),
            vmem((LEVELS, 512, 512), BF16),
            vmem((LEVELS, 2, TABLE, ANGLES), F32),
            vmem((LEVELS, 2, TABLE, ANGLES), F32),
            vmem((2, 2, width, ANGLES), BF16),
            vmem((2, 2, width + 2 * margin + 16, ANGLES), F32),
            vmem((2, width, ANGLES), BF16),
            vmem((2, 2, 2, margin, ANGLES), BF16),
            vmem((2, 2, width + 6 * RIM + 16, ANGLES), F32),
            vmem((2, 2, width + 4 * RIM, ANGLES), BF16),
            vmem((4, 2, hw + 4 * RIM, ANGLES), BF16),
            vmem((4, 2, hw + 4 * RIM + 16, ANGLES), F32),
            vmem((4, 2, hw + 2 * RIM + 16, ANGLES), F32),
            vmem((2, 4, 2, hw, ANGLES), BF16),
            vmem((4, 2, hw, ANGLES), BF16),
            vmem((2, 2, width, ANGLES), BF16),
            dma((4,)),
            dma((2,)),
            dma((2, 2)),
            dma((2, 2)),
            dma((4, CHUNKS)),
            dma((4, CHUNKS)),
            dma((CHUNKS,)),
            dma((CHUNKS,)),
            dma((4, CHUNKS)),
            dma((4, CHUNKS)),
            pltpu.SemaphoreType.REGULAR,
            pltpu.SemaphoreType.REGULAR((2,)),
            pltpu.SemaphoreType.REGULAR((4,)),
            pltpu.SemaphoreType.REGULAR((4,)),
        ],
        compiler_params=pltpu.CompilerParams(collective_id=0, has_side_effects=True),
        name="backprojection",
    )(image, interp_weights, range_taps, range_shifts)


def solution(mesh):
    return jax.shard_map(
        on_device,
        mesh=mesh,
        in_specs=(P(None, ("img", "sub"), None, "rng"), P(), P(), P()),
        out_specs=P(None, ("img", "sub"), None, "rng"),
        check_vma=False,
    )
```

```python
import math

import jax
import jax.numpy as jnp
from jax import lax
from jax.experimental import pallas as pl
from jax.experimental.pallas import tpu as pltpu
from jax.sharding import PartitionSpec as P

ANGLES = 128
RIM = 8
TAPS = 4
LEVELS = 4
PERIOD = 64
PHASE_STEP = 2.0 * math.pi / PERIOD

MESH = pl.DeviceIdType.MESH
F32 = jnp.float32
BF16 = jnp.bfloat16

CHUNK1 = ((0, 96), (96, 64), (160, 128))
CHUNK2 = ((0, 80), (80, 64), (144, 128))
CHUNK3 = ((0, 64), (64, 64), (128, 128))
CHUNKS = len(CHUNK3)
ROWS0 = (((256, 112), (0, 112)), ((112, 64), (368, 64)), ((176, 80), (432, 128)))
TABLE = 256


def kernel(
    image_hbm, weights_hbm, taps_hbm, shifts_hbm, out,
    image, weights, taps, shifts, wide, cos_t, sin_t,
    rows_bf, first, from_core, halo, x1, y1, units, x2, x3, y3, turned, blocks,
    load_sem, core_sem, halo_send, halo_recv, in_send, in_recv, pair_send, pair_recv, out_send, out_recv,
    ready_core, ready_rng, ready_in, ready_out,
):
    sub = lax.axis_index("sub")
    rng = lax.axis_index("rng")
    last_rng = lax.axis_size("rng") - 1
    core = sub % 2
    z = sub // 2
    zl = z % 8
    base = z - zl
    quad = zl % 4
    upper = zl // 4
    half = (zl // 2) % 2
    side0 = zl % 2
    width = image.shape[3]
    hw = width // 2

    load_image = pltpu.make_async_copy(image_hbm, image, load_sem.at[0])
    load_weights = pltpu.make_async_copy(weights_hbm, weights, load_sem.at[1])
    load_taps = pltpu.make_async_copy(taps_hbm, taps, load_sem.at[2])
    load_shifts = pltpu.make_async_copy(shifts_hbm, shifts, load_sem.at[3])
    load_image.start()
    load_weights.start()
    load_taps.start()
    load_shifts.start()

    def device(z_local, core_index):
        return {"sub": (base + z_local) * 2 + core_index}

    def order(z_local, core_index):
        return jnp.where(z_local * 2 + core_index == 0, 16, z_local * 2 + (1 - core_index))

    me = order(zl, core)
    partner = {"sub": z * 2 + (1 - core)}
    in_chips = [4 * core + q for q in range(4)]
    in_self = [jnp.logical_and(upper == core, quad == q) for q in range(4)]
    in_peers = [device(chip, upper) for chip in in_chips]
    in_later = [order(chip, upper) > me for chip in in_chips]
    out_self = [jnp.logical_and(in_self[q], side0 == core) for q in range(4)]
    out_dests = [device(chip, side0) for chip in in_chips]
    out_later = [order(chip, side0) > me for chip in in_chips]
    source_chips = [2 * k + core for k in range(4)]
    source_self = [jnp.logical_and(zl == source_chips[k], upper == core) for k in range(4)]
    out_sources = [device(chip, upper) for chip in source_chips]
    source_later = [order(chip, upper) > me for chip in source_chips]
    lower_rng, upper_rng = rng > 0, rng < last_rng

    barrier = pltpu.get_barrier_semaphore()

    def greet(who):
        pl.semaphore_signal(barrier, inc=1, device_id=who, device_id_type=MESH)

    def answer(sem, who):
        pl.semaphore_signal(sem, inc=1, device_id=who, device_id_type=MESH)

    def earlier(later, own):
        return jnp.logical_not(jnp.logical_or(later, own))

    @pl.when(core == 1)
    def _():
        greet(partner)

    @pl.when(lower_rng)
    def _():
        for c in range(2):
            greet({"sub": z * 2 + c, "rng": rng - 1})

    for peers, later in ((in_peers, in_later), (out_dests, out_later), (out_sources, source_later)):
        for q in range(4):
            @pl.when(later[q])
            def _():
                greet(peers[q])

    count = jnp.where(core == 0, 1, 0) + jnp.where(upper_rng, 2, 0)
    for later, own in ((in_later, in_self), (out_later, out_self), (source_later, source_self)):
        for q in range(4):
            count = count + jnp.where(earlier(later[q], own[q]), 1, 0)
    pl.when(count > 0)(lambda: pl.semaphore_wait(barrier, count))

    @pl.when(upper_rng)
    def _():
        for c in range(2):
            answer(ready_rng.at[core], {"sub": z * 2 + c, "rng": rng + 1})

    @pl.when(core == 0)
    def _():
        answer(ready_core, partner)

    for q in range(4):
        @pl.when(earlier(in_later[q], in_self[q]))
        def _():
            answer(ready_in.at[quad], in_peers[q])

        @pl.when(earlier(source_later[q], source_self[q]))
        def _():
            answer(ready_out.at[quad], out_sources[q])

    def fill_phase(level, h, place):
        r = lax.broadcasted_iota(jnp.int32, (PERIOD, ANGLES), 0)
        a = lax.broadcasted_iota(jnp.int32, (PERIOD, ANGLES), 1)
        phase = ((r * (h * ANGLES + a + 1) * (7 + level)) % PERIOD).astype(F32) * PHASE_STEP
        c, s = jnp.cos(phase), jnp.sin(phase)
        for i in range(TABLE // PERIOD):
            cos_t[level, place, pl.ds(i * PERIOD, PERIOD), :] = c
            sin_t[level, place, pl.ds(i * PERIOD, PERIOD), :] = s

    def fill_table(level):
        for h in range(2):
            fill_phase(level, h, h)

    load_image.wait()

    for ch in range(2):
        for j in range(2):
            for k in range(width // 128):
                block = image[ch, j, :, pl.ds(k * 128, 128)].astype(F32).T
                rows_bf[j, ch, pl.ds(k * 128, 128), :] = block.astype(BF16)

    def fill_part(level, side, h, place):
        wr = weights[level, side, h, 0].astype(F32).T.astype(BF16)
        wi = weights[level, side, h, 1].astype(F32).T.astype(BF16)
        for c, x, value in ((0, 0, wr), (1, 0, -wi), (0, 1, wi), (1, 1, wr)):
            wide[level, pl.ds((side * 2 + c) * 128, 128), pl.ds((place * 2 + x) * 128, 128)] = value

    def fill_wide(level):
        for side in range(2):
            for h in range(2):
                fill_part(level, side, h, h)

    to_core = pltpu.make_async_remote_copy(
        src_ref=rows_bf.at[1 - core],
        dst_ref=from_core,
        send_sem=core_sem.at[0],
        recv_sem=core_sem.at[1],
        device_id=partner,
        device_id_type=MESH,
    )
    margin = LEVELS * RIM

    def halo_copy(j, lr):
        start = 0 if lr == 0 else width - margin
        return pltpu.make_async_remote_copy(
            src_ref=rows_bf.at[j, :, pl.ds(start, margin), :],
            dst_ref=halo.at[core, lr],
            send_sem=halo_send.at[j, lr],
            recv_sem=halo_recv.at[core, lr],
            device_id={"sub": z * 2 + j, "rng": rng - 1 + 2 * lr},
            device_id_type=MESH,
        )

    def halo_wait(side, lr):
        return pltpu.make_async_remote_copy(
            src_ref=rows_bf.at[0, :, pl.ds(0, margin), :],
            dst_ref=halo.at[side, lr],
            send_sem=halo_send.at[0, lr],
            recv_sem=halo_recv.at[side, lr],
            device_id=partner,
            device_id_type=MESH,
        )

    @pl.when(core == 1)
    def _():
        pl.semaphore_wait(ready_core, 1)

    to_core.start()

    @pl.when(upper_rng)
    def _():
        for j in range(2):
            halo_copy(j, 1).start()

    load_taps.wait()
    load_shifts.wait()
    load_weights.wait()
    fill_wide(0)
    fill_table(0)

    @pl.when(lower_rng)
    def _():
        for j in range(2):
            pl.semaphore_wait(ready_rng.at[j], 1)
            halo_copy(j, 0).start()

    for ch in range(2):
        first[core, ch, pl.ds(margin, width), :] = rows_bf[core, ch].astype(F32)
    to_core.wait_recv()
    for ch in range(2):
        first[1 - core, ch, pl.ds(margin, width), :] = from_core[ch].astype(F32)

    def take_halo(lr):
        start, there = ((margin + width, upper_rng), (0, lower_rng))[lr]

        @pl.when(there)
        def _():
            for side in range(2):
                halo_wait(side, lr).wait_recv()
                for ch in range(2):
                    first[side, ch, pl.ds(start, margin), :] = halo[side, lr, ch].astype(F32)

        @pl.when(jnp.logical_not(there))
        def _():
            first[:, :, pl.ds(start, margin), :] = jnp.zeros((2, 2, margin, ANGLES), F32)

    def bits_of(row):
        code = row + RIM
        return [((code // v) % 2) == 1 for v in (1, 2, 4, 8)]

    def shift_row(level, side):
        return shifts[level, pl.ds(side, 1), :]

    def interpolate(load, rows, bits, level):
        n = rows + 8
        b0, b1, b2, b3 = bits
        v = jnp.where(
            b3,
            jnp.where(b2, load(12, n), load(8, n)),
            jnp.where(b2, load(4, n), load(0, n)),
        )
        v = jnp.where(b0, pltpu.roll(v, n - 1, 0), v)
        v = jnp.where(b1, pltpu.roll(v, n - 2, 0), v)
        total = v * taps[level, 0]
        for t in range(1, TAPS):
            total = total + pltpu.roll(v, n - t, 0) * taps[level, t]
        return total[:rows].astype(BF16)

    def turn(level, h, start, rows, re, im):
        c = cos_t[level, h, pl.ds(start, rows), :]
        s = sin_t[level, h, pl.ds(start, rows), :]
        return re * c - im * s, re * s + im * c

    bits0 = [bits_of(shift_row(0, side)) for side in range(2)]
    rows1 = width + 2 * (margin - RIM)

    def level0(b, rows):
        parts = []
        for side in range(2):
            for ch in range(2):
                parts.append(interpolate(lambda o, n: first[side, ch, pl.ds(b + o, n), :], rows, bits0[side], 0))
        merged = jnp.dot(jnp.concatenate(parts, axis=1), wide[0], preferred_element_type=F32)
        start = (b - (margin - RIM)) % PERIOD
        for h in range(2):
            re, im = merged[:, h * 256 : h * 256 + 128], merged[:, h * 256 + 128 : h * 256 + 256]
            re, im = turn(0, h, start, rows, re, im)
            x1[h, 0, pl.ds(b, rows), :] = re
            x1[h, 1, pl.ds(b, rows), :] = im

    def clear1(start):
        x1[:, :, pl.ds(start, margin - RIM), :] = jnp.zeros((2, 2, margin - RIM, ANGLES), F32)

    own_bits1 = [((shift_row(1, side0) + RIM) // v) % 2 == 1 for v in (1, 2, 4, 8)]

    def nth(i):
        q = core * i + (1 - core) * (3 - i)
        chip = 4 * core + q
        own = jnp.logical_and(upper == core, quad == q)
        return q, own, device(chip, upper), order(chip, upper) > me

    def in_copy(i, k):
        start, rows = CHUNK1[k]
        q, own, peer, later = nth(i)
        row = pl.multiple_of((q // 2) * hw + start, 32)
        return (
            y1.at[q % 2, :, pl.ds(row, rows), :],
            units.at[quad, :, pl.ds(start, rows), :],
            in_send.at[i, k],
            in_recv.at[quad, k],
            peer,
        )

    def send_unit(i, k):
        q, own, peer, later = nth(i)
        if k == 0:
            pl.when(later)(lambda: pl.semaphore_wait(ready_in.at[q], 1))
        start_copy(in_copy(i, k), own)

    def remote(src, dst, send, recv, peer):
        return pltpu.make_async_remote_copy(
            src_ref=src, dst_ref=dst, send_sem=send, recv_sem=recv, device_id=peer, device_id_type=MESH
        )

    def start_copy(parts, local):
        src, dst, send, recv, peer = parts

        @pl.when(local)
        def _():
            pltpu.make_async_copy(src, dst, recv).start()

        @pl.when(jnp.logical_not(local))
        def _():
            remote(*parts).start()

    def wait_sent(parts, local):
        @pl.when(jnp.logical_not(local))
        def _():
            remote(*parts).wait_send()

    for k in range(CHUNKS):
        level0(*ROWS0[k][0])
        if k == 0:
            take_halo(1)
        elif k == CHUNKS - 1:
            take_halo(0)
        level0(*ROWS0[k][1])
        if k == 0:
            pl.when(jnp.logical_not(lower_rng))(lambda: clear1(0))
        elif k == CHUNKS - 1:
            pl.when(jnp.logical_not(upper_rng))(lambda: clear1(rows1 - (margin - RIM)))
        start = CHUNK1[k][0]
        for part in range(2):
            if k == CHUNKS - 1 and part == 0:
                rows = hw - start
            else:
                rows = CHUNK1[k][1]
            for h in range(2):
                for ch in range(2):
                    at = part * hw + start
                    y1[h, ch, pl.ds(at, rows), :] = interpolate(
                        lambda o, n: x1[h, ch, pl.ds(at + o, n), :], rows, own_bits1, 1
                    )
        for i in range(3):
            send_unit(i, k)
        if k < CHUNKS - 1:
            pl.when(zl == 0)(lambda: send_unit(3, k))
        else:
            @pl.when(zl > 0)
            def _():
                for early in range(CHUNKS - 1):
                    send_unit(3, early)

            send_unit(3, k)

    fill_wide(1)
    fill_table(1)
    fill_wide(2)
    fill_table(2)
    for side in range(2):
        fill_part(3, side, core, 0)
    fill_phase(3, core, 0)

    bits2 = [bits_of(shift_row(2, side)) for side in range(2)]
    bits3 = bits_of(shift_row(3, core))
    at_start = jnp.logical_and(rng == 0, half == 0)
    at_end = jnp.logical_and(rng == last_rng, half == 1)

    def merge(level, lhs, start_row, rows, margin_rows, dst, slots):
        z = jnp.dot(lhs, wide[level], preferred_element_type=F32)
        start = (start_row - margin_rows) % PERIOD
        for h in range(2):
            re, im = turn(level, h, start, rows, z[:, h * 256 : h * 256 + 128], z[:, h * 256 + 128 : h * 256 + 256])
            dst[slots[h], 0, pl.ds(start_row, rows), :] = re
            dst[slots[h], 1, pl.ds(start_row, rows), :] = im

    def clear(dst, k, margin_rows):
        total = hw + 2 * margin_rows
        if 0 < k < CHUNKS - 1:
            return

        @pl.when(at_start if k == 0 else at_end)
        def _():
            at = 0 if k == 0 else total - margin_rows
            dst[:, :, pl.ds(at, margin_rows), :] = jnp.zeros((4, 2, margin_rows, ANGLES), F32)

    def pair_copy(k):
        start, rows = CHUNK3[k]
        ref = y3.at[core, :, :, pl.ds(start, rows), :]
        return pltpu.make_async_remote_copy(
            src_ref=ref, dst_ref=ref, send_sem=pair_send.at[k], recv_sem=pair_recv.at[k],
            device_id=partner, device_id_type=MESH,
        )

    def pair_wait(k):
        start, rows = CHUNK3[k]
        ref = y3.at[1 - core, :, :, pl.ds(start, rows), :]
        return pltpu.make_async_remote_copy(
            src_ref=ref, dst_ref=ref, send_sem=pair_send.at[k], recv_sem=pair_recv.at[k],
            device_id=partner, device_id_type=MESH,
        )

    def out_copy(q, k):
        start, rows = CHUNK3[k]
        row = pl.multiple_of(half * hw + start, 64)
        return (
            turned.at[q, :, pl.ds(start, rows), :],
            blocks.at[upper, :, pl.ds(row, rows), :],
            out_send.at[q, k],
            out_recv.at[zl // 2, k],
            out_dests[q],
        )

    def send_block(q, k):
        if k == 0:
            pl.when(out_later[q])(lambda: pl.semaphore_wait(ready_out.at[q], 1))
        start_copy(out_copy(q, k), out_self[q])

    for k in range(CHUNKS):
        start, rows = CHUNK1[k]
        for s in range(4):
            ref = units.at[s, :, pl.ds(start, rows), :]
            pltpu.make_async_remote_copy(
                src_ref=ref, dst_ref=ref, send_sem=in_send.at[0, k], recv_sem=in_recv.at[s, k],
                device_id=partner, device_id_type=MESH,
            ).wait_recv()
        for p in range(2):
            lhs = jnp.concatenate(
                [units[2 * p + side, ch, pl.ds(start, rows), :] for side in range(2) for ch in range(2)], axis=1
            )
            merge(1, lhs, start, rows, 2 * RIM, x2, (2 * p, 2 * p + 1))
        clear(x2, k, 2 * RIM)
        start, rows = CHUNK2[k]
        for p in range(2):
            lhs = jnp.concatenate(
                [
                    interpolate(lambda o, n: x2[p + 2 * side, ch, pl.ds(start + o, n), :], rows, bits2[side], 2)
                    for side in range(2)
                    for ch in range(2)
                ],
                axis=1,
            )
            merge(2, lhs, start, rows, RIM, x3, (p, p + 2))
        clear(x3, k, RIM)
        start, rows = CHUNK3[k]
        for s in range(4):
            for ch in range(2):
                y3[core, s, ch, pl.ds(start, rows), :] = interpolate(
                    lambda o, n: x3[s, ch, pl.ds(start + o, n), :], rows, bits3, 3
                )
        pair_copy(k).start()
        pair_wait(k).wait_recv()
        for s in range(4):
            lhs = jnp.concatenate(
                [y3[side, s, ch, pl.ds(start, rows), :] for side in range(2) for ch in range(2)], axis=1
            )
            merged = jnp.dot(lhs, wide[3, :, pl.ds(0, 256)], preferred_element_type=F32)
            re, im = turn(3, 0, start % PERIOD, rows, merged[:, :128], merged[:, 128:])
            turned[s, 0, pl.ds(start, rows), :] = re.astype(BF16)
            turned[s, 1, pl.ds(start, rows), :] = im.astype(BF16)
        for q in range(3):
            send_block(q, k)
    for k in range(CHUNKS):
        send_block(3, k)

    def block_wait(s, k):
        start, rows = CHUNK3[k]
        ref = blocks.at[s // 2, :, pl.ds((s % 2) * hw + start, rows), :]
        remote(ref, ref, out_send.at[0, k], out_recv.at[s, k], partner).wait_recv()

    for first_chunk, last_chunk, col in ((0, 1, 0), (2, 2, 128)):
        for s in range(4):
            for k in range(first_chunk, last_chunk + 1):
                block_wait(s, k)
            at = (s % 2) * hw + col
            for ch in range(2):
                block = blocks[s // 2, ch, pl.ds(at, 128), :].astype(F32).T
                out[ch, s // 2, :, pl.ds(at, 128)] = block.astype(BF16)

    to_core.wait_send()
    for j in range(2):
        @pl.when(lower_rng)
        def _():
            halo_copy(j, 0).wait_send()

        @pl.when(upper_rng)
        def _():
            halo_copy(j, 1).wait_send()

    for k in range(CHUNKS):
        for i in range(4):
            wait_sent(in_copy(i, k), nth(i)[1])
        pair_copy(k).wait_send()
        for q in range(4):
            wait_sent(out_copy(q, k), out_self[q])


def on_device(image, interp_weights, range_taps, range_shifts):
    width = image.shape[3]
    hw = width // 2
    margin = LEVELS * RIM
    dma = pltpu.SemaphoreType.DMA
    vmem = pltpu.VMEM
    return pl.pallas_call(
        kernel,
        out_shape=pltpu.VMEM(image.shape, image.dtype),
        in_specs=[
            pl.BlockSpec(memory_space=pl.ANY),
            pl.BlockSpec(memory_space=pl.ANY),
            pl.BlockSpec(memory_space=pl.ANY),
            pl.BlockSpec(memory_space=pl.ANY),
        ],
        out_specs=pl.BlockSpec(memory_space=pltpu.VMEM),
        scratch_shapes=[
            vmem(image.shape, BF16),
            vmem(interp_weights.shape, BF16),
            pltpu.SMEM(range_taps.shape, F32),
            vmem(range_shifts.shape, jnp.int32),
            vmem((LEVELS, 512, 512), BF16),
            vmem((LEVELS, 2, TABLE, ANGLES), F32),
            vmem((LEVELS, 2, TABLE, ANGLES), F32),
            vmem((2, 2, width, ANGLES), BF16),
            vmem((2, 2, width + 2 * margin + 16, ANGLES), F32),
            vmem((2, width, ANGLES), BF16),
            vmem((2, 2, 2, margin, ANGLES), BF16),
            vmem((2, 2, width + 6 * RIM + 16, ANGLES), F32),
            vmem((2, 2, width + 4 * RIM, ANGLES), BF16),
            vmem((4, 2, hw + 4 * RIM, ANGLES), BF16),
            vmem((4, 2, hw + 4 * RIM + 16, ANGLES), F32),
            vmem((4, 2, hw + 2 * RIM + 16, ANGLES), F32),
            vmem((2, 4, 2, hw, ANGLES), BF16),
            vmem((4, 2, hw, ANGLES), BF16),
            vmem((2, 2, width, ANGLES), BF16),
            dma((4,)),
            dma((2,)),
            dma((2, 2)),
            dma((2, 2)),
            dma((4, CHUNKS)),
            dma((4, CHUNKS)),
            dma((CHUNKS,)),
            dma((CHUNKS,)),
            dma((4, CHUNKS)),
            dma((4, CHUNKS)),
            pltpu.SemaphoreType.REGULAR,
            pltpu.SemaphoreType.REGULAR((2,)),
            pltpu.SemaphoreType.REGULAR((4,)),
            pltpu.SemaphoreType.REGULAR((4,)),
        ],
        compiler_params=pltpu.CompilerParams(collective_id=0, has_side_effects=True),
        name="backprojection",
    )(image, interp_weights, range_taps, range_shifts)


def solution(mesh):
    return jax.shard_map(
        on_device,
        mesh=mesh,
        in_specs=(P(None, ("img", "sub"), None, "rng"), P(), P(), P()),
        out_specs=P(None, ("img", "sub"), None, "rng"),
        check_vma=False,
    )
```

```python
import math

import jax
import jax.numpy as jnp
from jax import lax
from jax.experimental import pallas as pl
from jax.experimental.pallas import tpu as pltpu
from jax.sharding import PartitionSpec as P

ANGLES = 128
RIM = 8
TAPS = 4
LEVELS = 4
PERIOD = 64
PHASE_STEP = 2.0 * math.pi / PERIOD

MESH = pl.DeviceIdType.MESH
F32 = jnp.float32
BF16 = jnp.bfloat16

CHUNK1 = ((0, 96), (96, 64), (160, 128))
CHUNK2 = ((0, 80), (80, 64), (144, 128))
CHUNK3 = ((0, 64), (64, 64), (128, 128))
CHUNKS = len(CHUNK3)
ROWS0 = (((256, 112), (0, 112)), ((112, 64), (368, 64)), ((176, 80), (432, 128)))
TABLE = 256


def kernel(
    image_hbm, weights_hbm, taps_hbm, shifts_hbm, out,
    image, weights, taps, shifts, wide, cos_t, sin_t,
    rows_bf, first, from_core, halo, x1, y1, units, x2, x3, y3, turned, blocks,
    load_sem, core_sem, halo_send, halo_recv, in_send, in_recv, pair_send, pair_recv, out_send, out_recv,
    ready_core, ready_rng, ready_in, ready_out,
):
    sub = lax.axis_index("sub")
    rng = lax.axis_index("rng")
    last_rng = lax.axis_size("rng") - 1
    core = sub % 2
    z = sub // 2
    zl = z % 8
    base = z - zl
    quad = zl % 4
    upper = zl // 4
    half = (zl // 2) % 2
    side0 = zl % 2
    width = image.shape[3]
    hw = width // 2

    load_image = pltpu.make_async_copy(image_hbm, image, load_sem.at[0])
    load_weights = pltpu.make_async_copy(weights_hbm, weights, load_sem.at[1])
    load_taps = pltpu.make_async_copy(taps_hbm, taps, load_sem.at[2])
    load_shifts = pltpu.make_async_copy(shifts_hbm, shifts, load_sem.at[3])
    load_image.start()
    load_weights.start()
    load_taps.start()
    load_shifts.start()

    def device(z_local, core_index):
        return {"sub": (base + z_local) * 2 + core_index}

    def order(z_local, core_index):
        return jnp.where(z_local * 2 + core_index == 0, 16, z_local * 2 + (1 - core_index))

    me = order(zl, core)
    partner = {"sub": z * 2 + (1 - core)}
    in_chips = [4 * core + q for q in range(4)]
    in_self = [jnp.logical_and(upper == core, quad == q) for q in range(4)]
    in_peers = [device(chip, upper) for chip in in_chips]
    in_later = [order(chip, upper) > me for chip in in_chips]
    out_self = [jnp.logical_and(in_self[q], side0 == core) for q in range(4)]
    out_dests = [device(chip, side0) for chip in in_chips]
    out_later = [order(chip, side0) > me for chip in in_chips]
    source_chips = [2 * k + core for k in range(4)]
    source_self = [jnp.logical_and(zl == source_chips[k], upper == core) for k in range(4)]
    out_sources = [device(chip, upper) for chip in source_chips]
    source_later = [order(chip, upper) > me for chip in source_chips]
    lower_rng, upper_rng = rng > 0, rng < last_rng

    barrier = pltpu.get_barrier_semaphore()

    def greet(who):
        pl.semaphore_signal(barrier, inc=1, device_id=who, device_id_type=MESH)

    def answer(sem, who):
        pl.semaphore_signal(sem, inc=1, device_id=who, device_id_type=MESH)

    def earlier(later, own):
        return jnp.logical_not(jnp.logical_or(later, own))

    @pl.when(core == 1)
    def _():
        greet(partner)

    @pl.when(lower_rng)
    def _():
        for c in range(2):
            greet({"sub": z * 2 + c, "rng": rng - 1})

    for peers, later in ((in_peers, in_later), (out_dests, out_later), (out_sources, source_later)):
        for q in range(4):
            @pl.when(later[q])
            def _():
                greet(peers[q])

    count = jnp.where(core == 0, 1, 0) + jnp.where(upper_rng, 2, 0)
    for later, own in ((in_later, in_self), (out_later, out_self), (source_later, source_self)):
        for q in range(4):
            count = count + jnp.where(earlier(later[q], own[q]), 1, 0)

    def enter():
        pl.when(count > 0)(lambda: pl.semaphore_wait(barrier, count))

        @pl.when(upper_rng)
        def _():
            for c in range(2):
                answer(ready_rng.at[core], {"sub": z * 2 + c, "rng": rng + 1})

        @pl.when(core == 0)
        def _():
            answer(ready_core, partner)

        for q in range(4):
            @pl.when(earlier(in_later[q], in_self[q]))
            def _():
                answer(ready_in.at[quad], in_peers[q])

            @pl.when(earlier(source_later[q], source_self[q]))
            def _():
                answer(ready_out.at[quad], out_sources[q])

    last_to_enter = jnp.logical_and(zl == 0, core == 0)
    pl.when(last_to_enter)(enter)

    def fill_phase(level, h, place):
        r = lax.broadcasted_iota(jnp.int32, (PERIOD, ANGLES), 0)
        a = lax.broadcasted_iota(jnp.int32, (PERIOD, ANGLES), 1)
        phase = ((r * (h * ANGLES + a + 1) * (7 + level)) % PERIOD).astype(F32) * PHASE_STEP
        c, s = jnp.cos(phase), jnp.sin(phase)
        for i in range(TABLE // PERIOD):
            cos_t[level, place, pl.ds(i * PERIOD, PERIOD), :] = c
            sin_t[level, place, pl.ds(i * PERIOD, PERIOD), :] = s

    def fill_table(level):
        for h in range(2):
            fill_phase(level, h, h)

    load_image.wait()

    for ch in range(2):
        for j in range(2):
            for k in range(width // 128):
                block = image[ch, j, :, pl.ds(k * 128, 128)].astype(F32).T
                rows_bf[j, ch, pl.ds(k * 128, 128), :] = block.astype(BF16)

    pl.when(jnp.logical_not(last_to_enter))(enter)

    def fill_part(level, side, h, place):
        wr = weights[level, side, h, 0].astype(F32).T.astype(BF16)
        wi = weights[level, side, h, 1].astype(F32).T.astype(BF16)
        for c, x, value in ((0, 0, wr), (1, 0, -wi), (0, 1, wi), (1, 1, wr)):
            wide[level, pl.ds((side * 2 + c) * 128, 128), pl.ds((place * 2 + x) * 128, 128)] = value

    def fill_wide(level):
        for side in range(2):
            for h in range(2):
                fill_part(level, side, h, h)

    to_core = pltpu.make_async_remote_copy(
        src_ref=rows_bf.at[1 - core],
        dst_ref=from_core,
        send_sem=core_sem.at[0],
        recv_sem=core_sem.at[1],
        device_id=partner,
        device_id_type=MESH,
    )
    margin = LEVELS * RIM

    def halo_copy(j, lr):
        start = 0 if lr == 0 else width - margin
        return pltpu.make_async_remote_copy(
            src_ref=rows_bf.at[j, :, pl.ds(start, margin), :],
            dst_ref=halo.at[core, lr],
            send_sem=halo_send.at[j, lr],
            recv_sem=halo_recv.at[core, lr],
            device_id={"sub": z * 2 + j, "rng": rng - 1 + 2 * lr},
            device_id_type=MESH,
        )

    def halo_wait(side, lr):
        return pltpu.make_async_remote_copy(
            src_ref=rows_bf.at[0, :, pl.ds(0, margin), :],
            dst_ref=halo.at[side, lr],
            send_sem=halo_send.at[0, lr],
            recv_sem=halo_recv.at[side, lr],
            device_id=partner,
            device_id_type=MESH,
        )

    @pl.when(core == 1)
    def _():
        pl.semaphore_wait(ready_core, 1)

    to_core.start()

    @pl.when(upper_rng)
    def _():
        for j in range(2):
            halo_copy(j, 1).start()

    load_taps.wait()
    load_shifts.wait()
    load_weights.wait()
    fill_wide(0)
    fill_table(0)

    @pl.when(lower_rng)
    def _():
        for j in range(2):
            pl.semaphore_wait(ready_rng.at[j], 1)
            halo_copy(j, 0).start()

    for ch in range(2):
        first[core, ch, pl.ds(margin, width), :] = rows_bf[core, ch].astype(F32)
    to_core.wait_recv()
    for ch in range(2):
        first[1 - core, ch, pl.ds(margin, width), :] = from_core[ch].astype(F32)

    def take_halo(lr):
        start, there = ((margin + width, upper_rng), (0, lower_rng))[lr]

        @pl.when(there)
        def _():
            for side in range(2):
                halo_wait(side, lr).wait_recv()
                for ch in range(2):
                    first[side, ch, pl.ds(start, margin), :] = halo[side, lr, ch].astype(F32)

        @pl.when(jnp.logical_not(there))
        def _():
            first[:, :, pl.ds(start, margin), :] = jnp.zeros((2, 2, margin, ANGLES), F32)

    def bits_of(row):
        code = row + RIM
        return [((code // v) % 2) == 1 for v in (1, 2, 4, 8)]

    def shift_row(level, side):
        return shifts[level, pl.ds(side, 1), :]

    def interpolate(load, rows, bits, level):
        n = rows + 8
        b0, b1, b2, b3 = bits
        v = jnp.where(
            b3,
            jnp.where(b2, load(12, n), load(8, n)),
            jnp.where(b2, load(4, n), load(0, n)),
        )
        v = jnp.where(b0, pltpu.roll(v, n - 1, 0), v)
        v = jnp.where(b1, pltpu.roll(v, n - 2, 0), v)
        total = v * taps[level, 0]
        for t in range(1, TAPS):
            total = total + pltpu.roll(v, n - t, 0) * taps[level, t]
        return total[:rows].astype(BF16)

    def turn(level, h, start, rows, re, im):
        c = cos_t[level, h, pl.ds(start, rows), :]
        s = sin_t[level, h, pl.ds(start, rows), :]
        return re * c - im * s, re * s + im * c

    bits0 = [bits_of(shift_row(0, side)) for side in range(2)]
    rows1 = width + 2 * (margin - RIM)

    def level0(b, rows):
        parts = []
        for side in range(2):
            for ch in range(2):
                parts.append(interpolate(lambda o, n: first[side, ch, pl.ds(b + o, n), :], rows, bits0[side], 0))
        merged = jnp.dot(jnp.concatenate(parts, axis=1), wide[0], preferred_element_type=F32)
        start = (b - (margin - RIM)) % PERIOD
        for h in range(2):
            re, im = merged[:, h * 256 : h * 256 + 128], merged[:, h * 256 + 128 : h * 256 + 256]
            re, im = turn(0, h, start, rows, re, im)
            x1[h, 0, pl.ds(b, rows), :] = re
            x1[h, 1, pl.ds(b, rows), :] = im

    def clear1(start):
        x1[:, :, pl.ds(start, margin - RIM), :] = jnp.zeros((2, 2, margin - RIM, ANGLES), F32)

    own_bits1 = [((shift_row(1, side0) + RIM) // v) % 2 == 1 for v in (1, 2, 4, 8)]

    def nth(i):
        q = core * i + (1 - core) * (3 - i)
        chip = 4 * core + q
        own = jnp.logical_and(upper == core, quad == q)
        return q, own, device(chip, upper), order(chip, upper) > me

    ahead = jnp.logical_and(core == 1, jnp.logical_and(zl > 0, upper == 0))

    def in_copy(i, k):
        start, rows = CHUNK1[k]
        q, own, peer, later = nth(i)
        row = pl.multiple_of((q // 2) * hw + start, 32)
        return (
            y1.at[q % 2, :, pl.ds(row, rows), :],
            units.at[quad, :, pl.ds(start, rows), :],
            in_send.at[i, k],
            in_recv.at[quad, k],
            peer,
        )

    def send_unit(i, k):
        q, own, peer, later = nth(i)
        if k == 0:
            pl.when(later)(lambda: pl.semaphore_wait(ready_in.at[q], 1))
        start_copy(in_copy(i, k), own)

    def remote(src, dst, send, recv, peer):
        return pltpu.make_async_remote_copy(
            src_ref=src, dst_ref=dst, send_sem=send, recv_sem=recv, device_id=peer, device_id_type=MESH
        )

    def start_copy(parts, local):
        src, dst, send, recv, peer = parts

        @pl.when(local)
        def _():
            pltpu.make_async_copy(src, dst, recv).start()

        @pl.when(jnp.logical_not(local))
        def _():
            remote(*parts).start()

    def wait_sent(parts, local):
        @pl.when(jnp.logical_not(local))
        def _():
            remote(*parts).wait_send()

    for k in range(CHUNKS):
        level0(*ROWS0[k][0])
        if k == 0:
            take_halo(1)
        elif k == CHUNKS - 1:
            take_halo(0)
        level0(*ROWS0[k][1])
        if k == 0:
            pl.when(jnp.logical_not(lower_rng))(lambda: clear1(0))
        elif k == CHUNKS - 1:
            pl.when(jnp.logical_not(upper_rng))(lambda: clear1(rows1 - (margin - RIM)))
        start = CHUNK1[k][0]
        for part in range(2):
            if k == CHUNKS - 1 and part == 0:
                rows = hw - start
            else:
                rows = CHUNK1[k][1]
            for h in range(2):
                for ch in range(2):
                    at = part * hw + start
                    y1[h, ch, pl.ds(at, rows), :] = interpolate(
                        lambda o, n: x1[h, ch, pl.ds(at + o, n), :], rows, own_bits1, 1
                    )
        @pl.when(jnp.logical_not(ahead))
        def _():
            for i in range(3):
                send_unit(i, k)

        if k == CHUNKS - 1:
            @pl.when(ahead)
            def _():
                for i in range(3):
                    for each in range(CHUNKS):
                        send_unit(i, each)

        if k < CHUNKS - 1:
            pl.when(zl == 0)(lambda: send_unit(3, k))
        else:
            @pl.when(zl > 0)
            def _():
                for each in range(CHUNKS - 1):
                    send_unit(3, each)

            send_unit(3, k)

    fill_wide(1)
    fill_table(1)
    fill_wide(2)
    fill_table(2)
    for side in range(2):
        fill_part(3, side, core, 0)
    fill_phase(3, core, 0)

    bits2 = [bits_of(shift_row(2, side)) for side in range(2)]
    bits3 = bits_of(shift_row(3, core))
    at_start = jnp.logical_and(rng == 0, half == 0)
    at_end = jnp.logical_and(rng == last_rng, half == 1)

    def merge(level, lhs, start_row, rows, margin_rows, dst, slots):
        z = jnp.dot(lhs, wide[level], preferred_element_type=F32)
        start = (start_row - margin_rows) % PERIOD
        for h in range(2):
            re, im = turn(level, h, start, rows, z[:, h * 256 : h * 256 + 128], z[:, h * 256 + 128 : h * 256 + 256])
            dst[slots[h], 0, pl.ds(start_row, rows), :] = re
            dst[slots[h], 1, pl.ds(start_row, rows), :] = im

    def clear(dst, k, margin_rows):
        total = hw + 2 * margin_rows
        if 0 < k < CHUNKS - 1:
            return

        @pl.when(at_start if k == 0 else at_end)
        def _():
            at = 0 if k == 0 else total - margin_rows
            dst[:, :, pl.ds(at, margin_rows), :] = jnp.zeros((4, 2, margin_rows, ANGLES), F32)

    def pair_copy(k):
        start, rows = CHUNK3[k]
        ref = y3.at[core, :, :, pl.ds(start, rows), :]
        return pltpu.make_async_remote_copy(
            src_ref=ref, dst_ref=ref, send_sem=pair_send.at[k], recv_sem=pair_recv.at[k],
            device_id=partner, device_id_type=MESH,
        )

    def pair_wait(k):
        start, rows = CHUNK3[k]
        ref = y3.at[1 - core, :, :, pl.ds(start, rows), :]
        return pltpu.make_async_remote_copy(
            src_ref=ref, dst_ref=ref, send_sem=pair_send.at[k], recv_sem=pair_recv.at[k],
            device_id=partner, device_id_type=MESH,
        )

    def out_copy(q, k):
        start, rows = CHUNK3[k]
        row = pl.multiple_of(half * hw + start, 64)
        return (
            turned.at[q, :, pl.ds(start, rows), :],
            blocks.at[upper, :, pl.ds(row, rows), :],
            out_send.at[q, k],
            out_recv.at[zl // 2, k],
            out_dests[q],
        )

    def send_block(q, k):
        if k == 0:
            pl.when(out_later[q])(lambda: pl.semaphore_wait(ready_out.at[q], 1))
        start_copy(out_copy(q, k), out_self[q])

    for k in range(CHUNKS):
        start, rows = CHUNK1[k]
        for s in range(4):
            ref = units.at[s, :, pl.ds(start, rows), :]
            pltpu.make_async_remote_copy(
                src_ref=ref, dst_ref=ref, send_sem=in_send.at[0, k], recv_sem=in_recv.at[s, k],
                device_id=partner, device_id_type=MESH,
            ).wait_recv()
        for p in range(2):
            lhs = jnp.concatenate(
                [units[2 * p + side, ch, pl.ds(start, rows), :] for side in range(2) for ch in range(2)], axis=1
            )
            merge(1, lhs, start, rows, 2 * RIM, x2, (2 * p, 2 * p + 1))
        clear(x2, k, 2 * RIM)
        start, rows = CHUNK2[k]
        for p in range(2):
            lhs = jnp.concatenate(
                [
                    interpolate(lambda o, n: x2[p + 2 * side, ch, pl.ds(start + o, n), :], rows, bits2[side], 2)
                    for side in range(2)
                    for ch in range(2)
                ],
                axis=1,
            )
            merge(2, lhs, start, rows, RIM, x3, (p, p + 2))
        clear(x3, k, RIM)
        start, rows = CHUNK3[k]
        for s in range(4):
            for ch in range(2):
                y3[core, s, ch, pl.ds(start, rows), :] = interpolate(
                    lambda o, n: x3[s, ch, pl.ds(start + o, n), :], rows, bits3, 3
                )
        pair_copy(k).start()
        pair_wait(k).wait_recv()
        for s in range(4):
            lhs = jnp.concatenate(
                [y3[side, s, ch, pl.ds(start, rows), :] for side in range(2) for ch in range(2)], axis=1
            )
            merged = jnp.dot(lhs, wide[3, :, pl.ds(0, 256)], preferred_element_type=F32)
            re, im = turn(3, 0, start % PERIOD, rows, merged[:, :128], merged[:, 128:])
            turned[s, 0, pl.ds(start, rows), :] = re.astype(BF16)
            turned[s, 1, pl.ds(start, rows), :] = im.astype(BF16)
        for q in range(3):
            send_block(q, k)
    for k in range(CHUNKS):
        send_block(3, k)

    def block_wait(s, k):
        start, rows = CHUNK3[k]
        ref = blocks.at[s // 2, :, pl.ds((s % 2) * hw + start, rows), :]
        remote(ref, ref, out_send.at[0, k], out_recv.at[s, k], partner).wait_recv()

    for first_chunk, last_chunk, col in ((0, 1, 0), (2, 2, 128)):
        for s in range(4):
            for k in range(first_chunk, last_chunk + 1):
                block_wait(s, k)
            at = (s % 2) * hw + col
            for ch in range(2):
                block = blocks[s // 2, ch, pl.ds(at, 128), :].astype(F32).T
                out[ch, s // 2, :, pl.ds(at, 128)] = block.astype(BF16)

    to_core.wait_send()
    for j in range(2):
        @pl.when(lower_rng)
        def _():
            halo_copy(j, 0).wait_send()

        @pl.when(upper_rng)
        def _():
            halo_copy(j, 1).wait_send()

    for k in range(CHUNKS):
        for i in range(4):
            wait_sent(in_copy(i, k), nth(i)[1])
        pair_copy(k).wait_send()
        for q in range(4):
            wait_sent(out_copy(q, k), out_self[q])


def on_device(image, interp_weights, range_taps, range_shifts):
    width = image.shape[3]
    hw = width // 2
    margin = LEVELS * RIM
    dma = pltpu.SemaphoreType.DMA
    vmem = pltpu.VMEM
    return pl.pallas_call(
        kernel,
        out_shape=pltpu.VMEM(image.shape, image.dtype),
        in_specs=[
            pl.BlockSpec(memory_space=pl.ANY),
            pl.BlockSpec(memory_space=pl.ANY),
            pl.BlockSpec(memory_space=pl.ANY),
            pl.BlockSpec(memory_space=pl.ANY),
        ],
        out_specs=pl.BlockSpec(memory_space=pltpu.VMEM),
        scratch_shapes=[
            vmem(image.shape, BF16),
            vmem(interp_weights.shape, BF16),
            pltpu.SMEM(range_taps.shape, F32),
            vmem(range_shifts.shape, jnp.int32),
            vmem((LEVELS, 512, 512), BF16),
            vmem((LEVELS, 2, TABLE, ANGLES), F32),
            vmem((LEVELS, 2, TABLE, ANGLES), F32),
            vmem((2, 2, width, ANGLES), BF16),
            vmem((2, 2, width + 2 * margin + 16, ANGLES), F32),
            vmem((2, width, ANGLES), BF16),
            vmem((2, 2, 2, margin, ANGLES), BF16),
            vmem((2, 2, width + 6 * RIM + 16, ANGLES), F32),
            vmem((2, 2, width + 4 * RIM, ANGLES), BF16),
            vmem((4, 2, hw + 4 * RIM, ANGLES), BF16),
            vmem((4, 2, hw + 4 * RIM + 16, ANGLES), F32),
            vmem((4, 2, hw + 2 * RIM + 16, ANGLES), F32),
            vmem((2, 4, 2, hw, ANGLES), BF16),
            vmem((4, 2, hw, ANGLES), BF16),
            vmem((2, 2, width, ANGLES), BF16),
            dma((4,)),
            dma((2,)),
            dma((2, 2)),
            dma((2, 2)),
            dma((4, CHUNKS)),
            dma((4, CHUNKS)),
            dma((CHUNKS,)),
            dma((CHUNKS,)),
            dma((4, CHUNKS)),
            dma((4, CHUNKS)),
            pltpu.SemaphoreType.REGULAR,
            pltpu.SemaphoreType.REGULAR((2,)),
            pltpu.SemaphoreType.REGULAR((4,)),
            pltpu.SemaphoreType.REGULAR((4,)),
        ],
        compiler_params=pltpu.CompilerParams(collective_id=0, has_side_effects=True),
        name="backprojection",
    )(image, interp_weights, range_taps, range_shifts)


def solution(mesh):
    return jax.shard_map(
        on_device,
        mesh=mesh,
        in_specs=(P(None, ("img", "sub"), None, "rng"), P(), P(), P()),
        out_specs=P(None, ("img", "sub"), None, "rng"),
        check_vma=False,
    )
```

```python
import math

import jax
import jax.numpy as jnp
from jax import lax
from jax.experimental import pallas as pl
from jax.experimental.pallas import tpu as pltpu
from jax.sharding import PartitionSpec as P

ANGLES = 128
RIM = 8
TAPS = 4
LEVELS = 4
PERIOD = 64
PHASE_STEP = 2.0 * math.pi / PERIOD

MESH = pl.DeviceIdType.MESH
F32 = jnp.float32
BF16 = jnp.bfloat16

CHUNK1 = ((0, 64), (64, 64), (128, 64), (192, 96))
CHUNK2 = ((0, 48), (48, 64), (112, 64), (176, 96))
CHUNK3 = ((0, 32), (32, 64), (96, 64), (160, 96))
CHUNKS = len(CHUNK3)
ROWS0 = (((256, 80), (0, 80)), ((80, 64), (336, 64)), ((144, 64), (400, 64)), ((208, 48), (464, 96)))
TABLE = 256


def kernel(
    image_hbm, weights_hbm, taps_hbm, shifts_hbm, out,
    image, weights, taps, shifts, wide, cos_t, sin_t,
    rows_bf, first, from_core, halo, x1, y1, units, x2, x3, y3, turned, blocks,
    load_sem, core_sem, halo_send, halo_recv, in_send, in_recv, pair_send, pair_recv, out_send, out_recv,
    ready_core, ready_rng, ready_in, ready_out,
):
    sub = lax.axis_index("sub")
    rng = lax.axis_index("rng")
    last_rng = lax.axis_size("rng") - 1
    core = sub % 2
    z = sub // 2
    zl = z % 8
    base = z - zl
    quad = zl % 4
    upper = zl // 4
    half = (zl // 2) % 2
    side0 = zl % 2
    width = image.shape[3]
    hw = width // 2

    load_image = pltpu.make_async_copy(image_hbm, image, load_sem.at[0])
    load_weights = pltpu.make_async_copy(weights_hbm, weights, load_sem.at[1])
    load_taps = pltpu.make_async_copy(taps_hbm, taps, load_sem.at[2])
    load_shifts = pltpu.make_async_copy(shifts_hbm, shifts, load_sem.at[3])
    load_image.start()
    load_weights.start()
    load_taps.start()
    load_shifts.start()

    def device(z_local, core_index):
        return {"sub": (base + z_local) * 2 + core_index}

    def order(z_local, core_index):
        return jnp.where(z_local * 2 + core_index == 0, 16, z_local * 2 + (1 - core_index))

    me = order(zl, core)
    partner = {"sub": z * 2 + (1 - core)}
    in_chips = [4 * core + q for q in range(4)]
    in_self = [jnp.logical_and(upper == core, quad == q) for q in range(4)]
    in_peers = [device(chip, upper) for chip in in_chips]
    in_later = [order(chip, upper) > me for chip in in_chips]
    out_self = [jnp.logical_and(in_self[q], side0 == core) for q in range(4)]
    out_dests = [device(chip, side0) for chip in in_chips]
    out_later = [order(chip, side0) > me for chip in in_chips]
    source_chips = [2 * k + core for k in range(4)]
    source_self = [jnp.logical_and(zl == source_chips[k], upper == core) for k in range(4)]
    out_sources = [device(chip, upper) for chip in source_chips]
    source_later = [order(chip, upper) > me for chip in source_chips]
    lower_rng, upper_rng = rng > 0, rng < last_rng

    barrier = pltpu.get_barrier_semaphore()

    def greet(who):
        pl.semaphore_signal(barrier, inc=1, device_id=who, device_id_type=MESH)

    def answer(sem, who):
        pl.semaphore_signal(sem, inc=1, device_id=who, device_id_type=MESH)

    def earlier(later, own):
        return jnp.logical_not(jnp.logical_or(later, own))

    @pl.when(core == 1)
    def _():
        greet(partner)

    @pl.when(lower_rng)
    def _():
        for c in range(2):
            greet({"sub": z * 2 + c, "rng": rng - 1})

    for peers, later in ((in_peers, in_later), (out_dests, out_later), (out_sources, source_later)):
        for q in range(4):
            @pl.when(later[q])
            def _():
                greet(peers[q])

    count = jnp.where(core == 0, 1, 0) + jnp.where(upper_rng, 2, 0)
    for later, own in ((in_later, in_self), (out_later, out_self), (source_later, source_self)):
        for q in range(4):
            count = count + jnp.where(earlier(later[q], own[q]), 1, 0)

    def enter():
        pl.when(count > 0)(lambda: pl.semaphore_wait(barrier, count))

        @pl.when(upper_rng)
        def _():
            for c in range(2):
                answer(ready_rng.at[core], {"sub": z * 2 + c, "rng": rng + 1})

        @pl.when(core == 0)
        def _():
            answer(ready_core, partner)

        for q in range(4):
            @pl.when(earlier(in_later[q], in_self[q]))
            def _():
                answer(ready_in.at[quad], in_peers[q])

            @pl.when(earlier(source_later[q], source_self[q]))
            def _():
                answer(ready_out.at[quad], out_sources[q])

    last_to_enter = jnp.logical_and(zl == 0, core == 0)
    pl.when(last_to_enter)(enter)

    def fill_phase(level, h, place):
        r = lax.broadcasted_iota(jnp.int32, (PERIOD, ANGLES), 0)
        a = lax.broadcasted_iota(jnp.int32, (PERIOD, ANGLES), 1)
        phase = ((r * (h * ANGLES + a + 1) * (7 + level)) % PERIOD).astype(F32) * PHASE_STEP
        c, s = jnp.cos(phase), jnp.sin(phase)
        for i in range(TABLE // PERIOD):
            cos_t[level, place, pl.ds(i * PERIOD, PERIOD), :] = c
            sin_t[level, place, pl.ds(i * PERIOD, PERIOD), :] = s

    def fill_table(level):
        for h in range(2):
            fill_phase(level, h, h)

    load_image.wait()

    for ch in range(2):
        for j in range(2):
            for k in range(width // 128):
                block = image[ch, j, :, pl.ds(k * 128, 128)].astype(F32).T
                rows_bf[j, ch, pl.ds(k * 128, 128), :] = block.astype(BF16)

    pl.when(jnp.logical_not(last_to_enter))(enter)

    def fill_part(level, side, h, place):
        wr = weights[level, side, h, 0].astype(F32).T.astype(BF16)
        wi = weights[level, side, h, 1].astype(F32).T.astype(BF16)
        for c, x, value in ((0, 0, wr), (1, 0, -wi), (0, 1, wi), (1, 1, wr)):
            wide[level, pl.ds((side * 2 + c) * 128, 128), pl.ds((place * 2 + x) * 128, 128)] = value

    def fill_wide(level):
        for side in range(2):
            for h in range(2):
                fill_part(level, side, h, h)

    to_core = pltpu.make_async_remote_copy(
        src_ref=rows_bf.at[1 - core],
        dst_ref=from_core,
        send_sem=core_sem.at[0],
        recv_sem=core_sem.at[1],
        device_id=partner,
        device_id_type=MESH,
    )
    margin = LEVELS * RIM

    def halo_copy(j, lr):
        start = 0 if lr == 0 else width - margin
        return pltpu.make_async_remote_copy(
            src_ref=rows_bf.at[j, :, pl.ds(start, margin), :],
            dst_ref=halo.at[core, lr],
            send_sem=halo_send.at[j, lr],
            recv_sem=halo_recv.at[core, lr],
            device_id={"sub": z * 2 + j, "rng": rng - 1 + 2 * lr},
            device_id_type=MESH,
        )

    def halo_wait(side, lr):
        return pltpu.make_async_remote_copy(
            src_ref=rows_bf.at[0, :, pl.ds(0, margin), :],
            dst_ref=halo.at[side, lr],
            send_sem=halo_send.at[0, lr],
            recv_sem=halo_recv.at[side, lr],
            device_id=partner,
            device_id_type=MESH,
        )

    @pl.when(core == 1)
    def _():
        pl.semaphore_wait(ready_core, 1)

    to_core.start()

    @pl.when(upper_rng)
    def _():
        for j in range(2):
            halo_copy(j, 1).start()

    load_taps.wait()
    load_shifts.wait()
    load_weights.wait()
    fill_wide(0)
    fill_table(0)

    @pl.when(lower_rng)
    def _():
        for j in range(2):
            pl.semaphore_wait(ready_rng.at[j], 1)
            halo_copy(j, 0).start()

    for ch in range(2):
        first[core, ch, pl.ds(margin, width), :] = rows_bf[core, ch].astype(F32)
    to_core.wait_recv()
    for ch in range(2):
        first[1 - core, ch, pl.ds(margin, width), :] = from_core[ch].astype(F32)

    def take_halo(lr):
        start, there = ((margin + width, upper_rng), (0, lower_rng))[lr]

        @pl.when(there)
        def _():
            for side in range(2):
                halo_wait(side, lr).wait_recv()
                for ch in range(2):
                    first[side, ch, pl.ds(start, margin), :] = halo[side, lr, ch].astype(F32)

        @pl.when(jnp.logical_not(there))
        def _():
            first[:, :, pl.ds(start, margin), :] = jnp.zeros((2, 2, margin, ANGLES), F32)

    def bits_of(row):
        code = row + RIM
        return [((code // v) % 2) == 1 for v in (1, 2, 4, 8)]

    def shift_row(level, side):
        return shifts[level, pl.ds(side, 1), :]

    def interpolate(load, rows, bits, level):
        n = rows + 8
        b0, b1, b2, b3 = bits
        v = jnp.where(
            b3,
            jnp.where(b2, load(12, n), load(8, n)),
            jnp.where(b2, load(4, n), load(0, n)),
        )
        v = jnp.where(b0, pltpu.roll(v, n - 1, 0), v)
        v = jnp.where(b1, pltpu.roll(v, n - 2, 0), v)
        total = v * taps[level, 0]
        for t in range(1, TAPS):
            total = total + pltpu.roll(v, n - t, 0) * taps[level, t]
        return total[:rows].astype(BF16)

    def turn(level, h, start, rows, re, im):
        c = cos_t[level, h, pl.ds(start, rows), :]
        s = sin_t[level, h, pl.ds(start, rows), :]
        return re * c - im * s, re * s + im * c

    bits0 = [bits_of(shift_row(0, side)) for side in range(2)]
    rows1 = width + 2 * (margin - RIM)

    def level0(b, rows):
        parts = []
        for side in range(2):
            for ch in range(2):
                parts.append(interpolate(lambda o, n: first[side, ch, pl.ds(b + o, n), :], rows, bits0[side], 0))
        merged = jnp.dot(jnp.concatenate(parts, axis=1), wide[0], preferred_element_type=F32)
        start = (b - (margin - RIM)) % PERIOD
        for h in range(2):
            re, im = merged[:, h * 256 : h * 256 + 128], merged[:, h * 256 + 128 : h * 256 + 256]
            re, im = turn(0, h, start, rows, re, im)
            x1[h, 0, pl.ds(b, rows), :] = re
            x1[h, 1, pl.ds(b, rows), :] = im

    def clear1(start):
        x1[:, :, pl.ds(start, margin - RIM), :] = jnp.zeros((2, 2, margin - RIM, ANGLES), F32)

    own_bits1 = [((shift_row(1, side0) + RIM) // v) % 2 == 1 for v in (1, 2, 4, 8)]

    def nth(i):
        q = jnp.where(jnp.logical_and(core == 1, zl > 0), i, 3 - i)
        chip = 4 * core + q
        own = jnp.logical_and(upper == core, quad == q)
        return q, own, device(chip, upper), order(chip, upper) > me

    ahead = jnp.logical_and(core == 1, jnp.logical_and(zl > 0, upper == 0))

    def in_copy(i, k):
        start, rows = CHUNK1[k]
        q, own, peer, later = nth(i)
        row = pl.multiple_of((q // 2) * hw + start, 32)
        return (
            y1.at[q % 2, :, pl.ds(row, rows), :],
            units.at[quad, :, pl.ds(start, rows), :],
            in_send.at[i, k],
            in_recv.at[quad, k],
            peer,
        )

    def send_unit(i, k):
        q, own, peer, later = nth(i)
        if k == 0:
            pl.when(later)(lambda: pl.semaphore_wait(ready_in.at[q], 1))
        start_copy(in_copy(i, k), own)

    def remote(src, dst, send, recv, peer):
        return pltpu.make_async_remote_copy(
            src_ref=src, dst_ref=dst, send_sem=send, recv_sem=recv, device_id=peer, device_id_type=MESH
        )

    def start_copy(parts, local):
        src, dst, send, recv, peer = parts

        @pl.when(local)
        def _():
            pltpu.make_async_copy(src, dst, recv).start()

        @pl.when(jnp.logical_not(local))
        def _():
            remote(*parts).start()

    def wait_sent(parts, local):
        @pl.when(jnp.logical_not(local))
        def _():
            remote(*parts).wait_send()

    for k in range(CHUNKS):
        level0(*ROWS0[k][0])
        if k == 0:
            take_halo(1)
        elif k == CHUNKS - 1:
            take_halo(0)
        level0(*ROWS0[k][1])
        if k == 0:
            pl.when(jnp.logical_not(lower_rng))(lambda: clear1(0))
        elif k == CHUNKS - 1:
            pl.when(jnp.logical_not(upper_rng))(lambda: clear1(rows1 - (margin - RIM)))
        start = CHUNK1[k][0]
        for part in range(2):
            if k == CHUNKS - 1 and part == 0:
                rows = hw - start
            else:
                rows = CHUNK1[k][1]
            for h in range(2):
                for ch in range(2):
                    at = part * hw + start
                    y1[h, ch, pl.ds(at, rows), :] = interpolate(
                        lambda o, n: x1[h, ch, pl.ds(at + o, n), :], rows, own_bits1, 1
                    )
        @pl.when(jnp.logical_not(ahead))
        def _():
            for i in range(3):
                send_unit(i, k)

        if k == CHUNKS - 1:
            @pl.when(ahead)
            def _():
                for i in range(3):
                    for each in range(CHUNKS):
                        send_unit(i, each)

        if k < CHUNKS - 1:
            pl.when(zl == 0)(lambda: send_unit(3, k))
        else:
            @pl.when(zl > 0)
            def _():
                for each in range(CHUNKS - 1):
                    send_unit(3, each)

            send_unit(3, k)

    fill_wide(1)
    fill_table(1)
    fill_wide(2)
    fill_table(2)
    for side in range(2):
        fill_part(3, side, core, 0)
    fill_phase(3, core, 0)

    bits2 = [bits_of(shift_row(2, side)) for side in range(2)]
    bits3 = bits_of(shift_row(3, core))
    at_start = jnp.logical_and(rng == 0, half == 0)
    at_end = jnp.logical_and(rng == last_rng, half == 1)

    def merge(level, lhs, start_row, rows, margin_rows, dst, slots):
        z = jnp.dot(lhs, wide[level], preferred_element_type=F32)
        start = (start_row - margin_rows) % PERIOD
        for h in range(2):
            re, im = turn(level, h, start, rows, z[:, h * 256 : h * 256 + 128], z[:, h * 256 + 128 : h * 256 + 256])
            dst[slots[h], 0, pl.ds(start_row, rows), :] = re
            dst[slots[h], 1, pl.ds(start_row, rows), :] = im

    def clear(dst, k, margin_rows):
        total = hw + 2 * margin_rows
        if 0 < k < CHUNKS - 1:
            return

        @pl.when(at_start if k == 0 else at_end)
        def _():
            at = 0 if k == 0 else total - margin_rows
            dst[:, :, pl.ds(at, margin_rows), :] = jnp.zeros((4, 2, margin_rows, ANGLES), F32)

    def pair_copy(k):
        start, rows = CHUNK3[k]
        ref = y3.at[core, :, :, pl.ds(start, rows), :]
        return pltpu.make_async_remote_copy(
            src_ref=ref, dst_ref=ref, send_sem=pair_send.at[k], recv_sem=pair_recv.at[k],
            device_id=partner, device_id_type=MESH,
        )

    def pair_wait(k):
        start, rows = CHUNK3[k]
        ref = y3.at[1 - core, :, :, pl.ds(start, rows), :]
        return pltpu.make_async_remote_copy(
            src_ref=ref, dst_ref=ref, send_sem=pair_send.at[k], recv_sem=pair_recv.at[k],
            device_id=partner, device_id_type=MESH,
        )

    def out_copy(q, k):
        start, rows = CHUNK3[k]
        row = pl.multiple_of(half * hw + start, 32)
        return (
            turned.at[q, :, pl.ds(start, rows), :],
            blocks.at[upper, :, pl.ds(row, rows), :],
            out_send.at[q, k],
            out_recv.at[zl // 2, k],
            out_dests[q],
        )

    def send_block(q, k):
        if k == 0:
            pl.when(out_later[q])(lambda: pl.semaphore_wait(ready_out.at[q], 1))
        start_copy(out_copy(q, k), out_self[q])

    for k in range(CHUNKS):
        start, rows = CHUNK1[k]
        for s in range(4):
            ref = units.at[s, :, pl.ds(start, rows), :]
            pltpu.make_async_remote_copy(
                src_ref=ref, dst_ref=ref, send_sem=in_send.at[0, k], recv_sem=in_recv.at[s, k],
                device_id=partner, device_id_type=MESH,
            ).wait_recv()
        for p in range(2):
            lhs = jnp.concatenate(
                [units[2 * p + side, ch, pl.ds(start, rows), :] for side in range(2) for ch in range(2)], axis=1
            )
            merge(1, lhs, start, rows, 2 * RIM, x2, (2 * p, 2 * p + 1))
        clear(x2, k, 2 * RIM)
        start, rows = CHUNK2[k]
        for p in range(2):
            lhs = jnp.concatenate(
                [
                    interpolate(lambda o, n: x2[p + 2 * side, ch, pl.ds(start + o, n), :], rows, bits2[side], 2)
                    for side in range(2)
                    for ch in range(2)
                ],
                axis=1,
            )
            merge(2, lhs, start, rows, RIM, x3, (p, p + 2))
        clear(x3, k, RIM)
        start, rows = CHUNK3[k]
        for s in range(4):
            for ch in range(2):
                y3[core, s, ch, pl.ds(start, rows), :] = interpolate(
                    lambda o, n: x3[s, ch, pl.ds(start + o, n), :], rows, bits3, 3
                )
        pair_copy(k).start()
        pair_wait(k).wait_recv()
        for s in range(4):
            lhs = jnp.concatenate(
                [y3[side, s, ch, pl.ds(start, rows), :] for side in range(2) for ch in range(2)], axis=1
            )
            merged = jnp.dot(lhs, wide[3, :, pl.ds(0, 256)], preferred_element_type=F32)
            re, im = turn(3, 0, start % PERIOD, rows, merged[:, :128], merged[:, 128:])
            turned[s, 0, pl.ds(start, rows), :] = re.astype(BF16)
            turned[s, 1, pl.ds(start, rows), :] = im.astype(BF16)
        for q in range(3):
            send_block(q, k)
    for k in range(CHUNKS):
        send_block(3, k)

    def block_wait(s, k):
        start, rows = CHUNK3[k]
        ref = blocks.at[s // 2, :, pl.ds((s % 2) * hw + start, rows), :]
        remote(ref, ref, out_send.at[0, k], out_recv.at[s, k], partner).wait_recv()

    for first_chunk, last_chunk, col in ((0, 2, 0), (3, 3, 128)):
        for s in range(4):
            for k in range(first_chunk, last_chunk + 1):
                block_wait(s, k)
            at = (s % 2) * hw + col
            for ch in range(2):
                block = blocks[s // 2, ch, pl.ds(at, 128), :].astype(F32).T
                out[ch, s // 2, :, pl.ds(at, 128)] = block.astype(BF16)

    to_core.wait_send()
    for j in range(2):
        @pl.when(lower_rng)
        def _():
            halo_copy(j, 0).wait_send()

        @pl.when(upper_rng)
        def _():
            halo_copy(j, 1).wait_send()

    for k in range(CHUNKS):
        for i in range(4):
            wait_sent(in_copy(i, k), nth(i)[1])
        pair_copy(k).wait_send()
        for q in range(4):
            wait_sent(out_copy(q, k), out_self[q])


def on_device(image, interp_weights, range_taps, range_shifts):
    width = image.shape[3]
    hw = width // 2
    margin = LEVELS * RIM
    dma = pltpu.SemaphoreType.DMA
    vmem = pltpu.VMEM
    return pl.pallas_call(
        kernel,
        out_shape=pltpu.VMEM(image.shape, image.dtype),
        in_specs=[
            pl.BlockSpec(memory_space=pl.ANY),
            pl.BlockSpec(memory_space=pl.ANY),
            pl.BlockSpec(memory_space=pl.ANY),
            pl.BlockSpec(memory_space=pl.ANY),
        ],
        out_specs=pl.BlockSpec(memory_space=pltpu.VMEM),
        scratch_shapes=[
            vmem(image.shape, BF16),
            vmem(interp_weights.shape, BF16),
            pltpu.SMEM(range_taps.shape, F32),
            vmem(range_shifts.shape, jnp.int32),
            vmem((LEVELS, 512, 512), BF16),
            vmem((LEVELS, 2, TABLE, ANGLES), F32),
            vmem((LEVELS, 2, TABLE, ANGLES), F32),
            vmem((2, 2, width, ANGLES), BF16),
            vmem((2, 2, width + 2 * margin + 16, ANGLES), F32),
            vmem((2, width, ANGLES), BF16),
            vmem((2, 2, 2, margin, ANGLES), BF16),
            vmem((2, 2, width + 6 * RIM + 16, ANGLES), F32),
            vmem((2, 2, width + 4 * RIM, ANGLES), BF16),
            vmem((4, 2, hw + 4 * RIM, ANGLES), BF16),
            vmem((4, 2, hw + 4 * RIM + 16, ANGLES), F32),
            vmem((4, 2, hw + 2 * RIM + 16, ANGLES), F32),
            vmem((2, 4, 2, hw, ANGLES), BF16),
            vmem((4, 2, hw, ANGLES), BF16),
            vmem((2, 2, width, ANGLES), BF16),
            dma((4,)),
            dma((2,)),
            dma((2, 2)),
            dma((2, 2)),
            dma((4, CHUNKS)),
            dma((4, CHUNKS)),
            dma((CHUNKS,)),
            dma((CHUNKS,)),
            dma((4, CHUNKS)),
            dma((4, CHUNKS)),
            pltpu.SemaphoreType.REGULAR,
            pltpu.SemaphoreType.REGULAR((2,)),
            pltpu.SemaphoreType.REGULAR((4,)),
            pltpu.SemaphoreType.REGULAR((4,)),
        ],
        compiler_params=pltpu.CompilerParams(collective_id=0, has_side_effects=True),
        name="backprojection",
    )(image, interp_weights, range_taps, range_shifts)


def solution(mesh):
    return jax.shard_map(
        on_device,
        mesh=mesh,
        in_specs=(P(None, ("img", "sub"), None, "rng"), P(), P(), P()),
        out_specs=P(None, ("img", "sub"), None, "rng"),
        check_vma=False,
    )
```

```python
import math

import jax
import jax.numpy as jnp
from jax import lax
from jax.experimental import pallas as pl
from jax.experimental.pallas import tpu as pltpu
from jax.sharding import PartitionSpec as P

ANGLES = 128
RIM = 8
TAPS = 4
LEVELS = 4
PERIOD = 64
PHASE_STEP = 2.0 * math.pi / PERIOD

MESH = pl.DeviceIdType.MESH
F32 = jnp.float32
BF16 = jnp.bfloat16

CHUNK1 = ((0, 96), (96, 64), (160, 128))
CHUNK2 = ((0, 80), (80, 64), (144, 128))
CHUNK3 = ((0, 64), (64, 64), (128, 128))
CHUNKS = len(CHUNK3)
ROWS0 = (((256, 112), (0, 112)), ((112, 64), (368, 64)), ((176, 80), (432, 128)))
TABLE = 256


def kernel(
    image_hbm, weights_hbm, taps_hbm, shifts_hbm, out,
    image, weights, taps, shifts, wide, cos_t, sin_t,
    rows_bf, first, from_core, halo, x1, y1, units, x2, x3, y3, turned, blocks,
    load_sem, core_sem, halo_send, halo_recv, in_send, in_recv, pair_send, pair_recv, out_send, out_recv,
    ready_core, ready_rng, ready_in, ready_out,
):
    sub = lax.axis_index("sub")
    rng = lax.axis_index("rng")
    last_rng = lax.axis_size("rng") - 1
    core = sub % 2
    z = sub // 2
    zl = z % 8
    base = z - zl
    quad = zl % 4
    upper = zl // 4
    half = (zl // 2) % 2
    side0 = zl % 2
    width = image.shape[3]
    hw = width // 2

    def load_image(j, place):
        return pltpu.make_async_copy(image_hbm.at[:, j], image.at[:, j], load_sem.at[place])

    load_weights = pltpu.make_async_copy(weights_hbm, weights, load_sem.at[1])
    load_taps = pltpu.make_async_copy(taps_hbm, taps, load_sem.at[2])
    load_shifts = pltpu.make_async_copy(shifts_hbm, shifts, load_sem.at[3])
    load_image(1 - core, 0).start()
    load_image(core, 4).start()
    load_weights.start()
    load_taps.start()
    load_shifts.start()

    def device(z_local, core_index):
        return {"sub": (base + z_local) * 2 + core_index}

    def order(z_local, core_index):
        return jnp.where(z_local * 2 + core_index == 0, 16, z_local * 2 + (1 - core_index))

    me = order(zl, core)
    partner = {"sub": z * 2 + (1 - core)}
    in_chips = [4 * core + q for q in range(4)]
    in_self = [jnp.logical_and(upper == core, quad == q) for q in range(4)]
    in_peers = [device(chip, upper) for chip in in_chips]
    in_later = [order(chip, upper) > me for chip in in_chips]
    out_self = [jnp.logical_and(in_self[q], side0 == core) for q in range(4)]
    out_dests = [device(chip, side0) for chip in in_chips]
    out_later = [order(chip, side0) > me for chip in in_chips]
    source_chips = [2 * k + core for k in range(4)]
    source_self = [jnp.logical_and(zl == source_chips[k], upper == core) for k in range(4)]
    out_sources = [device(chip, upper) for chip in source_chips]
    source_later = [order(chip, upper) > me for chip in source_chips]
    lower_rng, upper_rng = rng > 0, rng < last_rng

    barrier = pltpu.get_barrier_semaphore()

    def greet(who):
        pl.semaphore_signal(barrier, inc=1, device_id=who, device_id_type=MESH)

    def answer(sem, who):
        pl.semaphore_signal(sem, inc=1, device_id=who, device_id_type=MESH)

    def earlier(later, own):
        return jnp.logical_not(jnp.logical_or(later, own))

    @pl.when(core == 1)
    def _():
        greet(partner)

    @pl.when(lower_rng)
    def _():
        for c in range(2):
            greet({"sub": z * 2 + c, "rng": rng - 1})

    for peers, later in ((in_peers, in_later), (out_dests, out_later), (out_sources, source_later)):
        for q in range(4):
            @pl.when(later[q])
            def _():
                greet(peers[q])

    count = jnp.where(core == 0, 1, 0) + jnp.where(upper_rng, 2, 0)
    for later, own in ((in_later, in_self), (out_later, out_self), (source_later, source_self)):
        for q in range(4):
            count = count + jnp.where(earlier(later[q], own[q]), 1, 0)

    def enter():
        pl.when(count > 0)(lambda: pl.semaphore_wait(barrier, count))

        @pl.when(upper_rng)
        def _():
            for c in range(2):
                answer(ready_rng.at[core], {"sub": z * 2 + c, "rng": rng + 1})

        @pl.when(core == 0)
        def _():
            answer(ready_core, partner)

        for q in range(4):
            @pl.when(earlier(in_later[q], in_self[q]))
            def _():
                answer(ready_in.at[quad], in_peers[q])

            @pl.when(earlier(source_later[q], source_self[q]))
            def _():
                answer(ready_out.at[quad], out_sources[q])

    last_to_enter = jnp.logical_and(zl == 0, core == 0)
    pl.when(last_to_enter)(enter)

    def fill_phase(level, h, place):
        r = lax.broadcasted_iota(jnp.int32, (PERIOD, ANGLES), 0)
        a = lax.broadcasted_iota(jnp.int32, (PERIOD, ANGLES), 1)
        phase = ((r * (h * ANGLES + a + 1) * (7 + level)) % PERIOD).astype(F32) * PHASE_STEP
        c, s = jnp.cos(phase), jnp.sin(phase)
        for i in range(TABLE // PERIOD):
            cos_t[level, place, pl.ds(i * PERIOD, PERIOD), :] = c
            sin_t[level, place, pl.ds(i * PERIOD, PERIOD), :] = s

    def fill_table(level):
        for h in range(2):
            fill_phase(level, h, h)

    def transpose(j):
        for ch in range(2):
            for k in range(width // 128):
                block = image[ch, j, :, pl.ds(k * 128, 128)].astype(F32).T
                rows_bf[j, ch, pl.ds(k * 128, 128), :] = block.astype(BF16)

    load_image(1 - core, 0).wait()
    transpose(1 - core)
    pl.when(jnp.logical_not(last_to_enter))(enter)

    def fill_part(level, side, h, place):
        wr = weights[level, side, h, 0].astype(F32).T.astype(BF16)
        wi = weights[level, side, h, 1].astype(F32).T.astype(BF16)
        for c, x, value in ((0, 0, wr), (1, 0, -wi), (0, 1, wi), (1, 1, wr)):
            wide[level, pl.ds((side * 2 + c) * 128, 128), pl.ds((place * 2 + x) * 128, 128)] = value

    def fill_wide(level):
        for side in range(2):
            for h in range(2):
                fill_part(level, side, h, h)

    to_core = pltpu.make_async_remote_copy(
        src_ref=rows_bf.at[1 - core],
        dst_ref=from_core,
        send_sem=core_sem.at[0],
        recv_sem=core_sem.at[1],
        device_id=partner,
        device_id_type=MESH,
    )
    margin = LEVELS * RIM

    def halo_copy(j, lr):
        start = 0 if lr == 0 else width - margin
        return pltpu.make_async_remote_copy(
            src_ref=rows_bf.at[j, :, pl.ds(start, margin), :],
            dst_ref=halo.at[core, lr],
            send_sem=halo_send.at[j, lr],
            recv_sem=halo_recv.at[core, lr],
            device_id={"sub": z * 2 + j, "rng": rng - 1 + 2 * lr},
            device_id_type=MESH,
        )

    def halo_wait(side, lr):
        return pltpu.make_async_remote_copy(
            src_ref=rows_bf.at[0, :, pl.ds(0, margin), :],
            dst_ref=halo.at[side, lr],
            send_sem=halo_send.at[0, lr],
            recv_sem=halo_recv.at[side, lr],
            device_id=partner,
            device_id_type=MESH,
        )

    @pl.when(core == 1)
    def _():
        pl.semaphore_wait(ready_core, 1)

    to_core.start()
    load_image(core, 4).wait()
    transpose(core)

    @pl.when(upper_rng)
    def _():
        for j in range(2):
            halo_copy(j, 1).start()

    load_taps.wait()
    load_shifts.wait()
    load_weights.wait()
    fill_wide(0)
    fill_table(0)

    @pl.when(lower_rng)
    def _():
        for j in range(2):
            pl.semaphore_wait(ready_rng.at[j], 1)
            halo_copy(j, 0).start()

    for ch in range(2):
        first[core, ch, pl.ds(margin, width), :] = rows_bf[core, ch].astype(F32)
    to_core.wait_recv()
    for ch in range(2):
        first[1 - core, ch, pl.ds(margin, width), :] = from_core[ch].astype(F32)

    def take_halo(lr):
        start, there = ((margin + width, upper_rng), (0, lower_rng))[lr]

        @pl.when(there)
        def _():
            for side in range(2):
                halo_wait(side, lr).wait_recv()
                for ch in range(2):
                    first[side, ch, pl.ds(start, margin), :] = halo[side, lr, ch].astype(F32)

        @pl.when(jnp.logical_not(there))
        def _():
            first[:, :, pl.ds(start, margin), :] = jnp.zeros((2, 2, margin, ANGLES), F32)

    def bits_of(row):
        code = row + RIM
        return [((code // v) % 2) == 1 for v in (1, 2, 4, 8)]

    def shift_row(level, side):
        return shifts[level, pl.ds(side, 1), :]

    def interpolate(load, rows, bits, level):
        n = rows + 8
        b0, b1, b2, b3 = bits
        v = jnp.where(
            b3,
            jnp.where(b2, load(12, n), load(8, n)),
            jnp.where(b2, load(4, n), load(0, n)),
        )
        v = jnp.where(b0, pltpu.roll(v, n - 1, 0), v)
        v = jnp.where(b1, pltpu.roll(v, n - 2, 0), v)
        total = v * taps[level, 0]
        for t in range(1, TAPS):
            total = total + pltpu.roll(v, n - t, 0) * taps[level, t]
        return total[:rows].astype(BF16)

    def turn(level, h, start, rows, re, im):
        c = cos_t[level, h, pl.ds(start, rows), :]
        s = sin_t[level, h, pl.ds(start, rows), :]
        return re * c - im * s, re * s + im * c

    bits0 = [bits_of(shift_row(0, side)) for side in range(2)]
    rows1 = width + 2 * (margin - RIM)

    def level0(b, rows):
        parts = []
        for side in range(2):
            for ch in range(2):
                parts.append(interpolate(lambda o, n: first[side, ch, pl.ds(b + o, n), :], rows, bits0[side], 0))
        merged = jnp.dot(jnp.concatenate(parts, axis=1), wide[0], preferred_element_type=F32)
        start = (b - (margin - RIM)) % PERIOD
        for h in range(2):
            re, im = merged[:, h * 256 : h * 256 + 128], merged[:, h * 256 + 128 : h * 256 + 256]
            re, im = turn(0, h, start, rows, re, im)
            x1[h, 0, pl.ds(b, rows), :] = re
            x1[h, 1, pl.ds(b, rows), :] = im

    def clear1(start):
        x1[:, :, pl.ds(start, margin - RIM), :] = jnp.zeros((2, 2, margin - RIM, ANGLES), F32)

    own_bits1 = [((shift_row(1, side0) + RIM) // v) % 2 == 1 for v in (1, 2, 4, 8)]

    def nth(i):
        q = core * i + (1 - core) * (3 - i)
        chip = 4 * core + q
        own = jnp.logical_and(upper == core, quad == q)
        return q, own, device(chip, upper), order(chip, upper) > me

    ahead = jnp.logical_and(core == 1, jnp.logical_and(zl > 0, upper == 0))

    def in_copy(i, k):
        start, rows = CHUNK1[k]
        q, own, peer, later = nth(i)
        row = pl.multiple_of((q // 2) * hw + start, 32)
        return (
            y1.at[q % 2, :, pl.ds(row, rows), :],
            units.at[quad, :, pl.ds(start, rows), :],
            in_send.at[i, k],
            in_recv.at[quad, k],
            peer,
        )

    def send_unit(i, k):
        q, own, peer, later = nth(i)
        if k == 0:
            pl.when(later)(lambda: pl.semaphore_wait(ready_in.at[q], 1))
        start_copy(in_copy(i, k), own)

    def remote(src, dst, send, recv, peer):
        return pltpu.make_async_remote_copy(
            src_ref=src, dst_ref=dst, send_sem=send, recv_sem=recv, device_id=peer, device_id_type=MESH
        )

    def start_copy(parts, local):
        src, dst, send, recv, peer = parts

        @pl.when(local)
        def _():
            pltpu.make_async_copy(src, dst, recv).start()

        @pl.when(jnp.logical_not(local))
        def _():
            remote(*parts).start()

    def wait_sent(parts, local):
        @pl.when(jnp.logical_not(local))
        def _():
            remote(*parts).wait_send()

    for k in range(CHUNKS):
        level0(*ROWS0[k][0])
        if k == 0:
            take_halo(1)
        elif k == CHUNKS - 1:
            take_halo(0)
        level0(*ROWS0[k][1])
        if k == 0:
            pl.when(jnp.logical_not(lower_rng))(lambda: clear1(0))
        elif k == CHUNKS - 1:
            pl.when(jnp.logical_not(upper_rng))(lambda: clear1(rows1 - (margin - RIM)))
        start = CHUNK1[k][0]
        for part in range(2):
            if k == CHUNKS - 1 and part == 0:
                rows = hw - start
            else:
                rows = CHUNK1[k][1]
            for h in range(2):
                for ch in range(2):
                    at = part * hw + start
                    y1[h, ch, pl.ds(at, rows), :] = interpolate(
                        lambda o, n: x1[h, ch, pl.ds(at + o, n), :], rows, own_bits1, 1
                    )
        @pl.when(jnp.logical_not(ahead))
        def _():
            for i in range(3):
                send_unit(i, k)

        if k == CHUNKS - 1:
            @pl.when(ahead)
            def _():
                for i in range(3):
                    for each in range(CHUNKS):
                        send_unit(i, each)

        if k < CHUNKS - 1:
            pl.when(zl == 0)(lambda: send_unit(3, k))
        else:
            @pl.when(zl > 0)
            def _():
                for each in range(CHUNKS - 1):
                    send_unit(3, each)

            send_unit(3, k)

    fill_wide(1)
    fill_table(1)
    fill_wide(2)
    fill_table(2)
    for side in range(2):
        fill_part(3, side, core, 0)
    fill_phase(3, core, 0)

    bits2 = [bits_of(shift_row(2, side)) for side in range(2)]
    bits3 = bits_of(shift_row(3, core))
    at_start = jnp.logical_and(rng == 0, half == 0)
    at_end = jnp.logical_and(rng == last_rng, half == 1)

    def merge(level, lhs, start_row, rows, margin_rows, dst, slots):
        z = jnp.dot(lhs, wide[level], preferred_element_type=F32)
        start = (start_row - margin_rows) % PERIOD
        for h in range(2):
            re, im = turn(level, h, start, rows, z[:, h * 256 : h * 256 + 128], z[:, h * 256 + 128 : h * 256 + 256])
            dst[slots[h], 0, pl.ds(start_row, rows), :] = re
            dst[slots[h], 1, pl.ds(start_row, rows), :] = im

    def clear(dst, k, margin_rows):
        total = hw + 2 * margin_rows
        if 0 < k < CHUNKS - 1:
            return

        @pl.when(at_start if k == 0 else at_end)
        def _():
            at = 0 if k == 0 else total - margin_rows
            dst[:, :, pl.ds(at, margin_rows), :] = jnp.zeros((4, 2, margin_rows, ANGLES), F32)

    def pair_copy(k):
        start, rows = CHUNK3[k]
        ref = y3.at[core, :, :, pl.ds(start, rows), :]
        return pltpu.make_async_remote_copy(
            src_ref=ref, dst_ref=ref, send_sem=pair_send.at[k], recv_sem=pair_recv.at[k],
            device_id=partner, device_id_type=MESH,
        )

    def pair_wait(k):
        start, rows = CHUNK3[k]
        ref = y3.at[1 - core, :, :, pl.ds(start, rows), :]
        return pltpu.make_async_remote_copy(
            src_ref=ref, dst_ref=ref, send_sem=pair_send.at[k], recv_sem=pair_recv.at[k],
            device_id=partner, device_id_type=MESH,
        )

    def out_copy(q, k):
        start, rows = CHUNK3[k]
        row = pl.multiple_of(half * hw + start, 64)
        return (
            turned.at[q, :, pl.ds(start, rows), :],
            blocks.at[upper, :, pl.ds(row, rows), :],
            out_send.at[q, k],
            out_recv.at[zl // 2, k],
            out_dests[q],
        )

    def send_block(q, k):
        if k == 0:
            pl.when(out_later[q])(lambda: pl.semaphore_wait(ready_out.at[q], 1))
        start_copy(out_copy(q, k), out_self[q])

    for k in range(CHUNKS):
        start, rows = CHUNK1[k]
        for s in range(4):
            ref = units.at[s, :, pl.ds(start, rows), :]
            pltpu.make_async_remote_copy(
                src_ref=ref, dst_ref=ref, send_sem=in_send.at[0, k], recv_sem=in_recv.at[s, k],
                device_id=partner, device_id_type=MESH,
            ).wait_recv()
        for p in range(2):
            lhs = jnp.concatenate(
                [units[2 * p + side, ch, pl.ds(start, rows), :] for side in range(2) for ch in range(2)], axis=1
            )
            merge(1, lhs, start, rows, 2 * RIM, x2, (2 * p, 2 * p + 1))
        clear(x2, k, 2 * RIM)
        start, rows = CHUNK2[k]
        for p in range(2):
            lhs = jnp.concatenate(
                [
                    interpolate(lambda o, n: x2[p + 2 * side, ch, pl.ds(start + o, n), :], rows, bits2[side], 2)
                    for side in range(2)
                    for ch in range(2)
                ],
                axis=1,
            )
            merge(2, lhs, start, rows, RIM, x3, (p, p + 2))
        clear(x3, k, RIM)
        start, rows = CHUNK3[k]
        for s in range(4):
            for ch in range(2):
                y3[core, s, ch, pl.ds(start, rows), :] = interpolate(
                    lambda o, n: x3[s, ch, pl.ds(start + o, n), :], rows, bits3, 3
                )
        pair_copy(k).start()
        pair_wait(k).wait_recv()
        for s in range(4):
            lhs = jnp.concatenate(
                [y3[side, s, ch, pl.ds(start, rows), :] for side in range(2) for ch in range(2)], axis=1
            )
            merged = jnp.dot(lhs, wide[3, :, pl.ds(0, 256)], preferred_element_type=F32)
            re, im = turn(3, 0, start % PERIOD, rows, merged[:, :128], merged[:, 128:])
            turned[s, 0, pl.ds(start, rows), :] = re.astype(BF16)
            turned[s, 1, pl.ds(start, rows), :] = im.astype(BF16)
        for q in range(2):
            send_block(q, k)
    for q in range(2, 4):
        for k in range(CHUNKS):
            send_block(q, k)

    def block_wait(s, k):
        start, rows = CHUNK3[k]
        ref = blocks.at[s // 2, :, pl.ds((s % 2) * hw + start, rows), :]
        remote(ref, ref, out_send.at[0, k], out_recv.at[s, k], partner).wait_recv()

    for first_chunk, last_chunk, col in ((0, 1, 0), (2, 2, 128)):
        for s in range(4):
            for k in range(first_chunk, last_chunk + 1):
                block_wait(s, k)
            at = (s % 2) * hw + col
            for ch in range(2):
                block = blocks[s // 2, ch, pl.ds(at, 128), :].astype(F32).T
                out[ch, s // 2, :, pl.ds(at, 128)] = block.astype(BF16)

    to_core.wait_send()
    for j in range(2):
        @pl.when(lower_rng)
        def _():
            halo_copy(j, 0).wait_send()

        @pl.when(upper_rng)
        def _():
            halo_copy(j, 1).wait_send()

    for k in range(CHUNKS):
        for i in range(4):
            wait_sent(in_copy(i, k), nth(i)[1])
        pair_copy(k).wait_send()
        for q in range(4):
            wait_sent(out_copy(q, k), out_self[q])


def on_device(image, interp_weights, range_taps, range_shifts):
    width = image.shape[3]
    hw = width // 2
    margin = LEVELS * RIM
    dma = pltpu.SemaphoreType.DMA
    vmem = pltpu.VMEM
    return pl.pallas_call(
        kernel,
        out_shape=pltpu.VMEM(image.shape, image.dtype),
        in_specs=[
            pl.BlockSpec(memory_space=pl.ANY),
            pl.BlockSpec(memory_space=pl.ANY),
            pl.BlockSpec(memory_space=pl.ANY),
            pl.BlockSpec(memory_space=pl.ANY),
        ],
        out_specs=pl.BlockSpec(memory_space=pltpu.VMEM),
        scratch_shapes=[
            vmem(image.shape, BF16),
            vmem(interp_weights.shape, BF16),
            pltpu.SMEM(range_taps.shape, F32),
            vmem(range_shifts.shape, jnp.int32),
            vmem((LEVELS, 512, 512), BF16),
            vmem((LEVELS, 2, TABLE, ANGLES), F32),
            vmem((LEVELS, 2, TABLE, ANGLES), F32),
            vmem((2, 2, width, ANGLES), BF16),
            vmem((2, 2, width + 2 * margin + 16, ANGLES), F32),
            vmem((2, width, ANGLES), BF16),
            vmem((2, 2, 2, margin, ANGLES), BF16),
            vmem((2, 2, width + 6 * RIM + 16, ANGLES), F32),
            vmem((2, 2, width + 4 * RIM, ANGLES), BF16),
            vmem((4, 2, hw + 4 * RIM, ANGLES), BF16),
            vmem((4, 2, hw + 4 * RIM + 16, ANGLES), F32),
            vmem((4, 2, hw + 2 * RIM + 16, ANGLES), F32),
            vmem((2, 4, 2, hw, ANGLES), BF16),
            vmem((4, 2, hw, ANGLES), BF16),
            vmem((2, 2, width, ANGLES), BF16),
            dma((5,)),
            dma((2,)),
            dma((2, 2)),
            dma((2, 2)),
            dma((4, CHUNKS)),
            dma((4, CHUNKS)),
            dma((CHUNKS,)),
            dma((CHUNKS,)),
            dma((4, CHUNKS)),
            dma((4, CHUNKS)),
            pltpu.SemaphoreType.REGULAR,
            pltpu.SemaphoreType.REGULAR((2,)),
            pltpu.SemaphoreType.REGULAR((4,)),
            pltpu.SemaphoreType.REGULAR((4,)),
        ],
        compiler_params=pltpu.CompilerParams(collective_id=0, has_side_effects=True),
        name="backprojection",
    )(image, interp_weights, range_taps, range_shifts)


def solution(mesh):
    return jax.shard_map(
        on_device,
        mesh=mesh,
        in_specs=(P(None, ("img", "sub"), None, "rng"), P(), P(), P()),
        out_specs=P(None, ("img", "sub"), None, "rng"),
        check_vma=False,
    )
```

```python
import math

import jax
import jax.numpy as jnp
from jax import lax
from jax.experimental import pallas as pl
from jax.experimental.pallas import tpu as pltpu
from jax.sharding import PartitionSpec as P

ANGLES = 128
RIM = 8
TAPS = 4
LEVELS = 4
PERIOD = 64
PHASE_STEP = 2.0 * math.pi / PERIOD

MESH = pl.DeviceIdType.MESH
F32 = jnp.float32
BF16 = jnp.bfloat16

CHUNK1 = ((0, 96), (96, 64), (160, 128))
CHUNK2 = ((0, 80), (80, 64), (144, 128))
CHUNK3 = ((0, 64), (64, 64), (128, 128))
CHUNKS = len(CHUNK3)
ROWS0 = (((256, 112), (0, 112)), ((112, 64), (368, 64)), ((176, 80), (432, 128)))
TABLE = 256


def kernel(
    image_hbm, weights_hbm, taps_hbm, shifts_hbm, out,
    image, weights, taps, shifts, wide, cos_t, sin_t,
    rows_bf, first, from_core, halo, x1, y1, units, x2, x3, y3, turned, blocks,
    load_sem, core_sem, halo_send, halo_recv, in_send, in_recv, pair_send, pair_recv, out_send, out_recv,
    ready_core, ready_rng, ready_in, ready_out,
):
    sub = lax.axis_index("sub")
    rng = lax.axis_index("rng")
    last_rng = lax.axis_size("rng") - 1
    core = sub % 2
    z = sub // 2
    zl = z % 8
    base = z - zl
    quad = zl % 4
    upper = zl // 4
    half = (zl // 2) % 2
    side0 = zl % 2
    width = image.shape[3]
    hw = width // 2

    def load_image(j, place):
        return pltpu.make_async_copy(image_hbm.at[:, j], image.at[:, j], load_sem.at[place])

    load_weights = pltpu.make_async_copy(weights_hbm, weights, load_sem.at[1])
    load_taps = pltpu.make_async_copy(taps_hbm, taps, load_sem.at[2])
    load_shifts = pltpu.make_async_copy(shifts_hbm, shifts, load_sem.at[3])
    load_image(1 - core, 0).start()
    load_image(core, 4).start()
    load_weights.start()
    load_taps.start()
    load_shifts.start()

    def device(z_local, core_index):
        return {"sub": (base + z_local) * 2 + core_index}

    def order(z_local, core_index):
        return jnp.where(z_local * 2 + core_index == 0, 16, z_local * 2 + (1 - core_index))

    me = order(zl, core)
    partner = {"sub": z * 2 + (1 - core)}
    in_chips = [4 * core + q for q in range(4)]
    in_self = [jnp.logical_and(upper == core, quad == q) for q in range(4)]
    in_peers = [device(chip, upper) for chip in in_chips]
    in_later = [order(chip, upper) > me for chip in in_chips]
    out_self = [jnp.logical_and(in_self[q], side0 == core) for q in range(4)]
    out_dests = [device(chip, side0) for chip in in_chips]
    out_later = [order(chip, side0) > me for chip in in_chips]
    source_chips = [2 * k + core for k in range(4)]
    source_self = [jnp.logical_and(zl == source_chips[k], upper == core) for k in range(4)]
    out_sources = [device(chip, upper) for chip in source_chips]
    source_later = [order(chip, upper) > me for chip in source_chips]
    lower_rng, upper_rng = rng > 0, rng < last_rng

    barrier = pltpu.get_barrier_semaphore()

    def greet(who):
        pl.semaphore_signal(barrier, inc=1, device_id=who, device_id_type=MESH)

    def answer(sem, who):
        pl.semaphore_signal(sem, inc=1, device_id=who, device_id_type=MESH)

    def earlier(later, own):
        return jnp.logical_not(jnp.logical_or(later, own))

    @pl.when(core == 1)
    def _():
        greet(partner)

    @pl.when(lower_rng)
    def _():
        for c in range(2):
            greet({"sub": z * 2 + c, "rng": rng - 1})

    for peers, later in ((in_peers, in_later), (out_dests, out_later), (out_sources, source_later)):
        for q in range(4):
            @pl.when(later[q])
            def _():
                greet(peers[q])

    count = jnp.where(core == 0, 1, 0) + jnp.where(upper_rng, 2, 0)
    for later, own in ((in_later, in_self), (out_later, out_self), (source_later, source_self)):
        for q in range(4):
            count = count + jnp.where(earlier(later[q], own[q]), 1, 0)

    def enter():
        pl.when(count > 0)(lambda: pl.semaphore_wait(barrier, count))

        @pl.when(upper_rng)
        def _():
            for c in range(2):
                answer(ready_rng.at[core], {"sub": z * 2 + c, "rng": rng + 1})

        @pl.when(core == 0)
        def _():
            answer(ready_core, partner)

        for q in range(4):
            @pl.when(earlier(in_later[q], in_self[q]))
            def _():
                answer(ready_in.at[quad], in_peers[q])

            @pl.when(earlier(source_later[q], source_self[q]))
            def _():
                answer(ready_out.at[quad], out_sources[q])

    last_to_enter = jnp.logical_and(zl == 0, core == 0)
    pl.when(last_to_enter)(enter)

    def fill_phase(level, h, place):
        r = lax.broadcasted_iota(jnp.int32, (PERIOD, ANGLES), 0)
        a = lax.broadcasted_iota(jnp.int32, (PERIOD, ANGLES), 1)
        phase = ((r * (h * ANGLES + a + 1) * (7 + level)) % PERIOD).astype(F32) * PHASE_STEP
        c, s = jnp.cos(phase), jnp.sin(phase)
        for i in range(TABLE // PERIOD):
            cos_t[level, place, pl.ds(i * PERIOD, PERIOD), :] = c
            sin_t[level, place, pl.ds(i * PERIOD, PERIOD), :] = s

    def fill_table(level):
        for h in range(2):
            fill_phase(level, h, h)

    def transpose(j):
        for ch in range(2):
            for k in range(width // 128):
                block = image[ch, j, :, pl.ds(k * 128, 128)].astype(F32).T
                rows_bf[j, ch, pl.ds(k * 128, 128), :] = block.astype(BF16)

    load_image(1 - core, 0).wait()
    transpose(1 - core)
    pl.when(jnp.logical_not(last_to_enter))(enter)

    def fill_part(level, side, h, place):
        wr = weights[level, side, h, 0].astype(F32).T.astype(BF16)
        wi = weights[level, side, h, 1].astype(F32).T.astype(BF16)
        for c, x, value in ((0, 0, wr), (1, 0, -wi), (0, 1, wi), (1, 1, wr)):
            wide[level, pl.ds((side * 2 + c) * 128, 128), pl.ds((place * 2 + x) * 128, 128)] = value

    def fill_wide(level):
        for side in range(2):
            for h in range(2):
                fill_part(level, side, h, h)

    to_core = pltpu.make_async_remote_copy(
        src_ref=rows_bf.at[1 - core],
        dst_ref=from_core,
        send_sem=core_sem.at[0],
        recv_sem=core_sem.at[1],
        device_id=partner,
        device_id_type=MESH,
    )
    margin = LEVELS * RIM

    def halo_copy(j, lr):
        start = 0 if lr == 0 else width - margin
        return pltpu.make_async_remote_copy(
            src_ref=rows_bf.at[j, :, pl.ds(start, margin), :],
            dst_ref=halo.at[core, lr],
            send_sem=halo_send.at[j, lr],
            recv_sem=halo_recv.at[core, lr],
            device_id={"sub": z * 2 + j, "rng": rng - 1 + 2 * lr},
            device_id_type=MESH,
        )

    def halo_wait(side, lr):
        return pltpu.make_async_remote_copy(
            src_ref=rows_bf.at[0, :, pl.ds(0, margin), :],
            dst_ref=halo.at[side, lr],
            send_sem=halo_send.at[0, lr],
            recv_sem=halo_recv.at[side, lr],
            device_id=partner,
            device_id_type=MESH,
        )

    @pl.when(core == 1)
    def _():
        pl.semaphore_wait(ready_core, 1)

    to_core.start()
    load_image(core, 4).wait()
    transpose(core)

    @pl.when(upper_rng)
    def _():
        for j in range(2):
            halo_copy(j, 1).start()

    load_taps.wait()
    load_shifts.wait()
    load_weights.wait()
    fill_wide(0)
    fill_table(0)

    @pl.when(lower_rng)
    def _():
        for j in range(2):
            pl.semaphore_wait(ready_rng.at[j], 1)
            halo_copy(j, 0).start()

    for ch in range(2):
        first[core, ch, pl.ds(margin, width), :] = rows_bf[core, ch].astype(F32)
    to_core.wait_recv()
    for ch in range(2):
        first[1 - core, ch, pl.ds(margin, width), :] = from_core[ch].astype(F32)

    def take_halo(lr):
        start, there = ((margin + width, upper_rng), (0, lower_rng))[lr]

        @pl.when(there)
        def _():
            for side in range(2):
                halo_wait(side, lr).wait_recv()
                for ch in range(2):
                    first[side, ch, pl.ds(start, margin), :] = halo[side, lr, ch].astype(F32)

        @pl.when(jnp.logical_not(there))
        def _():
            first[:, :, pl.ds(start, margin), :] = jnp.zeros((2, 2, margin, ANGLES), F32)

    def bits_of(row):
        code = row + RIM
        return [((code // v) % 2) == 1 for v in (1, 2, 4, 8)]

    def shift_row(level, side):
        return shifts[level, pl.ds(side, 1), :]

    def interpolate(load, rows, bits, level):
        n = rows + 8
        b0, b1, b2, b3 = bits
        v = jnp.where(
            b3,
            jnp.where(b2, load(12, n), load(8, n)),
            jnp.where(b2, load(4, n), load(0, n)),
        )
        v = jnp.where(b0, pltpu.roll(v, n - 1, 0), v)
        v = jnp.where(b1, pltpu.roll(v, n - 2, 0), v)
        total = v * taps[level, 0]
        for t in range(1, TAPS):
            total = total + pltpu.roll(v, n - t, 0) * taps[level, t]
        return total[:rows].astype(BF16)

    def turn(level, h, start, rows, re, im):
        c = cos_t[level, h, pl.ds(start, rows), :]
        s = sin_t[level, h, pl.ds(start, rows), :]
        return re * c - im * s, re * s + im * c

    bits0 = [bits_of(shift_row(0, side)) for side in range(2)]
    rows1 = width + 2 * (margin - RIM)

    def level0(b, rows):
        parts = []
        for side in range(2):
            for ch in range(2):
                parts.append(interpolate(lambda o, n: first[side, ch, pl.ds(b + o, n), :], rows, bits0[side], 0))
        merged = jnp.dot(jnp.concatenate(parts, axis=1), wide[0], preferred_element_type=F32)
        start = (b - (margin - RIM)) % PERIOD
        for h in range(2):
            re, im = merged[:, h * 256 : h * 256 + 128], merged[:, h * 256 + 128 : h * 256 + 256]
            re, im = turn(0, h, start, rows, re, im)
            x1[h, 0, pl.ds(b, rows), :] = re
            x1[h, 1, pl.ds(b, rows), :] = im

    def clear1(start):
        x1[:, :, pl.ds(start, margin - RIM), :] = jnp.zeros((2, 2, margin - RIM, ANGLES), F32)

    own_bits1 = [((shift_row(1, side0) + RIM) // v) % 2 == 1 for v in (1, 2, 4, 8)]

    def nth(i):
        q = core * i + (1 - core) * (3 - i)
        chip = 4 * core + q
        own = jnp.logical_and(upper == core, quad == q)
        return q, own, device(chip, upper), order(chip, upper) > me

    ahead = jnp.logical_and(core == 1, jnp.logical_and(zl > 0, upper == 0))

    def in_copy(i, k):
        start, rows = CHUNK1[k]
        q, own, peer, later = nth(i)
        row = pl.multiple_of((q // 2) * hw + start, 32)
        return (
            y1.at[q % 2, :, pl.ds(row, rows), :],
            units.at[quad, :, pl.ds(start, rows), :],
            in_send.at[i, k],
            in_recv.at[quad, k],
            peer,
        )

    def send_unit(i, k):
        q, own, peer, later = nth(i)
        if k == 0:
            pl.when(later)(lambda: pl.semaphore_wait(ready_in.at[q], 1))
        start_copy(in_copy(i, k), own)

    def remote(src, dst, send, recv, peer):
        return pltpu.make_async_remote_copy(
            src_ref=src, dst_ref=dst, send_sem=send, recv_sem=recv, device_id=peer, device_id_type=MESH
        )

    def start_copy(parts, local):
        src, dst, send, recv, peer = parts

        @pl.when(local)
        def _():
            pltpu.make_async_copy(src, dst, recv).start()

        @pl.when(jnp.logical_not(local))
        def _():
            remote(*parts).start()

    def wait_sent(parts, local):
        @pl.when(jnp.logical_not(local))
        def _():
            remote(*parts).wait_send()

    for k in range(CHUNKS):
        level0(*ROWS0[k][0])
        if k == 0:
            take_halo(1)
        elif k == CHUNKS - 1:
            take_halo(0)
        level0(*ROWS0[k][1])
        if k == 0:
            pl.when(jnp.logical_not(lower_rng))(lambda: clear1(0))
        elif k == CHUNKS - 1:
            pl.when(jnp.logical_not(upper_rng))(lambda: clear1(rows1 - (margin - RIM)))
        start = CHUNK1[k][0]
        for part in range(2):
            if k == CHUNKS - 1 and part == 0:
                rows = hw - start
            else:
                rows = CHUNK1[k][1]
            for h in range(2):
                for ch in range(2):
                    at = part * hw + start
                    y1[h, ch, pl.ds(at, rows), :] = interpolate(
                        lambda o, n: x1[h, ch, pl.ds(at + o, n), :], rows, own_bits1, 1
                    )
        @pl.when(jnp.logical_not(ahead))
        def _():
            for i in range(3):
                send_unit(i, k)

        if k == CHUNKS - 1:
            @pl.when(ahead)
            def _():
                for i in range(3):
                    for each in range(CHUNKS):
                        send_unit(i, each)

        if k < CHUNKS - 1:
            pl.when(zl == 0)(lambda: send_unit(3, k))
        else:
            @pl.when(zl > 0)
            def _():
                for each in range(CHUNKS - 1):
                    send_unit(3, each)

            send_unit(3, k)

    fill_wide(1)
    fill_table(1)
    fill_wide(2)
    fill_table(2)
    for side in range(2):
        fill_part(3, side, core, 0)
    fill_phase(3, core, 0)

    bits2 = [bits_of(shift_row(2, side)) for side in range(2)]
    bits3 = bits_of(shift_row(3, core))
    at_start = jnp.logical_and(rng == 0, half == 0)
    at_end = jnp.logical_and(rng == last_rng, half == 1)

    def merge(level, lhs, start_row, rows, margin_rows, dst, slots):
        z = jnp.dot(lhs, wide[level], preferred_element_type=F32)
        start = (start_row - margin_rows) % PERIOD
        for h in range(2):
            re, im = turn(level, h, start, rows, z[:, h * 256 : h * 256 + 128], z[:, h * 256 + 128 : h * 256 + 256])
            dst[slots[h], 0, pl.ds(start_row, rows), :] = re
            dst[slots[h], 1, pl.ds(start_row, rows), :] = im

    def clear(dst, k, margin_rows):
        total = hw + 2 * margin_rows
        if 0 < k < CHUNKS - 1:
            return

        @pl.when(at_start if k == 0 else at_end)
        def _():
            at = 0 if k == 0 else total - margin_rows
            dst[:, :, pl.ds(at, margin_rows), :] = jnp.zeros((4, 2, margin_rows, ANGLES), F32)

    def pair_copy(k):
        start, rows = CHUNK3[k]
        ref = y3.at[core, :, :, pl.ds(start, rows), :]
        return pltpu.make_async_remote_copy(
            src_ref=ref, dst_ref=ref, send_sem=pair_send.at[k], recv_sem=pair_recv.at[k],
            device_id=partner, device_id_type=MESH,
        )

    def pair_wait(k):
        start, rows = CHUNK3[k]
        ref = y3.at[1 - core, :, :, pl.ds(start, rows), :]
        return pltpu.make_async_remote_copy(
            src_ref=ref, dst_ref=ref, send_sem=pair_send.at[k], recv_sem=pair_recv.at[k],
            device_id=partner, device_id_type=MESH,
        )

    def out_copy(q, k):
        start, rows = CHUNK3[k]
        row = pl.multiple_of(half * hw + start, 64)
        return (
            turned.at[q, :, pl.ds(start, rows), :],
            blocks.at[upper, :, pl.ds(row, rows), :],
            out_send.at[q, k],
            out_recv.at[zl // 2, k],
            out_dests[q],
        )

    def send_block(q, k):
        if k == 0:
            pl.when(out_later[q])(lambda: pl.semaphore_wait(ready_out.at[q], 1))
        start_copy(out_copy(q, k), out_self[q])

    for k in range(CHUNKS):
        start, rows = CHUNK1[k]
        for s in range(4):
            ref = units.at[s, :, pl.ds(start, rows), :]
            pltpu.make_async_remote_copy(
                src_ref=ref, dst_ref=ref, send_sem=in_send.at[0, k], recv_sem=in_recv.at[s, k],
                device_id=partner, device_id_type=MESH,
            ).wait_recv()
        for p in range(2):
            lhs = jnp.concatenate(
                [units[2 * p + side, ch, pl.ds(start, rows), :] for side in range(2) for ch in range(2)], axis=1
            )
            merge(1, lhs, start, rows, 2 * RIM, x2, (2 * p, 2 * p + 1))
        clear(x2, k, 2 * RIM)
        start, rows = CHUNK2[k]
        for p in range(2):
            lhs = jnp.concatenate(
                [
                    interpolate(lambda o, n: x2[p + 2 * side, ch, pl.ds(start + o, n), :], rows, bits2[side], 2)
                    for side in range(2)
                    for ch in range(2)
                ],
                axis=1,
            )
            merge(2, lhs, start, rows, RIM, x3, (p, p + 2))
        clear(x3, k, RIM)
        start, rows = CHUNK3[k]
        for s in range(4):
            for ch in range(2):
                y3[core, s, ch, pl.ds(start, rows), :] = interpolate(
                    lambda o, n: x3[s, ch, pl.ds(start + o, n), :], rows, bits3, 3
                )
        pair_copy(k).start()
        pair_wait(k).wait_recv()
        for s in range(4):
            lhs = jnp.concatenate(
                [y3[side, s, ch, pl.ds(start, rows), :] for side in range(2) for ch in range(2)], axis=1
            )
            merged = jnp.dot(lhs, wide[3, :, pl.ds(0, 256)], preferred_element_type=F32)
            re, im = turn(3, 0, start % PERIOD, rows, merged[:, :128], merged[:, 128:])
            turned[s, 0, pl.ds(start, rows), :] = re.astype(BF16)
            turned[s, 1, pl.ds(start, rows), :] = im.astype(BF16)
        for q in range(2):
            send_block(q, k)
    for q in range(2, 4):
        for k in range(CHUNKS):
            send_block(q, k)

    to_core.wait_send()
    for j in range(2):
        @pl.when(lower_rng)
        def _():
            halo_copy(j, 0).wait_send()

        @pl.when(upper_rng)
        def _():
            halo_copy(j, 1).wait_send()

    for k in range(CHUNKS):
        for i in range(4):
            wait_sent(in_copy(i, k), nth(i)[1])
        pair_copy(k).wait_send()
        for q in range(4):
            wait_sent(out_copy(q, k), out_self[q])

    def block_wait(s, k):
        start, rows = CHUNK3[k]
        ref = blocks.at[s // 2, :, pl.ds((s % 2) * hw + start, rows), :]
        remote(ref, ref, out_send.at[0, k], out_recv.at[s, k], partner).wait_recv()

    for first_chunk, last_chunk, col in ((0, 1, 0), (2, 2, 128)):
        for s in range(4):
            for k in range(first_chunk, last_chunk + 1):
                block_wait(s, k)
            at = (s % 2) * hw + col
            for ch in range(2):
                block = blocks[s // 2, ch, pl.ds(at, 128), :].astype(F32).T
                out[ch, s // 2, :, pl.ds(at, 128)] = block.astype(BF16)


def on_device(image, interp_weights, range_taps, range_shifts):
    width = image.shape[3]
    hw = width // 2
    margin = LEVELS * RIM
    dma = pltpu.SemaphoreType.DMA
    vmem = pltpu.VMEM
    return pl.pallas_call(
        kernel,
        out_shape=pltpu.VMEM(image.shape, image.dtype),
        in_specs=[
            pl.BlockSpec(memory_space=pl.ANY),
            pl.BlockSpec(memory_space=pl.ANY),
            pl.BlockSpec(memory_space=pl.ANY),
            pl.BlockSpec(memory_space=pl.ANY),
        ],
        out_specs=pl.BlockSpec(memory_space=pltpu.VMEM),
        scratch_shapes=[
            vmem(image.shape, BF16),
            vmem(interp_weights.shape, BF16),
            pltpu.SMEM(range_taps.shape, F32),
            vmem(range_shifts.shape, jnp.int32),
            vmem((LEVELS, 512, 512), BF16),
            vmem((LEVELS, 2, TABLE, ANGLES), F32),
            vmem((LEVELS, 2, TABLE, ANGLES), F32),
            vmem((2, 2, width, ANGLES), BF16),
            vmem((2, 2, width + 2 * margin + 16, ANGLES), F32),
            vmem((2, width, ANGLES), BF16),
            vmem((2, 2, 2, margin, ANGLES), BF16),
            vmem((2, 2, width + 6 * RIM + 16, ANGLES), F32),
            vmem((2, 2, width + 4 * RIM, ANGLES), BF16),
            vmem((4, 2, hw + 4 * RIM, ANGLES), BF16),
            vmem((4, 2, hw + 4 * RIM + 16, ANGLES), F32),
            vmem((4, 2, hw + 2 * RIM + 16, ANGLES), F32),
            vmem((2, 4, 2, hw, ANGLES), BF16),
            vmem((4, 2, hw, ANGLES), BF16),
            vmem((2, 2, width, ANGLES), BF16),
            dma((5,)),
            dma((2,)),
            dma((2, 2)),
            dma((2, 2)),
            dma((4, CHUNKS)),
            dma((4, CHUNKS)),
            dma((CHUNKS,)),
            dma((CHUNKS,)),
            dma((4, CHUNKS)),
            dma((4, CHUNKS)),
            pltpu.SemaphoreType.REGULAR,
            pltpu.SemaphoreType.REGULAR((2,)),
            pltpu.SemaphoreType.REGULAR((4,)),
            pltpu.SemaphoreType.REGULAR((4,)),
        ],
        compiler_params=pltpu.CompilerParams(collective_id=0, has_side_effects=True),
        name="backprojection",
    )(image, interp_weights, range_taps, range_shifts)


def solution(mesh):
    return jax.shard_map(
        on_device,
        mesh=mesh,
        in_specs=(P(None, ("img", "sub"), None, "rng"), P(), P(), P()),
        out_specs=P(None, ("img", "sub"), None, "rng"),
        check_vma=False,
    )
```
